32 devices in a mesh: data: 2 (over x), fsdp: 4 (over z), ep: 4 (over y, core).
Axes of the slice: x: 2, y: 2, z: 4, core: 2. Of those that a mesh axis runs over, the one named last changes fastest.
Arguments:
- x_in: bfloat16 [32, 512, 1024], P(('data', 'fsdp', 'ep')), parts along dimension 0
- expert_idx: int32 [32, 512, 8], P(('data', 'fsdp', 'ep')), parts along dimension 0
- expert_slot: int32 [32, 512, 8], P(('data', 'fsdp', 'ep')), parts along dimension 0
- expert_gate: bfloat16 [32, 512, 8], P(('data', 'fsdp', 'ep')), parts along dimension 0
- attn_gain: bfloat16 [1024], replicated
- w_qkv: bfloat16 [1024, 3, 16, 64], P('fsdp')
- w_out: bfloat16 [16, 64, 1024], P('fsdp')
- moe_gain: bfloat16 [1024], replicated
- w_gate: bfloat16 [32, 1024, 512], P('ep', 'fsdp')
- w_up: bfloat16 [32, 1024, 512], P('ep', 'fsdp')
- w_down: bfloat16 [32, 512, 1024], P('ep', None, 'fsdp')
Outputs:
- output: bfloat16 [32, 512, 1024], P(('data', 'fsdp', 'ep')), parts along dimension 0
There are 2 independent parts. The reference program is written for one: setup_inputs(seed, part) draws one part's arguments, and reference() takes and returns one part's arrays. A program takes and returns all parts, laid end to end along the dimension named above; an argument that names none is the same for every part.
All inputs are finite; a program needn't handle non-finite values.
Results may differ from the reference program's by a relative error of at most 0.0144674.
Values are sent between devices in bfloat16 or wider.
A program may use at most 1 GiB of HBM per device.

```python
import jax
import jax.numpy as jnp
from jax import lax

D_MODEL = 1024
N_HEADS = 16
HEAD_DIM = 64
EXPERTS = 32
TOP_K = 8
FFN_DIM = 512
BATCH_DEV = 1
SEQ_LEN = 512
FSDP_SIZE = 4
EP_SIZE = 4
CAPACITY = 168

N_DEV = FSDP_SIZE * EP_SIZE
BATCH_ROWS = N_DEV * BATCH_DEV
TOK_DEV = BATCH_DEV * SEQ_LEN
COVER_LEN = (EXPERTS + N_DEV - 1) // N_DEV
NORM_EPS = 1e-6
ROPE_BASE = 10000.0


def draw_routing(rng_key):
    key_base, key_perm, key_hot = jax.random.split(rng_key, 3)
    base_score = jax.random.randint(key_base, (N_DEV, TOK_DEV, EXPERTS), 0, 4096)
    skew_bias = jax.random.permutation(key_perm, EXPERTS) * (4096 // EXPERTS)
    hot_expert = jax.random.randint(key_hot, (), 0, EXPERTS)
    expert_ids = jnp.arange(EXPERTS)
    tok_pos = jnp.arange(TOK_DEV)[None, :]
    dev_pos = jnp.arange(N_DEV)[:, None]
    cover_ids = (dev_pos * COVER_LEN + tok_pos - CAPACITY) % EXPERTS
    in_cover = (tok_pos >= CAPACITY) & (tok_pos < CAPACITY + COVER_LEN)
    forced = jnp.where(tok_pos < CAPACITY, hot_expert, jnp.where(in_cover, cover_ids, -1))
    route_score = base_score + skew_bias + 16384 * (forced[:, :, None] == expert_ids).astype(jnp.int32)
    route_score = route_score * EXPERTS + expert_ids
    chosen = lax.top_k(route_score, TOP_K)[1].astype(jnp.int32)

    def slot_one(dev_ids):
        flat_ids = dev_ids.reshape(TOK_DEV * TOP_K)
        hit_mask = (flat_ids[:, None] == expert_ids[None, :]).astype(jnp.int32)
        prior_count = jnp.sum((jnp.cumsum(hit_mask, axis=0) - hit_mask) * hit_mask, axis=1)
        return jnp.where(prior_count < CAPACITY, prior_count, -1).reshape(TOK_DEV, TOP_K)

    slot_vals = lax.map(slot_one, chosen).astype(jnp.int32)
    out_shape = (BATCH_ROWS, SEQ_LEN, TOP_K)
    return chosen.reshape(out_shape), slot_vals.reshape(out_shape)


def setup_inputs(seed: int = 0, part: int = 0) -> dict:
    part_key = jax.random.fold_in(jax.random.key(seed), part)
    key_tokens, key_route, key_weights = jax.random.split(part_key, 3)
    shared = jax.random.split(jax.random.key(seed + 1), 7)
    expert_idx, expert_slot = draw_routing(key_route)
    x_in = jax.random.normal(key_tokens, (BATCH_ROWS, SEQ_LEN, D_MODEL), jnp.float32)
    expert_gate = jax.random.uniform(key_weights, (BATCH_ROWS, SEQ_LEN, TOP_K), jnp.float32, 0.5, 1.5)
    attn_gain = jax.random.uniform(shared[0], (D_MODEL,), jnp.float32, 0.5, 1.5)
    moe_gain = jax.random.uniform(shared[1], (D_MODEL,), jnp.float32, 0.5, 1.5)
    w_qkv = jax.random.normal(shared[2], (D_MODEL, 3, N_HEADS, HEAD_DIM), jnp.float32) * (1.5 * D_MODEL ** -0.5)
    w_out = jax.random.normal(shared[3], (N_HEADS, HEAD_DIM, D_MODEL), jnp.float32) * (N_HEADS * HEAD_DIM) ** -0.5
    w_gate = jax.random.normal(shared[4], (EXPERTS, D_MODEL, FFN_DIM), jnp.float32) * D_MODEL ** -0.5
    w_up = jax.random.normal(shared[5], (EXPERTS, D_MODEL, FFN_DIM), jnp.float32) * D_MODEL ** -0.5
    w_down = jax.random.normal(shared[6], (EXPERTS, FFN_DIM, D_MODEL), jnp.float32) * FFN_DIM ** -0.5
    return {
        'x_in': x_in.astype(jnp.bfloat16),
        'expert_idx': expert_idx,
        'expert_slot': expert_slot,
        'expert_gate': expert_gate.astype(jnp.bfloat16),
        'attn_gain': attn_gain.astype(jnp.bfloat16),
        'w_qkv': w_qkv.astype(jnp.bfloat16),
        'w_out': w_out.astype(jnp.bfloat16),
        'moe_gain': moe_gain.astype(jnp.bfloat16),
        'w_gate': w_gate.astype(jnp.bfloat16),
        'w_up': w_up.astype(jnp.bfloat16),
        'w_down': w_down.astype(jnp.bfloat16),
    }


def rms_norm(hidden, gain_vec):
    wide = hidden.astype(jnp.float32)
    inv_rms = lax.rsqrt(jnp.mean(wide * wide, axis=-1, keepdims=True) + NORM_EPS)
    return (wide * inv_rms * gain_vec.astype(jnp.float32)).astype(jnp.bfloat16)


def rope_tables():
    half_dim = HEAD_DIM // 2
    inv_freq = ROPE_BASE ** (-jnp.arange(half_dim, dtype=jnp.float32) / half_dim)
    angles = jnp.arange(SEQ_LEN, dtype=jnp.float32)[:, None] * inv_freq[None, :]
    return jnp.cos(angles)[:, None, :], jnp.sin(angles)[:, None, :]


def rotate(heads_in, cos_tab, sin_tab):
    half_dim = HEAD_DIM // 2
    first_half = heads_in[..., :half_dim]
    second_half = heads_in[..., half_dim:]
    return jnp.concatenate([first_half * cos_tab - second_half * sin_tab, second_half * cos_tab + first_half * sin_tab], axis=-1)


def attend_one(seq_in, attn_gain, w_qkv, w_out, cos_tab, sin_tab):
    normed = rms_norm(seq_in, attn_gain)
    qkv_proj = jnp.dot(normed, w_qkv.reshape(D_MODEL, 3 * N_HEADS * HEAD_DIM), preferred_element_type=jnp.float32).reshape(SEQ_LEN, 3, N_HEADS, HEAD_DIM)
    query_rot = rotate(qkv_proj[:, 0], cos_tab, sin_tab).astype(jnp.bfloat16).astype(jnp.float32)
    keys_rot = rotate(qkv_proj[:, 1], cos_tab, sin_tab).astype(jnp.bfloat16).astype(jnp.float32)
    values = qkv_proj[:, 2].astype(jnp.bfloat16).astype(jnp.float32)
    scores = jnp.einsum('qhd,khd->hqk', query_rot, keys_rot) * (HEAD_DIM ** -0.5)
    causal = jnp.arange(SEQ_LEN)[:, None] >= jnp.arange(SEQ_LEN)[None, :]
    attn_probs = jax.nn.softmax(jnp.where(causal[None], scores, -1e30), axis=-1).astype(jnp.bfloat16)
    context = jnp.einsum('hqk,khd->qhd', attn_probs.astype(jnp.float32), values).astype(jnp.bfloat16)
    attn_out = jnp.dot(context.reshape(SEQ_LEN, N_HEADS * HEAD_DIM), w_out.reshape(N_HEADS * HEAD_DIM, D_MODEL), preferred_element_type=jnp.float32)
    return (seq_in.astype(jnp.float32) + attn_out).astype(jnp.bfloat16)


def reference(x_in, expert_idx, expert_slot, expert_gate, attn_gain, w_qkv, w_out, moe_gain, w_gate, w_up, w_down):
    cos_tab, sin_tab = rope_tables()
    hidden = lax.map(lambda seq_in: attend_one(seq_in, attn_gain, w_qkv, w_out, cos_tab, sin_tab), x_in)
    normed = rms_norm(hidden, moe_gain).reshape(N_DEV, TOK_DEV, D_MODEL)
    total_slots = EXPERTS * CAPACITY
    dest_pos = jnp.where(expert_slot >= 0, expert_idx * CAPACITY + expert_slot, total_slots).reshape(N_DEV, TOK_DEV * TOP_K)
    gate_flat = expert_gate.astype(jnp.float32).reshape(N_DEV, TOK_DEV * TOP_K)
    tok_index = jnp.broadcast_to(jnp.arange(TOK_DEV)[:, None], (TOK_DEV, TOP_K)).reshape(TOK_DEV * TOP_K)

    def invert(dest_row, gate_row):
        owner_row = jnp.full((total_slots,), TOK_DEV, jnp.int32).at[dest_row].set(tok_index, mode='drop')
        weight_row = jnp.zeros((total_slots,), jnp.float32).at[dest_row].set(gate_row, mode='drop')
        return owner_row, weight_row

    owner_tok, slot_weight = jax.vmap(invert)(dest_pos, gate_flat)
    owner_tok = owner_tok.reshape(N_DEV, EXPERTS, CAPACITY).transpose(1, 0, 2)
    slot_weight = slot_weight.reshape(N_DEV, EXPERTS, CAPACITY).transpose(1, 0, 2)

    def expert_step(moe_acc, step_in):
        owner_e, weight_e, gate_w, up_w, down_w = step_in
        safe_ids = jnp.minimum(owner_e, TOK_DEV - 1)
        tok_rows = jax.vmap(lambda dev_rows, row_ids: dev_rows[row_ids])(normed, safe_ids).reshape(N_DEV * CAPACITY, D_MODEL)
        gate_act = jnp.dot(tok_rows, gate_w, preferred_element_type=jnp.float32)
        up_act = jnp.dot(tok_rows, up_w, preferred_element_type=jnp.float32)
        inner_act = (jax.nn.silu(gate_act) * up_act).astype(jnp.bfloat16)
        expert_out = jnp.dot(inner_act, down_w, preferred_element_type=jnp.float32).astype(jnp.bfloat16)
        contrib = expert_out.astype(jnp.float32).reshape(N_DEV, CAPACITY, D_MODEL) * weight_e[:, :, None]
        moe_acc = jax.vmap(lambda acc_rows, row_ids, add_rows: acc_rows.at[row_ids].add(add_rows, mode='drop'))(moe_acc, owner_e, contrib)
        return moe_acc, None

    moe_sum = lax.scan(expert_step, jnp.zeros((N_DEV, TOK_DEV, D_MODEL), jnp.float32), (owner_tok, slot_weight, w_gate, w_up, w_down))[0]
    result = hidden.astype(jnp.float32) + moe_sum.reshape(BATCH_ROWS, SEQ_LEN, D_MODEL)
    return result.astype(jnp.bfloat16)
```

```python
import functools

import jax
import jax.numpy as jnp
from jax import lax
from jax.experimental import pallas as pl
from jax.experimental.pallas import tpu as pltpu
from jax.sharding import PartitionSpec as P

NORM_EPS = 1e-6
ROPE_BASE = 10000.0
MESH_ID = pl.DeviceIdType.MESH
VMEM_LIMIT = 60 * 1024 * 1024


def rms_norm(hidden, gain_vec):
    wide = hidden.astype(jnp.float32)
    inv_rms = lax.rsqrt(jnp.mean(wide * wide, axis=-1, keepdims=True) + NORM_EPS)
    return (wide * inv_rms * gain_vec.astype(jnp.float32)).astype(jnp.bfloat16)


def attention_block(x_blk, attn_gain, w_qkv, w_out):
    seq_len = x_blk.shape[1]
    head_dim = w_qkv.shape[3]
    half_dim = head_dim // 2
    normed = rms_norm(x_blk, attn_gain)
    qkv_proj = jnp.einsum('bsd,dthe->bsthe', normed, w_qkv, preferred_element_type=jnp.float32)
    inv_freq = ROPE_BASE ** (-jnp.arange(half_dim, dtype=jnp.float32) / half_dim)
    angles = jnp.arange(seq_len, dtype=jnp.float32)[:, None] * inv_freq[None, :]
    cos_tab = jnp.cos(angles)[None, :, None, :]
    sin_tab = jnp.sin(angles)[None, :, None, :]

    def rotate(heads_in):
        first_half = heads_in[..., :half_dim]
        second_half = heads_in[..., half_dim:]
        return jnp.concatenate([first_half * cos_tab - second_half * sin_tab, second_half * cos_tab + first_half * sin_tab], axis=-1)

    query_rot = rotate(qkv_proj[:, :, 0]).astype(jnp.bfloat16)
    keys_rot = rotate(qkv_proj[:, :, 1]).astype(jnp.bfloat16)
    values = qkv_proj[:, :, 2].astype(jnp.bfloat16)
    scores = jnp.einsum('bqhe,bkhe->bhqk', query_rot, keys_rot, preferred_element_type=jnp.float32) * (head_dim ** -0.5)
    causal = jnp.arange(seq_len)[:, None] >= jnp.arange(seq_len)[None, :]
    attn_probs = jax.nn.softmax(jnp.where(causal, scores, -1e30), axis=-1).astype(jnp.bfloat16)
    context = jnp.einsum('bhqk,bkhe->bqhe', attn_probs, values, preferred_element_type=jnp.float32).astype(jnp.bfloat16)
    attn_out = jnp.einsum('crif,ife->cre', context, w_out, preferred_element_type=jnp.float32)
    return (x_blk.astype(jnp.float32) + attn_out).astype(jnp.bfloat16)


def capacity_of(tok_count, top_k, experts):
    return 8 * ((5 * tok_count * top_k) // (32 * experts) + 1)


def layer_place():
    dx, dz, ep = lax.axis_index('data'), lax.axis_index('fsdp'), lax.axis_index('ep')
    return dx, dz, ep // 2, ep % 2


def flip(pos, bit):
    return (1 - pos) if bit else pos


def related(place, chip_rel, core_rel):
    dx, dz, dy, dc = place
    return flip(dx, chip_rel & 1), dz, flip(dy, chip_rel & 2), flip(dc, core_rel)


def slot_of(place):
    dx, _, dy, dc = place
    return dx * 4 + dy * 2 + dc


def dev_id(place):
    dx, dz, dy, dc = place
    return (dx, dz, dy * 2 + dc)


def greet(places):
    barrier = pltpu.get_barrier_semaphore()
    for place in places:
        pl.semaphore_signal(barrier, inc=1, device_id=dev_id(place), device_id_type=MESH_ID)
    pl.semaphore_wait(barrier, len(places))


class Sender:
    def __init__(self, send_sems):
        self.send_sems = send_sems
        self.copies = []

    def send(self, src, dst, recv_sem, place):
        copy = pltpu.make_async_remote_copy(src_ref=src, dst_ref=dst, send_sem=self.send_sems.at[len(self.copies)], recv_sem=recv_sem, device_id=dev_id(place), device_id_type=MESH_ID)
        copy.start()
        self.copies.append(copy)
        return copy

    def drain(self):
        for copy in self.copies:
            copy.wait_send()


def wait_in(ref, sem):
    pltpu.make_async_copy(ref, ref, sem).wait()


def spread_in_layer(place, sender, own_src, part_ref, recv_sems):
    across_x, across_y, partner = related(place, 1, 0), related(place, 2, 0), related(place, 0, 1)
    mine = slot_of(place)

    def pass_on(chip_rel, half, target, rel_there, core_there, first=False):
        owner = slot_of(related(place, chip_rel, 0))
        src = own_src(half) if first else part_ref(owner, half)
        sender.send(src, part_ref(owner, half), recv_sems(rel_there, core_there, half), target)

    for half in (0, 1):
        pass_on(0, half, across_x, 1, 0, True)
        pass_on(0, 1 - half, across_y, 2, 0, True)
    for half in (0, 1):
        pass_on(0, half, partner, 0, 1, True)
    yield

    def arrived(chip_rel, core_rel, half):
        owner = slot_of(related(place, chip_rel, core_rel))
        wait_in(part_ref(owner, half), recv_sems(chip_rel, core_rel, half))

    arrived(1, 0, 0)
    pass_on(1, 0, across_y, 3, 0)
    pass_on(1, 0, partner, 1, 1)
    arrived(2, 0, 1)
    pass_on(2, 1, across_x, 3, 0)
    pass_on(2, 1, partner, 2, 1)
    yield
    arrived(1, 0, 1)
    pass_on(1, 1, partner, 1, 1)
    arrived(2, 0, 0)
    pass_on(2, 0, partner, 2, 1)
    yield
    arrived(3, 0, 0)
    pass_on(3, 0, partner, 3, 1)
    arrived(3, 0, 1)
    pass_on(3, 1, partner, 3, 1)
    yield
    for chip_rel in range(4):
        for half in (0, 1):
            arrived(chip_rel, 1, half)
    yield


def attn_gather_kernel(shard_ref, out_ref, send_sems, z_sems, recv_sems, own_sem):
    place = layer_place()
    dx, dz, dy, dc = place
    rows = shard_ref.shape[0]
    piece = rows // 8
    z_peers = [(dx, (dz + step) % 4, dy, dc) for step in (1, 2, 3)]
    layer_peers = [related(place, 1, 0), related(place, 2, 0), related(place, 0, 1)]
    greet(z_peers + layer_peers)
    sender = Sender(send_sems)
    mine = slot_of(place)
    my_rows = pl.ds(pl.multiple_of(mine * piece, piece), piece)
    for index, step in enumerate((1, 3, 2)):
        target = (dx, (dz + step) % 4, dy, dc)
        dst = out_ref.at[pl.ds(pl.multiple_of(dz * rows + mine * piece, piece), piece)]
        sender.send(shard_ref.at[my_rows], dst, z_sems.at[index], target)
    own = pltpu.make_async_copy(shard_ref, out_ref.at[pl.ds(pl.multiple_of(dz * rows, rows), rows)], own_sem)
    own.start()
    streams = []
    for index, step in enumerate((1, 3, 2)):
        source_z = (dz + 4 - step) % 4

        def part_ref(slot, half, source_z=source_z):
            start = source_z * rows + slot * piece + half * (piece // 2)
            return out_ref.at[pl.ds(pl.multiple_of(start, piece // 2), piece // 2)]

        def recv_sem(chip_rel, core_rel, half, index=index):
            return recv_sems.at[index, chip_rel, core_rel, half]

        whole = out_ref.at[pl.ds(pl.multiple_of(source_z * rows + mine * piece, piece), piece)]
        streams.append((whole, index, spread_in_layer(place, sender, functools.partial(part_ref, mine), part_ref, recv_sem)))
    for whole, index, stream in streams:
        wait_in(whole, z_sems.at[index])
        next(stream)
    for _ in range(4):
        for _, _, stream in streams:
            next(stream)
    own.wait()
    sender.drain()


def gather_attention_weights(shard):
    rows, cols = shard.shape
    n_send = 3 + 3 * 14
    return pl.pallas_call(
        attn_gather_kernel,
        out_shape=jax.ShapeDtypeStruct((4 * rows, cols), shard.dtype),
        in_specs=[pl.BlockSpec(memory_space=pltpu.VMEM)],
        out_specs=pl.BlockSpec(memory_space=pl.ANY),
        scratch_shapes=[
            pltpu.SemaphoreType.DMA((n_send,)),
            pltpu.SemaphoreType.DMA((3,)),
            pltpu.SemaphoreType.DMA((3, 4, 2, 2)),
            pltpu.SemaphoreType.DMA,
        ],
        compiler_params=pltpu.CompilerParams(collective_id=1, has_side_effects=True, vmem_limit_bytes=VMEM_LIMIT),
        cost_estimate=pl.CostEstimate(flops=30_000_000_000, bytes_accessed=10_000_000, transcendentals=0),
        name='attn_gather',
    )(shard)


def token_gather_kernel(own_ref, out_ref, send_sems, recv_sems, own_sem):
    place = layer_place()
    greet([related(place, 1, 0), related(place, 2, 0), related(place, 0, 1)])
    sender = Sender(send_sems)
    half_rows = own_ref.shape[0] // 2

    def part_ref(slot, half):
        return out_ref.at[slot, pl.ds(half * half_rows, half_rows)]

    def own_half(half):
        return own_ref.at[pl.ds(half * half_rows, half_rows)]

    def recv_sem(chip_rel, core_rel, half):
        return recv_sems.at[chip_rel, core_rel, half]

    stream = spread_in_layer(place, sender, own_half, part_ref, recv_sem)
    next(stream)
    own = pltpu.make_async_copy(own_ref, out_ref.at[slot_of(place)], own_sem)
    own.start()
    for _ in range(4):
        next(stream)
    own.wait()
    sender.drain()


def gather_tokens(own):
    rows, cols = own.shape
    return pl.pallas_call(
        token_gather_kernel,
        out_shape=jax.ShapeDtypeStruct((8, rows, cols), own.dtype),
        in_specs=[pl.BlockSpec(memory_space=pltpu.VMEM)],
        out_specs=pl.BlockSpec(memory_space=pl.ANY),
        scratch_shapes=[
            pltpu.SemaphoreType.DMA((14,)),
            pltpu.SemaphoreType.DMA((4, 2, 2)),
            pltpu.SemaphoreType.DMA,
        ],
        compiler_params=pltpu.CompilerParams(collective_id=2, has_side_effects=True, vmem_limit_bytes=VMEM_LIMIT),
        cost_estimate=pl.CostEstimate(flops=30_000_000_000, bytes_accessed=10_000_000, transcendentals=0),
        name='token_gather',
    )(own)


def dispatch_kernel(capacity, u_ref, slot_row_ref, slot_col_ref, gate_col_ref, rows_ref, comb_ref):
    tokens = u_ref.shape[0]
    n_exp = slot_row_ref.shape[0]
    slot_ids = lax.broadcasted_iota(jnp.int32, (capacity, tokens), 0).astype(jnp.float32)
    for e in range(n_exp):
        one_hot = jnp.where(slot_ids == slot_row_ref[e:e + 1, :], 1.0, 0.0).astype(jnp.bfloat16)
        rows_ref[e] = jnp.dot(one_hot, u_ref[...], preferred_element_type=jnp.float32).astype(jnp.bfloat16)
    buf_ids = lax.broadcasted_iota(jnp.int32, (tokens, n_exp * capacity), 1).astype(jnp.float32)
    comb = jnp.zeros((tokens, n_exp * capacity), jnp.float32)
    for e in range(n_exp):
        slot_e = slot_col_ref[:, e:e + 1]
        dest_e = jnp.where(slot_e >= 0.0, slot_e + float(e * capacity), -1.0)
        comb = jnp.where(buf_ids == dest_e, gate_col_ref[:, e:e + 1], comb)
    comb_ref[...] = comb.astype(jnp.bfloat16)


def dispatch(gathered, slot_row, slot_col, gate_col, tokens, capacity):
    n_src, _, cols = gathered.shape
    n_exp = slot_row.shape[1]
    return pl.pallas_call(
        functools.partial(dispatch_kernel, capacity),
        grid=(n_src,),
        out_shape=(
            jax.ShapeDtypeStruct((n_exp, n_src, capacity, cols), jnp.bfloat16),
            jax.ShapeDtypeStruct((n_src, tokens, n_exp * capacity), jnp.bfloat16),
        ),
        in_specs=[
            pl.BlockSpec((None, tokens, cols), lambda s: (s, 0, 0)),
            pl.BlockSpec((None, n_exp, tokens), lambda s: (s, 0, 0)),
            pl.BlockSpec((None, tokens, n_exp), lambda s: (s, 0, 0)),
            pl.BlockSpec((None, tokens, n_exp), lambda s: (s, 0, 0)),
        ],
        out_specs=(
            pl.BlockSpec((n_exp, None, capacity, cols), lambda s: (0, s, 0, 0)),
            pl.BlockSpec((None, tokens, n_exp * capacity), lambda s: (s, 0, 0)),
        ),
        compiler_params=pltpu.CompilerParams(vmem_limit_bytes=VMEM_LIMIT),
        cost_estimate=pl.CostEstimate(flops=10_000_000_000, bytes_accessed=30_000_000, transcendentals=0),
        name='dispatch',
    )(gathered, slot_row, slot_col, gate_col)


def inner_kernel(rows_ref, gate_ref, up_ref, inner_ref):
    depth = rows_ref.shape[-1]
    gate_w = gate_ref[...].reshape(depth, gate_ref.shape[-1])
    up_w = up_ref[...].reshape(depth, up_ref.shape[-1])
    gate_act = jnp.dot(rows_ref[...], gate_w, preferred_element_type=jnp.float32)
    up_act = jnp.dot(rows_ref[...], up_w, preferred_element_type=jnp.float32)
    inner_ref[...] = (gate_act * jax.nn.sigmoid(gate_act) * up_act).astype(jnp.bfloat16)


def expert_inner(rows, w_gate, w_up):
    n_exp, n_src, capacity, depth = rows.shape
    parts, _, part_depth, ffn = w_gate.shape
    tall = rows.reshape(n_exp, n_src * capacity, depth)
    tile = n_src * capacity // 2
    weight_spec = pl.BlockSpec((parts, None, part_depth, ffn), lambda e, t: (0, e, 0, 0))
    return pl.pallas_call(
        inner_kernel,
        grid=(n_exp, 2),
        out_shape=jax.ShapeDtypeStruct((n_exp, n_src * capacity, ffn), jnp.bfloat16),
        in_specs=[pl.BlockSpec((None, tile, depth), lambda e, t: (e, t, 0)), weight_spec, weight_spec],
        out_specs=pl.BlockSpec((None, tile, ffn), lambda e, t: (e, t, 0)),
        compiler_params=pltpu.CompilerParams(vmem_limit_bytes=VMEM_LIMIT),
        cost_estimate=pl.CostEstimate(flops=12_000_000_000, bytes_accessed=30_000_000, transcendentals=0),
        name='expert_inner',
    )(tall, w_gate, w_up)


def back_kernel(capacity, inner_ref, comb_ref, down_ref, out_ref, wide_w, y_buf, send_core, got_core, acc, got_x, got_y, got_last, send_sems, core_sems, x_sems, y_sems, last_sems):
    place = layer_place()
    across_x, across_y, partner = related(place, 1, 0), related(place, 2, 0), related(place, 0, 1)
    greet([across_x, across_y, partner])
    sender = Sender(send_sems)
    n_exp, n_rows, ffn = inner_ref.shape
    parts, _, _, part_cols = down_ref.shape
    n_src = n_rows // capacity
    for p in range(parts):
        wide_w[:, :, p * part_cols:(p + 1) * part_cols] = down_ref[p]
    for e in range(n_exp):
        y_tall = jnp.dot(inner_ref[e], wide_w[e], preferred_element_type=jnp.float32).astype(jnp.bfloat16)
        for s in range(n_src):
            y_buf[s, e * capacity:(e + 1) * capacity, :] = y_tall[s * capacity:(s + 1) * capacity]
    half_cols = acc.shape[-1]

    def partial(chip_rel, core_rel, half):
        slot = slot_of(related(place, chip_rel, core_rel))
        cols = pl.ds(half * half_cols, half_cols)
        return jnp.dot(comb_ref[slot], y_buf[slot, :, cols], preferred_element_type=jnp.float32)

    order = (3, 1, 2, 0)
    for chip_rel in order:
        for half in (0, 1):
            send_core[chip_rel, half] = partial(chip_rel, 1, half)
            sender.send(send_core.at[chip_rel, half], got_core.at[chip_rel, half], core_sems.at[chip_rel, half], partner)
    for chip_rel in order:
        for half in (0, 1):
            mine = partial(chip_rel, 0, half)
            wait_in(got_core.at[chip_rel, half], core_sems.at[chip_rel, half])
            acc[chip_rel, half] = mine + got_core[chip_rel, half]
            if chip_rel & 1 and half == 0:
                where = 0 if chip_rel == 3 else 1
                sender.send(acc.at[chip_rel, 0], got_x.at[where], x_sems.at[where], across_x)
            if chip_rel & 2 and half == 1:
                where = 0 if chip_rel == 3 else 1
                sender.send(acc.at[chip_rel, 1], got_y.at[where], y_sems.at[where], across_y)
    wait_in(got_x.at[0], x_sems.at[0])
    acc[2, 0] += got_x[0]
    sender.send(acc.at[2, 0], got_last.at[0], last_sems.at[0], across_y)
    wait_in(got_y.at[0], y_sems.at[0])
    acc[1, 1] += got_y[0]
    sender.send(acc.at[1, 1], got_last.at[1], last_sems.at[1], across_x)
    wait_in(got_x.at[1], x_sems.at[1])
    wait_in(got_y.at[1], y_sems.at[1])
    wait_in(got_last.at[0], last_sems.at[0])
    out_ref[:, :half_cols] = acc[0, 0] + got_x[1] + got_last[0]
    wait_in(got_last.at[1], last_sems.at[1])
    out_ref[:, half_cols:] = acc[0, 1] + got_y[1] + got_last[1]
    sender.drain()


def expert_back(inner, comb, down, capacity, collective_id):
    n_exp, n_rows, ffn = inner.shape
    parts, _, _, part_cols = down.shape
    n_src, tokens, buf_rows = comb.shape
    cols = parts * part_cols
    half = (tokens, cols // 2)
    return pl.pallas_call(
        functools.partial(back_kernel, capacity),
        out_shape=jax.ShapeDtypeStruct((tokens, cols), jnp.float32),
        in_specs=[pl.BlockSpec(memory_space=pltpu.VMEM)] * 3,
        out_specs=pl.BlockSpec(memory_space=pltpu.VMEM),
        scratch_shapes=[
            pltpu.VMEM((n_exp, ffn, cols), jnp.bfloat16),
            pltpu.VMEM((n_src, buf_rows, cols), jnp.bfloat16),
            pltpu.VMEM((4, 2) + half, jnp.float32),
            pltpu.VMEM((4, 2) + half, jnp.float32),
            pltpu.VMEM((4, 2) + half, jnp.float32),
            pltpu.VMEM((2,) + half, jnp.float32),
            pltpu.VMEM((2,) + half, jnp.float32),
            pltpu.VMEM((2,) + half, jnp.float32),
            pltpu.SemaphoreType.DMA((14,)),
            pltpu.SemaphoreType.DMA((4, 2)),
            pltpu.SemaphoreType.DMA((2,)),
            pltpu.SemaphoreType.DMA((2,)),
            pltpu.SemaphoreType.DMA((2,)),
        ],
        compiler_params=pltpu.CompilerParams(collective_id=collective_id, has_side_effects=True, vmem_limit_bytes=VMEM_LIMIT),
        cost_estimate=pl.CostEstimate(flops=30_000_000_000, bytes_accessed=30_000_000, transcendentals=0),
        name='expert_back',
    )(inner, comb, down)


def solution(mesh):
    tok_spec = P(('data', 'fsdp', 'ep'), None, None)

    def local_step(x_blk, idx_blk, slot_blk, gate_blk, attn_gain, qkv_shard, out_shard, moe_gain, gate_shard, up_shard, down_shard):
        batch_rows, seq_len, d_model = x_blk.shape
        tokens = batch_rows * seq_len
        top_k = idx_blk.shape[-1]
        here = gate_shard.shape[0] // 2
        experts = gate_shard.shape[0] * lax.axis_size('ep')
        capacity = capacity_of(tokens, top_k, experts)
        first = lax.axis_index('data') * here
        gate_half = lax.dynamic_slice_in_dim(gate_shard, first, here, 0)
        up_half = lax.dynamic_slice_in_dim(up_shard, first, here, 0)
        down_half = lax.dynamic_slice_in_dim(down_shard, first, here, 0)
        mid = down_half.shape[2] // 2
        w_gate = lax.all_gather(gate_half, 'fsdp')
        w_up = lax.all_gather(up_half, 'fsdp')
        w_down = [lax.all_gather(down_half[:, :, :mid], 'fsdp'), lax.all_gather(down_half[:, :, mid:], 'fsdp')]

        _, triple, heads, head_dim = qkv_shard.shape
        width = heads * head_dim
        flat_shard = jnp.concatenate([qkv_shard.reshape(-1, triple * width), out_shard.reshape(-1, d_model)], axis=1)
        flat = gather_attention_weights(flat_shard)
        w_qkv = flat[:, :triple * width].reshape(d_model, triple, heads, head_dim)
        w_out = flat[:, triple * width:].reshape(heads, head_dim, d_model)
        hidden = attention_block(x_blk, attn_gain, w_qkv, w_out)
        normed = rms_norm(hidden, moe_gain).reshape(tokens, d_model)

        idx_t = idx_blk.reshape(tokens, top_k).T[:, None, :]
        slot_t = slot_blk.reshape(tokens, top_k).T[:, None, :].astype(jnp.float32)
        gate_t = gate_blk.reshape(tokens, top_k).T[:, None, :].astype(jnp.float32)
        hits = idx_t == jnp.arange(experts, dtype=jnp.int32)[None, :, None]
        slot_tab = jnp.sum(jnp.where(hits, slot_t + 1.0, 0.0), axis=0) - 1.0
        gate_tab = jnp.sum(jnp.where(hits, gate_t, 0.0), axis=0)
        tables = jnp.concatenate([slot_tab, gate_tab], axis=1).astype(jnp.bfloat16)
        gathered = gather_tokens(jnp.concatenate([normed, tables], axis=0))
        my_first = lax.axis_index('ep') * gate_shard.shape[0] + first
        my_tables = lax.dynamic_slice_in_dim(gathered[:, tokens:], my_first, here, 1).astype(jnp.float32)
        slot_row = my_tables[:, :, :tokens]
        slot_col = slot_row.transpose(0, 2, 1)
        gate_col = my_tables[:, :, tokens:].transpose(0, 2, 1)
        rows, comb = dispatch(gathered, slot_row, slot_col, gate_col, tokens, capacity)

        inner = expert_inner(rows, w_gate, w_up)
        sums = [expert_back(inner, comb, w_down[i], capacity, 3 + i) for i in range(2)]
        parts = w_down[0].shape[0]
        moe_sum = jnp.stack([part.reshape(tokens, parts, mid) for part in sums], axis=2).reshape(tokens, d_model)
        result = hidden.reshape(tokens, d_model).astype(jnp.float32) + moe_sum
        return result.astype(jnp.bfloat16).reshape(batch_rows, seq_len, d_model)

    return jax.shard_map(local_step, mesh=mesh, in_specs=(tok_spec, tok_spec, tok_spec, tok_spec, P(None), P('fsdp', None, None, None), P('fsdp', None, None), P(None), P('ep', 'fsdp', None), P('ep', 'fsdp', None), P('ep', None, 'fsdp')), out_specs=tok_spec, check_vma=False)
```

```python
import functools

import jax
import jax.numpy as jnp
from jax import lax
from jax.experimental import pallas as pl
from jax.experimental.pallas import tpu as pltpu
from jax.sharding import PartitionSpec as P

NORM_EPS = 1e-6
ROPE_BASE = 10000.0
MESH_ID = pl.DeviceIdType.MESH
VMEM_LIMIT = 60 * 1024 * 1024


def rms_norm(hidden, gain_vec):
    wide = hidden.astype(jnp.float32)
    inv_rms = lax.rsqrt(jnp.mean(wide * wide, axis=-1, keepdims=True) + NORM_EPS)
    return (wide * inv_rms * gain_vec.astype(jnp.float32)).astype(jnp.bfloat16)


def attention_block(x_blk, attn_gain, w_qkv, w_out):
    seq_len = x_blk.shape[1]
    head_dim = w_qkv.shape[3]
    half_dim = head_dim // 2
    normed = rms_norm(x_blk, attn_gain)
    qkv_proj = jnp.einsum('bsd,dthe->bsthe', normed, w_qkv, preferred_element_type=jnp.float32)
    inv_freq = ROPE_BASE ** (-jnp.arange(half_dim, dtype=jnp.float32) / half_dim)
    angles = jnp.arange(seq_len, dtype=jnp.float32)[:, None] * inv_freq[None, :]
    cos_tab = jnp.cos(angles)[None, :, None, :]
    sin_tab = jnp.sin(angles)[None, :, None, :]

    def rotate(heads_in):
        first_half = heads_in[..., :half_dim]
        second_half = heads_in[..., half_dim:]
        return jnp.concatenate([first_half * cos_tab - second_half * sin_tab, second_half * cos_tab + first_half * sin_tab], axis=-1)

    query_rot = rotate(qkv_proj[:, :, 0]).astype(jnp.bfloat16)
    keys_rot = rotate(qkv_proj[:, :, 1]).astype(jnp.bfloat16)
    values = qkv_proj[:, :, 2].astype(jnp.bfloat16)
    scores = jnp.einsum('bqhe,bkhe->bhqk', query_rot, keys_rot, preferred_element_type=jnp.float32) * (head_dim ** -0.5)
    causal = jnp.arange(seq_len)[:, None] >= jnp.arange(seq_len)[None, :]
    attn_probs = jax.nn.softmax(jnp.where(causal, scores, -1e30), axis=-1).astype(jnp.bfloat16)
    context = jnp.einsum('bhqk,bkhe->bqhe', attn_probs, values, preferred_element_type=jnp.float32).astype(jnp.bfloat16)
    attn_out = jnp.einsum('crif,ife->cre', context, w_out, preferred_element_type=jnp.float32)
    return (x_blk.astype(jnp.float32) + attn_out).astype(jnp.bfloat16)


def capacity_of(tok_count, top_k, experts):
    return 8 * ((5 * tok_count * top_k) // (32 * experts) + 1)


def layer_place():
    dx, dz, ep = lax.axis_index('data'), lax.axis_index('fsdp'), lax.axis_index('ep')
    return dx, dz, ep // 2, ep % 2


def flip(pos, bit):
    return (1 - pos) if bit else pos


def related(place, chip_rel, core_rel):
    dx, dz, dy, dc = place
    return flip(dx, chip_rel & 1), dz, flip(dy, chip_rel & 2), flip(dc, core_rel)


def slot_of(place):
    dx, _, dy, dc = place
    return dx * 4 + dy * 2 + dc


def dev_id(place):
    dx, dz, dy, dc = place
    return (dx, dz, dy * 2 + dc)


def greet(places):
    barrier = pltpu.get_barrier_semaphore()
    for place in places:
        pl.semaphore_signal(barrier, inc=1, device_id=dev_id(place), device_id_type=MESH_ID)
    pl.semaphore_wait(barrier, len(places))


class Sender:
    def __init__(self, send_sems):
        self.send_sems = send_sems
        self.copies = []

    def send(self, src, dst, recv_sem, place):
        copy = pltpu.make_async_remote_copy(src_ref=src, dst_ref=dst, send_sem=self.send_sems.at[len(self.copies)], recv_sem=recv_sem, device_id=dev_id(place), device_id_type=MESH_ID)
        copy.start()
        self.copies.append(copy)
        return copy

    def drain(self):
        for copy in self.copies:
            copy.wait_send()


def wait_in(ref, sem):
    pltpu.make_async_copy(ref, ref, sem).wait()


def spread_in_layer(place, sender, own_src, part_ref, recv_sems):
    across_x, across_y, partner = related(place, 1, 0), related(place, 2, 0), related(place, 0, 1)
    mine = slot_of(place)

    def pass_on(chip_rel, half, target, rel_there, core_there, first=False):
        owner = slot_of(related(place, chip_rel, 0))
        src = own_src(half) if first else part_ref(owner, half)
        sender.send(src, part_ref(owner, half), recv_sems(rel_there, core_there, half), target)

    for half in (0, 1):
        pass_on(0, half, across_x, 1, 0, True)
        pass_on(0, 1 - half, across_y, 2, 0, True)
    for half in (0, 1):
        pass_on(0, half, partner, 0, 1, True)
    yield

    def arrived(chip_rel, core_rel, half):
        owner = slot_of(related(place, chip_rel, core_rel))
        wait_in(part_ref(owner, half), recv_sems(chip_rel, core_rel, half))

    arrived(1, 0, 0)
    pass_on(1, 0, across_y, 3, 0)
    pass_on(1, 0, partner, 1, 1)
    arrived(2, 0, 1)
    pass_on(2, 1, across_x, 3, 0)
    pass_on(2, 1, partner, 2, 1)
    yield
    arrived(1, 0, 1)
    pass_on(1, 1, partner, 1, 1)
    arrived(2, 0, 0)
    pass_on(2, 0, partner, 2, 1)
    yield
    arrived(3, 0, 0)
    pass_on(3, 0, partner, 3, 1)
    arrived(3, 0, 1)
    pass_on(3, 1, partner, 3, 1)
    yield
    for chip_rel in range(4):
        for half in (0, 1):
            arrived(chip_rel, 1, half)
    yield


def attn_gather_kernel(shard_ref, out_ref, send_sems, z_sems, recv_sems, own_sem):
    place = layer_place()
    dx, dz, dy, dc = place
    rows = shard_ref.shape[0]
    piece = rows // 8
    z_peers = [(dx, (dz + step) % 4, dy, dc) for step in (1, 2, 3)]
    layer_peers = [related(place, 1, 0), related(place, 2, 0), related(place, 0, 1)]
    greet(z_peers + layer_peers)
    sender = Sender(send_sems)
    mine = slot_of(place)
    my_rows = pl.ds(pl.multiple_of(mine * piece, piece), piece)
    for index, step in enumerate((1, 3, 2)):
        target = (dx, (dz + step) % 4, dy, dc)
        dst = out_ref.at[pl.ds(pl.multiple_of(dz * rows + mine * piece, piece), piece)]
        sender.send(shard_ref.at[my_rows], dst, z_sems.at[index], target)
    own = pltpu.make_async_copy(shard_ref, out_ref.at[pl.ds(pl.multiple_of(dz * rows, rows), rows)], own_sem)
    own.start()
    streams = []
    for index, step in enumerate((1, 3, 2)):
        source_z = (dz + 4 - step) % 4

        def part_ref(slot, half, source_z=source_z):
            start = source_z * rows + slot * piece + half * (piece // 2)
            return out_ref.at[pl.ds(pl.multiple_of(start, piece // 2), piece // 2)]

        def recv_sem(chip_rel, core_rel, half, index=index):
            return recv_sems.at[index, chip_rel, core_rel, half]

        whole = out_ref.at[pl.ds(pl.multiple_of(source_z * rows + mine * piece, piece), piece)]
        streams.append((whole, index, spread_in_layer(place, sender, functools.partial(part_ref, mine), part_ref, recv_sem)))
    for whole, index, stream in streams:
        wait_in(whole, z_sems.at[index])
        next(stream)
    for _ in range(4):
        for _, _, stream in streams:
            next(stream)
    own.wait()
    sender.drain()


def gather_attention_weights(shard):
    rows, cols = shard.shape
    n_send = 3 + 3 * 14
    return pl.pallas_call(
        attn_gather_kernel,
        out_shape=jax.ShapeDtypeStruct((4 * rows, cols), shard.dtype),
        in_specs=[pl.BlockSpec(memory_space=pltpu.VMEM)],
        out_specs=pl.BlockSpec(memory_space=pl.ANY),
        scratch_shapes=[
            pltpu.SemaphoreType.DMA((n_send,)),
            pltpu.SemaphoreType.DMA((3,)),
            pltpu.SemaphoreType.DMA((3, 4, 2, 2)),
            pltpu.SemaphoreType.DMA,
        ],
        compiler_params=pltpu.CompilerParams(collective_id=1, has_side_effects=True, vmem_limit_bytes=VMEM_LIMIT),
        cost_estimate=pl.CostEstimate(flops=30_000_000_000, bytes_accessed=10_000_000, transcendentals=0),
        name='attn_gather',
    )(shard)


def token_gather_kernel(own_ref, out_ref, send_sems, recv_sems, own_sem):
    place = layer_place()
    greet([related(place, 1, 0), related(place, 2, 0), related(place, 0, 1)])
    sender = Sender(send_sems)
    half_rows = own_ref.shape[0] // 2

    def part_ref(slot, half):
        return out_ref.at[slot, pl.ds(half * half_rows, half_rows)]

    def own_half(half):
        return own_ref.at[pl.ds(half * half_rows, half_rows)]

    def recv_sem(chip_rel, core_rel, half):
        return recv_sems.at[chip_rel, core_rel, half]

    stream = spread_in_layer(place, sender, own_half, part_ref, recv_sem)
    next(stream)
    own = pltpu.make_async_copy(own_ref, out_ref.at[slot_of(place)], own_sem)
    own.start()
    for _ in range(4):
        next(stream)
    own.wait()
    sender.drain()


def gather_tokens(own):
    rows, cols = own.shape
    return pl.pallas_call(
        token_gather_kernel,
        out_shape=jax.ShapeDtypeStruct((8, rows, cols), own.dtype),
        in_specs=[pl.BlockSpec(memory_space=pltpu.VMEM)],
        out_specs=pl.BlockSpec(memory_space=pl.ANY),
        scratch_shapes=[
            pltpu.SemaphoreType.DMA((14,)),
            pltpu.SemaphoreType.DMA((4, 2, 2)),
            pltpu.SemaphoreType.DMA,
        ],
        compiler_params=pltpu.CompilerParams(collective_id=2, has_side_effects=True, vmem_limit_bytes=VMEM_LIMIT),
        cost_estimate=pl.CostEstimate(flops=30_000_000_000, bytes_accessed=10_000_000, transcendentals=0),
        name='token_gather',
    )(own)


def dispatch_kernel(pad_cap, n_exp, gathered_ref, rows_ref, comb_ref):
    tokens = comb_ref.shape[0]
    experts = gathered_ref.shape[0] - tokens
    first = (lax.axis_index('ep') * 2 + lax.axis_index('data')) * n_exp
    u = gathered_ref[:tokens]
    tables = gathered_ref[tokens:]
    pick_row = (lax.broadcasted_iota(jnp.int32, (8, experts), 1) == first + lax.broadcasted_iota(jnp.int32, (8, experts), 0)).astype(jnp.bfloat16)
    slot_row = jnp.dot(pick_row, tables, preferred_element_type=jnp.float32)
    pick_col = (lax.broadcasted_iota(jnp.int32, (experts, 128), 0) == first + lax.broadcasted_iota(jnp.int32, (experts, 128), 1)).astype(jnp.bfloat16)
    col_tab = lax.dot_general(tables, pick_col, (((0,), (0,)), ((), ())), preferred_element_type=jnp.float32)
    slot_ids = lax.broadcasted_iota(jnp.int32, (pad_cap, tokens), 0).astype(jnp.float32)
    for e in range(n_exp):
        one_hot = jnp.where(slot_ids == slot_row[e:e + 1, :tokens], 1.0, 0.0).astype(jnp.bfloat16)
        rows_ref[e] = jnp.dot(one_hot, u, preferred_element_type=jnp.float32).astype(jnp.bfloat16)
    buf_ids = lax.broadcasted_iota(jnp.int32, (tokens, n_exp * pad_cap), 1).astype(jnp.float32)
    comb = jnp.zeros((tokens, n_exp * pad_cap), jnp.float32)
    for e in range(n_exp):
        slot_e = col_tab[:tokens, e:e + 1]
        dest_e = jnp.where(slot_e >= 0.0, slot_e + float(e * pad_cap), -1.0)
        comb = jnp.where(buf_ids == dest_e, col_tab[tokens:, e:e + 1], comb)
    comb_ref[...] = comb.astype(jnp.bfloat16)


def dispatch(gathered, tokens, pad_cap, n_exp):
    n_src, all_rows, cols = gathered.shape
    return pl.pallas_call(
        functools.partial(dispatch_kernel, pad_cap, n_exp),
        grid=(n_src,),
        out_shape=(
            jax.ShapeDtypeStruct((n_exp, n_src, pad_cap, cols), jnp.bfloat16),
            jax.ShapeDtypeStruct((n_src, tokens, n_exp * pad_cap), jnp.bfloat16),
        ),
        in_specs=[pl.BlockSpec((None, all_rows, cols), lambda s: (s, 0, 0))],
        out_specs=(
            pl.BlockSpec((n_exp, None, pad_cap, cols), lambda s: (0, s, 0, 0)),
            pl.BlockSpec((None, tokens, n_exp * pad_cap), lambda s: (s, 0, 0)),
        ),
        compiler_params=pltpu.CompilerParams(vmem_limit_bytes=VMEM_LIMIT),
        cost_estimate=pl.CostEstimate(flops=10_000_000_000, bytes_accessed=30_000_000, transcendentals=0),
        name='dispatch',
    )(gathered)


def toggled(pos, bit):
    return pos + bit - 2 * pos * bit


def moe_kernel(rows_hbm, gate_up_hbm, comb_hbm, down_ref, hidden_ref, out_ref,
               row_buf, gate_buf, up_buf, inner, comb, down_all, y_buf, send_core, acc, got_core, got_x, got_y, got_last,
               load_sems, comb_sem, z_own_sems, z_pass_sems, z_recv_sems,
               core_send, core_recv, x_send, x_recv, y_send, y_recv, last_send, last_recv):
    place = layer_place()
    dx, dz, dy, dc = place
    n_exp, n_rows, ffn = inner.shape
    n_src, tokens, _ = comb.shape
    pad_cap = n_rows // n_src
    half_cols = acc.shape[-1]
    block_cols = 2 * half_cols
    row_tile = n_rows // 4
    depth = row_buf.shape[-1]
    across_x, across_y, partner = related(place, 1, 0), related(place, 2, 0), related(place, 0, 1)
    upper = dz // 2
    inside = (dz == 1) | (dz == 2)
    at_end = (dz == 0) | (dz == 3)

    def at_z(z):
        return (dx, z, dy, dc)

    def remote(src, dst, send_sem, recv_sem, where):
        return pltpu.make_async_remote_copy(src_ref=src, dst_ref=dst, send_sem=send_sem, recv_sem=recv_sem, device_id=dev_id(where), device_id_type=MESH_ID)

    def load(e):
        slot = e % 2
        return [
            pltpu.make_async_copy(rows_hbm.at[e], row_buf.at[slot], load_sems.at[0, slot]),
            pltpu.make_async_copy(gate_up_hbm.at[:, 0, e], gate_buf.at[slot], load_sems.at[1, slot]),
            pltpu.make_async_copy(gate_up_hbm.at[:, 1, e], up_buf.at[slot], load_sems.at[2, slot]),
        ]

    for copy in load(0):
        copy.start()
    comb_copy = pltpu.make_async_copy(comb_hbm, comb, comb_sem)
    comb_copy.start()

    barrier = pltpu.get_barrier_semaphore()
    for target in (across_x, across_y, partner):
        pl.semaphore_signal(barrier, inc=1, device_id=dev_id(target), device_id_type=MESH_ID)

    @pl.when(dz > 0)
    def _():
        pl.semaphore_signal(barrier, inc=1, device_id=dev_id(at_z(dz - 1)), device_id_type=MESH_ID)

    @pl.when(dz < 3)
    def _():
        pl.semaphore_signal(barrier, inc=1, device_id=dev_id(at_z(dz + 1)), device_id_type=MESH_ID)

    @pl.when(inside)
    def _():
        pl.semaphore_wait(barrier, 5)

    @pl.when(at_end)
    def _():
        pl.semaphore_wait(barrier, 4)

    pair = n_exp // 2

    def piece(p, sub):
        return down_all.at[p, pl.ds(sub * pair, pair)]

    def own_copy(side, sub):
        target = dz - 1 if side == 0 else dz + 1
        return remote(down_ref.at[pl.ds(sub * pair, pair)], piece(dz, sub), z_own_sems.at[side, sub], z_recv_sems.at[dz, sub], at_z(target))

    def pass_copy(which, p, target, sub):
        return remote(piece(p, sub), piece(p, sub), z_pass_sems.at[which, sub], z_recv_sems.at[p, sub], at_z(target))

    for sub in (0, 1):
        @pl.when(dz > 0)
        def _():
            own_copy(0, sub).start()

        @pl.when(dz < 3)
        def _():
            own_copy(1, sub).start()

    down_all[dz] = down_ref[...]
    far, far_target = 3 * (2 - dz), 3 * (dz - 1)

    def pass_near(sub):
        @pl.when(inside)
        def _():
            wait_in(piece(dz - 1, sub), z_recv_sems.at[dz - 1, sub])
            pass_copy(0, dz - 1, dz + 1, sub).start()
            wait_in(piece(dz + 1, sub), z_recv_sems.at[dz + 1, sub])
            pass_copy(1, dz + 1, dz - 1, sub).start()

    def pass_far(sub):
        @pl.when(inside)
        def _():
            wait_in(piece(far, sub), z_recv_sems.at[far, sub])
            pass_copy(2, far, far_target, sub).start()

    for e in range(n_exp):
        if e + 1 < n_exp:
            for copy in load(e + 1):
                copy.start()
        for copy in load(e):
            copy.wait()
        slot = e % 2

        def tile_body(t, carry):
            at = pl.ds(pl.multiple_of(t * row_tile, row_tile), row_tile)
            rows = row_buf[slot, at]
            gate_act = jnp.dot(rows, gate_buf[slot].reshape(depth, ffn), preferred_element_type=jnp.float32)
            up_act = jnp.dot(rows, up_buf[slot].reshape(depth, ffn), preferred_element_type=jnp.float32)
            inner[e, at] = (gate_act * jax.nn.sigmoid(gate_act) * up_act).astype(jnp.bfloat16)
            return carry

        lax.fori_loop(0, 4, tile_body, 0)
    pass_near(0)
    comb_copy.wait()

    def block_of(i):
        if i == 0:
            return dz
        near_end = dz + upper * (3 - 2 * dz)
        low = i - near_end if i == 1 else i
        return low + upper * (3 - 2 * low)

    def rel_slot(rel, core_rel):
        return toggled(dx, rel % 2) * 4 + toggled(dy, rel // 2) * 2 + flip(dc, core_rel)

    def core_copy(i, rel):
        return remote(send_core.at[i % 2, rel], got_core.at[i, rel], core_send.at[i, rel], core_recv.at[i, rel], partner)

    def x_copy(i, rel):
        where = (3 - rel) // 2
        return remote(acc.at[i % 2, rel, 0], got_x.at[i, where], x_send.at[i, where], x_recv.at[i, where], across_x)

    def y_copy(i, rel):
        where = 3 - rel
        return remote(acc.at[i % 2, rel, 1], got_y.at[i, where], y_send.at[i, where], y_recv.at[i, where], across_y)

    def last_copy(i, which):
        rel, half, target = ((2, 0, across_y), (1, 1, across_x))[which]
        return remote(acc.at[i % 2, rel, half], got_last.at[i, which], last_send.at[i, which], last_recv.at[i, which], target)

    def start_block(i):
        p = block_of(i)
        if i:
            @pl.when(at_end)
            def _():
                for sub in (0, 1):
                    wait_in(piece(p, sub), z_recv_sems.at[p, sub])

        def y_body(e, carry):
            y_tall = jnp.dot(inner[e], down_all[p, e], preferred_element_type=jnp.float32).astype(jnp.bfloat16)
            at = pl.ds(pl.multiple_of(e * pad_cap, pad_cap), pad_cap)
            for s in range(n_src):
                y_buf[s, at] = y_tall[s * pad_cap:(s + 1) * pad_cap]
            return carry

        lax.fori_loop(0, n_exp, y_body, 0)

        def partial(rel, core_rel):
            slot = rel_slot(rel, core_rel)
            return jnp.dot(comb[slot], y_buf[slot], preferred_element_type=jnp.float32)

        def core_body(k, carry):
            rel = 3 - k
            send_core[i % 2, rel] = partial(rel, 1)
            core_copy(i, rel).start()
            return carry

        def own_body(k, carry):
            rel = 3 - k
            mine = partial(rel, 0)
            wait_in(got_core.at[i, rel], core_recv.at[i, rel])
            mine = mine + got_core[i, rel]
            acc[i % 2, rel, 0] = mine[:, :half_cols]
            acc[i % 2, rel, 1] = mine[:, half_cols:]

            @pl.when(rel % 2 == 1)
            def _():
                x_copy(i, rel).start()

            @pl.when(rel // 2 == 1)
            def _():
                y_copy(i, rel).start()

            return carry

        lax.fori_loop(0, 4, core_body, 0)
        lax.fori_loop(0, 4, own_body, 0)

    def turn_block(i):
        wait_in(got_x.at[i, 0], x_recv.at[i, 0])
        acc[i % 2, 2, 0] += got_x[i, 0]
        last_copy(i, 0).start()
        wait_in(got_y.at[i, 0], y_recv.at[i, 0])
        acc[i % 2, 1, 1] += got_y[i, 0]
        last_copy(i, 1).start()

    def end_block(i):
        p = block_of(i)
        for half, got, got_sems in ((0, got_x, x_recv), (1, got_y, y_recv)):
            wait_in(got.at[i, 1], got_sems.at[i, 1])
            wait_in(got_last.at[i, half], last_recv.at[i, half])
            cols = pl.ds(pl.multiple_of(p * block_cols + half * half_cols, half_cols), half_cols)
            total = acc[i % 2, 0, half] + got[i, 1] + got_last[i, half]
            out_ref[:, cols] = (hidden_ref[:, cols].astype(jnp.float32) + total).astype(jnp.bfloat16)
        for rel in range(4):
            core_copy(i, rel).wait_send()
        for rel in (3, 1):
            x_copy(i, rel).wait_send()
        for rel in (3, 2):
            y_copy(i, rel).wait_send()
        for which in (0, 1):
            last_copy(i, which).wait_send()

    start_block(0)
    pass_near(1)
    turn_block(0)
    start_block(1)
    end_block(0)
    pass_far(0)
    turn_block(1)
    start_block(2)
    pass_far(1)
    end_block(1)
    turn_block(2)
    start_block(3)
    end_block(2)
    turn_block(3)
    end_block(3)

    for sub in (0, 1):
        @pl.when(dz > 0)
        def _():
            own_copy(0, sub).wait_send()

        @pl.when(dz < 3)
        def _():
            own_copy(1, sub).wait_send()

        @pl.when(inside)
        def _():
            pass_copy(0, dz - 1, dz + 1, sub).wait_send()
            pass_copy(1, dz + 1, dz - 1, sub).wait_send()
            pass_copy(2, far, far_target, sub).wait_send()


def moe(rows, gate_up, comb, down_half, hidden, collective_id):
    n_exp, n_src, pad_cap, depth = rows.shape
    parts, _, _, part_depth, ffn = gate_up.shape
    _, tokens, buf_rows = comb.shape
    block_cols = down_half.shape[-1]
    half = block_cols // 2
    tall = rows.reshape(n_exp, n_src * pad_cap, depth)
    dma = pltpu.SemaphoreType.DMA
    return pl.pallas_call(
        moe_kernel,
        out_shape=jax.ShapeDtypeStruct(hidden.shape, jnp.bfloat16),
        in_specs=[pl.BlockSpec(memory_space=pl.ANY)] * 3 + [pl.BlockSpec(memory_space=pltpu.VMEM)] * 2,
        out_specs=pl.BlockSpec(memory_space=pltpu.VMEM),
        scratch_shapes=[
            pltpu.VMEM((2, n_src * pad_cap, depth), jnp.bfloat16),
            pltpu.VMEM((2, parts, part_depth, ffn), jnp.bfloat16),
            pltpu.VMEM((2, parts, part_depth, ffn), jnp.bfloat16),
            pltpu.VMEM((n_exp, n_src * pad_cap, ffn), jnp.bfloat16),
            pltpu.VMEM(comb.shape, jnp.bfloat16),
            pltpu.VMEM((parts,) + down_half.shape, jnp.bfloat16),
            pltpu.VMEM((n_src, buf_rows, block_cols), jnp.bfloat16),
            pltpu.VMEM((2, 4, tokens, block_cols), jnp.float32),
            pltpu.VMEM((2, 4, 2, tokens, half), jnp.float32),
            pltpu.VMEM((parts, 4, tokens, block_cols), jnp.float32),
            pltpu.VMEM((parts, 2, tokens, half), jnp.float32),
            pltpu.VMEM((parts, 2, tokens, half), jnp.float32),
            pltpu.VMEM((parts, 2, tokens, half), jnp.float32),
            dma((3, 2)), dma, dma((2, 2)), dma((3, 2)), dma((parts, 2)),
            dma((parts, 4)), dma((parts, 4)), dma((parts, 2)), dma((parts, 2)),
            dma((parts, 2)), dma((parts, 2)), dma((parts, 2)), dma((parts, 2)),
        ],
        compiler_params=pltpu.CompilerParams(collective_id=collective_id, has_side_effects=True, vmem_limit_bytes=62 * 1024 * 1024),
        cost_estimate=pl.CostEstimate(flops=30_000_000_000, bytes_accessed=30_000_000, transcendentals=0),
        name='moe',
    )(tall, gate_up, comb, down_half, hidden)


def solution(mesh):
    tok_spec = P(('data', 'fsdp', 'ep'), None, None)

    def local_step(x_blk, idx_blk, slot_blk, gate_blk, attn_gain, qkv_shard, out_shard, moe_gain, gate_shard, up_shard, down_shard):
        batch_rows, seq_len, d_model = x_blk.shape
        tokens = batch_rows * seq_len
        top_k = idx_blk.shape[-1]
        here = gate_shard.shape[0] // 2
        experts = gate_shard.shape[0] * lax.axis_size('ep')
        capacity = capacity_of(tokens, top_k, experts)
        first = lax.axis_index('data') * here
        gate_half = lax.dynamic_slice_in_dim(gate_shard, first, here, 0)
        up_half = lax.dynamic_slice_in_dim(up_shard, first, here, 0)
        down_half = lax.dynamic_slice_in_dim(down_shard, first, here, 0)
        gate_up = lax.all_gather(jnp.stack([gate_half, up_half]), 'fsdp')

        _, triple, heads, head_dim = qkv_shard.shape
        width = heads * head_dim
        flat_shard = jnp.concatenate([qkv_shard.reshape(-1, triple * width), out_shard.reshape(-1, d_model)], axis=1)
        flat = gather_attention_weights(flat_shard)
        w_qkv = flat[:, :triple * width].reshape(d_model, triple, heads, head_dim)
        w_out = flat[:, triple * width:].reshape(heads, head_dim, d_model)
        hidden = attention_block(x_blk, attn_gain, w_qkv, w_out)
        normed = rms_norm(hidden, moe_gain).reshape(tokens, d_model)

        idx_t = idx_blk.reshape(tokens, top_k).T[:, None, :]
        slot_t = slot_blk.reshape(tokens, top_k).T[:, None, :].astype(jnp.float32)
        gate_t = gate_blk.reshape(tokens, top_k).T[:, None, :].astype(jnp.float32)
        hits = idx_t == jnp.arange(experts, dtype=jnp.int32)[None, :, None]
        slot_tab = jnp.sum(jnp.where(hits, slot_t + 1.0, 0.0), axis=0) - 1.0
        gate_tab = jnp.sum(jnp.where(hits, gate_t, 0.0), axis=0)
        tables = jnp.concatenate([slot_tab, gate_tab], axis=1).astype(jnp.bfloat16)
        gathered = gather_tokens(jnp.concatenate([normed, tables], axis=0))
        pad_cap = 16 * ((capacity + 15) // 16)
        rows, comb = dispatch(gathered, tokens, pad_cap, here)
        result = moe(rows, gate_up, comb, down_half, hidden.reshape(tokens, d_model), 3)
        return result.reshape(batch_rows, seq_len, d_model)

    return jax.shard_map(local_step, mesh=mesh, in_specs=(tok_spec, tok_spec, tok_spec, tok_spec, P(None), P('fsdp', None, None, None), P('fsdp', None, None), P(None), P('ep', 'fsdp', None), P('ep', 'fsdp', None), P('ep', None, 'fsdp')), out_specs=tok_spec, check_vma=False)
```

```python
import functools

import jax
import jax.numpy as jnp
import numpy as np
from jax import lax
from jax.experimental import pallas as pl
from jax.experimental.pallas import tpu as pltpu
from jax.sharding import PartitionSpec as P

NORM_EPS = 1e-6
ROPE_BASE = 10000.0
MESH_ID = pl.DeviceIdType.MESH
LANES = 128


def capacity_of(tok_count, top_k, experts):
    return 8 * ((5 * tok_count * top_k) // (32 * experts) + 1)


def rope_tables(seq_len, head_dim):
    half = head_dim // 2
    lane = np.arange(LANES)
    inv_freq = ROPE_BASE ** (-(lane % half) / half)
    angles = np.arange(seq_len)[:, None] * inv_freq[None, :]
    sign = np.where(lane % head_dim < half, -1.0, 1.0)
    return np.cos(angles).astype(np.float32), (np.sin(angles) * sign).astype(np.float32)


def layer_place():
    dx, dz, ep = lax.axis_index('data'), lax.axis_index('fsdp'), lax.axis_index('ep')
    return dx, dz, ep // 2, ep % 2


def flip(pos, bit):
    return (1 - pos) if bit else pos


def toggled(pos, bit):
    return pos + bit - 2 * pos * bit


def related(place, chip_rel, core_rel):
    dx, dz, dy, dc = place
    return flip(dx, chip_rel & 1), dz, flip(dy, chip_rel & 2), flip(dc, core_rel)


def slot_of(place):
    dx, _, dy, dc = place
    return dx * 4 + dy * 2 + dc


def dev_id(place):
    dx, dz, dy, dc = place
    return (dx, dz, dy * 2 + dc)


def remote(src, dst, send_sem, recv_sem, where):
    return pltpu.make_async_remote_copy(src_ref=src, dst_ref=dst, send_sem=send_sem, recv_sem=recv_sem, device_id=dev_id(where), device_id_type=MESH_ID)


def wait_in(ref, sem):
    pltpu.make_async_copy(ref, ref, sem).wait()


class Sender:
    def __init__(self, send_sems):
        self.send_sems = send_sems
        self.copies = []

    def send(self, src, dst, recv_sem, place):
        copy = remote(src, dst, self.send_sems.at[len(self.copies)], recv_sem, place)
        copy.start()
        self.copies.append(copy)

    def drain(self):
        for copy in self.copies:
            copy.wait_send()


def spread_in_layer(place, sender, own_src, part_ref, recv_sems):
    across_x, across_y, partner = related(place, 1, 0), related(place, 2, 0), related(place, 0, 1)

    def pass_on(chip_rel, half, target, rel_there, core_there, first=False):
        owner = slot_of(related(place, chip_rel, 0))
        src = own_src(half) if first else part_ref(owner, half)
        sender.send(src, part_ref(owner, half), recv_sems(rel_there, core_there, half), target)

    for half in (0, 1):
        pass_on(0, half, across_x, 1, 0, True)
        pass_on(0, 1 - half, across_y, 2, 0, True)
    for half in (0, 1):
        pass_on(0, half, partner, 0, 1, True)
    yield

    def arrived(chip_rel, core_rel, half):
        owner = slot_of(related(place, chip_rel, core_rel))
        wait_in(part_ref(owner, half), recv_sems(chip_rel, core_rel, half))

    arrived(1, 0, 0)
    pass_on(1, 0, across_y, 3, 0)
    pass_on(1, 0, partner, 1, 1)
    arrived(2, 0, 1)
    pass_on(2, 1, across_x, 3, 0)
    pass_on(2, 1, partner, 2, 1)
    yield
    arrived(1, 0, 1)
    pass_on(1, 1, partner, 1, 1)
    arrived(2, 0, 0)
    pass_on(2, 0, partner, 2, 1)
    yield
    arrived(3, 0, 0)
    pass_on(3, 0, partner, 3, 1)
    arrived(3, 0, 1)
    pass_on(3, 1, partner, 3, 1)
    yield
    for chip_rel in range(4):
        for half in (0, 1):
            arrived(chip_rel, 1, half)
    yield


def norm_rows(src, gain_ref, dst, rows):
    tile = 128

    def body(t, carry):
        at = pl.ds(pl.multiple_of(t * tile, tile), tile)
        wide = src[at].astype(jnp.float32)
        inv_rms = lax.rsqrt(jnp.mean(wide * wide, axis=-1, keepdims=True) + NORM_EPS)
        dst[at] = (wide * inv_rms * gain_ref[...]).astype(jnp.bfloat16)
        return carry

    lax.fori_loop(0, rows // tile, body, 0)


def attend(x_ref, normed, weights, cos_ref, sin_ref, qkv, hidden, head_dim):
    tokens, d_model = x_ref.shape
    lane = lax.broadcasted_iota(jnp.int32, (tokens, LANES), 1)
    low_half = lane % head_dim < head_dim // 2
    first_head = lax.broadcasted_iota(jnp.int32, (tokens // 2, LANES), 1) < head_dim
    group = 2 * LANES
    q_tile = tokens // 2
    scale = head_dim ** -0.5

    def rotate(val):
        swapped = jnp.where(low_half, pltpu.roll(val, LANES - head_dim // 2, 1), pltpu.roll(val, head_dim // 2, 1))
        return (val * cos_ref[...] + swapped * sin_ref[...]).astype(jnp.bfloat16)

    def project(b, cols):
        return jnp.dot(normed[:tokens], weights[b, :d_model, cols], preferred_element_type=jnp.float32)

    def group_body(g, carry):
        cols = pl.ds(pl.multiple_of(g * group, group), group)
        query, keys = project(0, cols), project(1, cols)
        values = project(2, cols).astype(jnp.bfloat16)
        for pair in (0, 1):
            at = slice(pair * LANES, (pair + 1) * LANES)
            qkv[0, :tokens, at] = rotate(query[:, at])
            qkv[1, :tokens, at] = rotate(keys[:, at])
            qkv[2, :tokens, at] = values[:, at]
        for pair in (0, 1):
            at = slice(pair * LANES, (pair + 1) * LANES)
            for tile in (0, 1):
                n_keys = (tile + 1) * q_tile
                q_pair = qkv[0, tile * q_tile:(tile + 1) * q_tile, at]
                k_pair, v_pair = qkv[1, :n_keys, at], qkv[2, :n_keys, at]
                row_id = lax.broadcasted_iota(jnp.int32, (q_tile, n_keys), 0) + tile * q_tile
                causal = row_id >= lax.broadcasted_iota(jnp.int32, (q_tile, n_keys), 1)
                outs = []
                for head in (0, 1):
                    q_head = jnp.where(first_head if head == 0 else ~first_head, q_pair, jnp.zeros((), jnp.bfloat16))
                    scores = lax.dot_general(q_head, k_pair, (((1,), (1,)), ((), ())), preferred_element_type=jnp.float32)
                    scores = jnp.where(causal, scores * scale, -1e30)
                    top = jnp.max(scores, axis=-1, keepdims=True)
                    weight = jnp.exp(scores - top)
                    probs = (weight * (1.0 / jnp.sum(weight, axis=-1, keepdims=True))).astype(jnp.bfloat16)
                    outs.append(jnp.dot(probs, v_pair, preferred_element_type=jnp.float32))
                out_cols = pl.ds(pl.multiple_of(g * group + pair * LANES, LANES), LANES)
                qkv[3, tile * q_tile:(tile + 1) * q_tile, out_cols] = jnp.where(first_head, outs[0], outs[1]).astype(jnp.bfloat16)
        return carry

    lax.fori_loop(0, d_model // group, group_body, 0)

    def out_body(g, carry):
        cols = pl.ds(pl.multiple_of(g * group, group), group)
        attn_out = jnp.dot(qkv[3, :tokens], weights[3, :d_model, cols], preferred_element_type=jnp.float32)
        hidden[:, cols] = (x_ref[:, cols].astype(jnp.float32) + attn_out).astype(jnp.bfloat16)
        return carry

    lax.fori_loop(0, d_model // group, out_body, 0)


def layer_kernel(head_dim, pad_cap,
                 x_ref, idx_ref, slot_ref, gate_ref, attn_gain_ref, moe_gain_ref, cos_ref, sin_ref,
                 qkv_hbm, proj_hbm, gate_hbm, up_hbm, down_hbm,
                 out_ref, tok_hbm,
                 big, gate_up, down_all, work, own_tok, hidden, inner, comb, y_buf, send_core, acc, got_core, got_x, got_y, got_last,
                 attn_send, attn_z_send, attn_z_recv, attn_recv, load_sems, tok_send, tok_recv, tok_sem, tok_load,
                 z_own, z_pass, z_recv, core_send, core_recv, x_send, x_recv, y_send, y_recv, last_send, last_recv):
    place = layer_place()
    dx, dz, dy, dc = place
    tokens, d_model = x_ref.shape
    experts = own_tok.shape[0] - tokens
    n_exp, n_rows, ffn = inner.shape
    n_src = comb.shape[0]
    block_cols = acc.shape[-1]
    half_tok = tokens // 2
    n_sub = down_all.shape[1]
    chunks = n_exp + n_sub
    across_x, across_y, partner = related(place, 1, 0), related(place, 2, 0), related(place, 0, 1)
    upper = dz // 2
    inside = (dz == 1) | (dz == 2)
    at_end = (dz == 0) | (dz == 3)
    first_exp = dx * n_exp
    mine = slot_of(place)

    def at_z(z):
        return (dx, z, dy, dc)

    barrier = pltpu.get_barrier_semaphore()
    for target in [at_z((dz + step) % 4) for step in (1, 2, 3)] + [across_x, across_y, partner]:
        pl.semaphore_signal(barrier, inc=1, device_id=dev_id(target), device_id_type=MESH_ID)
    pl.semaphore_wait(barrier, 6)

    shard_rows = qkv_hbm.shape[0]
    piece = shard_rows // 8

    def attn_src(b, rows):
        return proj_hbm.at[rows] if b == 3 else qkv_hbm.at[rows, pl.ds(b * d_model, d_model)]

    my_rows = pl.ds(pl.multiple_of(mine * piece, piece), piece)
    landing = pl.ds(pl.multiple_of(dz * shard_rows + mine * piece, piece), piece)
    z_copies = []
    for index, step in enumerate((1, 3, 2)):
        for b in range(4):
            copy = remote(attn_src(b, my_rows), big.at[b, landing], attn_z_send.at[index, b], attn_z_recv.at[index, b], at_z((dz + step) % 4))
            copy.start()
            z_copies.append(copy)

    def chunk_refs(p, j):
        if j < n_exp:
            return [gate_up.at[p, j, m] for m in (0, 1)]
        return [down_all.at[p, j - n_exp]]

    def chunk_srcs(j):
        if j < n_exp:
            return [gate_hbm.at[first_exp + j], up_hbm.at[first_exp + j]]
        return [down_hbm.at[pl.ds(first_exp, n_exp), :, pl.ds((j - n_exp) * block_cols, block_cols)]]

    def own_copies(side, j):
        target = at_z(dz - 1 if side == 0 else dz + 1)
        return [remote(src, dst, z_own.at[side, j, m], z_recv.at[dz, j, m], target) for m, (src, dst) in enumerate(zip(chunk_srcs(j), chunk_refs(dz, j)))]

    def pass_copies(which, p, j, z):
        return [remote(ref, ref, z_pass.at[which, j, m], z_recv.at[p, j, m], at_z(z)) for m, ref in enumerate(chunk_refs(p, j))]

    def wait_chunk(p, j):
        for m, ref in enumerate(chunk_refs(p, j)):
            wait_in(ref, z_recv.at[p, j, m])

    end_z, mid_z, far_z = 3 * (dz - 1), 3 - dz, 3 * (2 - dz)
    passes = ((end_z, mid_z), (mid_z, end_z), (far_z, end_z))

    def send_own(j):
        if j >= chunks:
            return

        @pl.when(dz > 0)
        def _():
            for copy in own_copies(0, j):
                copy.start()

        @pl.when(dz < 3)
        def _():
            for copy in own_copies(1, j):
                copy.start()

    def serve(j):
        @pl.when(inside)
        def _():
            for which, (p, z) in enumerate(passes):
                wait_chunk(p, j)
                for copy in pass_copies(which, p, j, z):
                    copy.start()
        send_own(j + 2)

    def need(j):
        @pl.when(at_end)
        def _():
            for k in range(3):
                wait_chunk(k + 1 - upper, j)

    send_own(0)
    send_own(1)
    own_loads = []
    for b in range(4):
        rows = pl.ds(pl.multiple_of(dz * shard_rows, shard_rows), shard_rows)
        own_loads.append(pltpu.make_async_copy(attn_src(b, pl.ds(0, shard_rows)), big.at[b, rows], load_sems.at[b]))
    for j in range(chunks):
        for m, (src, dst) in enumerate(zip(chunk_srcs(j), chunk_refs(dz, j))):
            own_loads.append(pltpu.make_async_copy(src, dst, load_sems.at[4 + 2 * j + m]))
    for copy in own_loads:
        copy.start()

    norm_rows(x_ref, attn_gain_ref, own_tok, tokens)

    expert_ids = lax.broadcasted_iota(jnp.int32, (experts, tokens), 0)
    slot_tab = jnp.zeros((experts, tokens), jnp.float32)
    gate_tab = jnp.zeros((experts, tokens), jnp.float32)
    for k in range(idx_ref.shape[0]):
        hit = expert_ids == idx_ref[k:k + 1, :]
        slot_tab = slot_tab + jnp.where(hit, slot_ref[k:k + 1, :].astype(jnp.float32) + 1.0, 0.0)
        gate_tab = gate_tab + jnp.where(hit, gate_ref[k:k + 1, :].astype(jnp.float32), 0.0)
    own_tok[tokens:, :tokens] = (slot_tab - 1.0).astype(jnp.bfloat16)
    own_tok[tokens:, tokens:] = gate_tab.astype(jnp.bfloat16)

    sender = Sender(attn_send)
    streams = []
    for index, step in enumerate((1, 3, 2)):
        source_z = (dz + 4 - step) % 4

        def part_ref(slot, half, source_z=source_z):
            start = source_z * shard_rows + slot * piece + half * (piece // 2)
            return big.at[:, pl.ds(pl.multiple_of(start, piece // 2), piece // 2)]

        def recv_sem(chip_rel, core_rel, half, index=index):
            return attn_recv.at[index, chip_rel, core_rel, half]

        arrival = pl.ds(pl.multiple_of(source_z * shard_rows + mine * piece, piece), piece)
        streams.append((arrival, index, spread_in_layer(place, sender, functools.partial(part_ref, mine), part_ref, recv_sem)))
    for arrival, index, stream in streams:
        for b in range(4):
            wait_in(big.at[b, arrival], attn_z_recv.at[index, b])
        next(stream)
    for _ in range(4):
        for _, _, stream in streams:
            next(stream)
    serve(0)
    for copy in own_loads:
        copy.wait()

    attend(x_ref, own_tok, big, cos_ref, sin_ref, work, hidden, head_dim)
    norm_rows(hidden, moe_gain_ref, own_tok, tokens)
    sender.drain()
    for copy in z_copies:
        copy.wait_send()

    tok_sender = Sender(tok_send)
    half_rows = own_tok.shape[0] // 2

    def tok_part(slot, half):
        return tok_hbm.at[slot, pl.ds(half * half_rows, half_rows)]

    def tok_half(half):
        return own_tok.at[pl.ds(half * half_rows, half_rows)]

    stream = spread_in_layer(place, tok_sender, tok_half, tok_part, lambda chip_rel, core_rel, half: tok_recv.at[chip_rel, core_rel, half])
    next(stream)
    tok_copy = pltpu.make_async_copy(own_tok, tok_hbm.at[mine], tok_sem)
    tok_copy.start()
    serve(1)
    for _ in range(4):
        next(stream)
    tok_copy.wait()
    tok_sender.drain()
    serve(2)

    def tok_in(s):
        return pltpu.make_async_copy(tok_hbm.at[s], work.at[s % 2], tok_load.at[s % 2])

    my_first = (lax.axis_index('ep') * 2 + dx) * n_exp
    pick_row = (lax.broadcasted_iota(jnp.int32, (8, experts), 1) == my_first + lax.broadcasted_iota(jnp.int32, (8, experts), 0)).astype(jnp.bfloat16)
    pick_col = (lax.broadcasted_iota(jnp.int32, (experts, LANES), 0) == my_first + lax.broadcasted_iota(jnp.int32, (experts, LANES), 1)).astype(jnp.bfloat16)
    tok_in(0).start()

    def dispatch_body(s, carry):
        @pl.when(s + 1 < n_src)
        def _():
            tok_in(s + 1).start()

        tok_in(s).wait()
        u = work[s % 2, :tokens]
        tables = work[s % 2, tokens:]
        slot_row = jnp.dot(pick_row, tables, preferred_element_type=jnp.float32)
        col_tab = lax.dot_general(tables, pick_col, (((0,), (0,)), ((), ())), preferred_element_type=jnp.float32)
        slot_ids = lax.broadcasted_iota(jnp.int32, (pad_cap, tokens), 0).astype(jnp.float32)
        rows = pl.ds(pl.multiple_of(s * pad_cap, pad_cap), pad_cap)
        for e in range(n_exp):
            one_hot = jnp.where(slot_ids == slot_row[e:e + 1, :tokens], 1.0, 0.0).astype(jnp.bfloat16)
            big[e, rows] = jnp.dot(one_hot, u, preferred_element_type=jnp.float32).astype(jnp.bfloat16)
        buf_ids = lax.broadcasted_iota(jnp.int32, (tokens, n_exp * pad_cap), 1).astype(jnp.float32)
        gates = jnp.zeros((tokens, n_exp * pad_cap), jnp.float32)
        for e in range(n_exp):
            slot_e = col_tab[:tokens, e:e + 1]
            dest_e = jnp.where(slot_e >= 0.0, slot_e + float(e * pad_cap), -1.0)
            gates = jnp.where(buf_ids == dest_e, col_tab[tokens:, e:e + 1], gates)
        comb[s] = gates.astype(jnp.bfloat16)
        return carry

    lax.fori_loop(0, n_src, dispatch_body, 0)
    serve(3)

    row_tile = n_rows // 4

    def expert_inner(e):
        need(e)

        def tile_body(t, carry):
            at = pl.ds(pl.multiple_of(t * row_tile, row_tile), row_tile)
            rows = big[e, at]
            gate_act = jnp.dot(rows, gate_up[:, e, 0].reshape(d_model, ffn), preferred_element_type=jnp.float32)
            up_act = jnp.dot(rows, gate_up[:, e, 1].reshape(d_model, ffn), preferred_element_type=jnp.float32)
            inner[e, at] = (gate_act * jax.nn.sigmoid(gate_act) * up_act).astype(jnp.bfloat16)
            return carry

        lax.fori_loop(0, 4, tile_body, 0)

    for e in range(n_exp - 1):
        expert_inner(e)
    serve(4)
    expert_inner(n_exp - 1)

    def block_of(i):
        if isinstance(i, int) and i < n_sub:
            return dz, i
        k, sub = (i - n_sub) % 3 + 1, (i - n_sub) // 3
        near_end = dz + upper * (3 - 2 * dz)
        low = k - near_end * ((3 - k) // 2)
        return low + upper * (3 - 2 * low), sub

    def rel_slot(rel, core_rel):
        return toggled(dx, rel % 2) * 4 + toggled(dy, rel // 2) * 2 + flip(dc, core_rel)

    halves = (pl.ds(0, half_tok), pl.ds(half_tok, half_tok))

    def core_copy(i, rel):
        return remote(send_core.at[i % 2, rel], got_core.at[i % 2, rel], core_send.at[i, rel], core_recv.at[i, rel], partner)

    def x_copy(i, rel):
        where = (3 - rel) // 2
        return remote(acc.at[i % 2, rel, halves[0]], got_x.at[i % 3, where], x_send.at[i, where], x_recv.at[i, where], across_x)

    def y_copy(i, rel):
        where = 3 - rel
        return remote(acc.at[i % 2, rel, halves[1]], got_y.at[i % 3, where], y_send.at[i, where], y_recv.at[i, where], across_y)

    def last_copy(i, which):
        rel, target = ((2, across_y), (1, across_x))[which]
        return remote(acc.at[i % 2, rel, halves[which]], got_last.at[i % 3, which], last_send.at[i, which], last_recv.at[i, which], target)

    def start_block(i):
        p, sub = block_of(i)
        if not (isinstance(i, int) and i < n_sub):
            @pl.when(at_end)
            def _():
                wait_in(down_all.at[p, sub], z_recv.at[p, n_exp + sub, 0])

        def y_body(e, carry):
            y_tall = jnp.dot(inner[e], down_all[p, sub, e], preferred_element_type=jnp.float32).astype(jnp.bfloat16)
            at = pl.ds(pl.multiple_of(e * pad_cap, pad_cap), pad_cap)
            for s in range(n_src):
                y_buf[s, at] = y_tall[s * pad_cap:(s + 1) * pad_cap]
            return carry

        lax.fori_loop(0, n_exp, y_body, 0)

        def partial(rel, core_rel):
            slot = rel_slot(rel, core_rel)
            return jnp.dot(comb[slot], y_buf[slot], preferred_element_type=jnp.float32)

        def core_body(k, carry):
            rel = 3 - k
            send_core[i % 2, rel] = partial(rel, 1)
            core_copy(i, rel).start()
            return carry

        def own_body(k, carry):
            rel = 3 - k
            own = partial(rel, 0)
            wait_in(got_core.at[i % 2, rel], core_recv.at[i, rel])
            acc[i % 2, rel] = own + got_core[i % 2, rel]

            @pl.when(rel % 2 == 1)
            def _():
                x_copy(i, rel).start()

            @pl.when(rel // 2 == 1)
            def _():
                y_copy(i, rel).start()

            return carry

        lax.fori_loop(0, 4, core_body, 0)
        lax.fori_loop(0, 4, own_body, 0)

    def turn_block(i):
        wait_in(got_x.at[i % 3, 0], x_recv.at[i, 0])
        acc[i % 2, 2, halves[0]] += got_x[i % 3, 0]
        last_copy(i, 0).start()
        wait_in(got_y.at[i % 3, 0], y_recv.at[i, 0])
        acc[i % 2, 1, halves[1]] += got_y[i % 3, 0]
        last_copy(i, 1).start()

    def end_block(i):
        p, sub = block_of(i)
        cols = pl.ds(pl.multiple_of((p * n_sub + sub) * block_cols, block_cols), block_cols)
        for half, got, got_sems in ((0, got_x, x_recv), (1, got_y, y_recv)):
            wait_in(got.at[i % 3, 1], got_sems.at[i, 1])
            wait_in(got_last.at[i % 3, half], last_recv.at[i, half])
            total = acc[i % 2, 0, halves[half]] + got[i % 3, 1] + got_last[i % 3, half]
            out_ref[halves[half], cols] = (hidden[halves[half], cols].astype(jnp.float32) + total).astype(jnp.bfloat16)
        for rel in range(4):
            core_copy(i, rel).wait_send()
        for rel in (3, 1):
            x_copy(i, rel).wait_send()
        for rel in (3, 2):
            y_copy(i, rel).wait_send()
        for which in (0, 1):
            last_copy(i, which).wait_send()

    blocks = 4 * n_sub
    start_block(0)
    turn_block(0)
    start_block(1)
    serve(5)
    end_block(0)
    turn_block(1)
    start_block(2)
    end_block(1)

    def block_body(i, carry):
        turn_block(i)

        @pl.when(i + 1 < blocks)
        def _():
            start_block(i + 1)

        end_block(i)
        return carry

    lax.fori_loop(2, blocks, block_body, 0)

    for j in range(chunks):
        @pl.when(dz > 0)
        def _():
            for copy in own_copies(0, j):
                copy.wait_send()

        @pl.when(dz < 3)
        def _():
            for copy in own_copies(1, j):
                copy.wait_send()

        @pl.when(inside)
        def _():
            for which, (p, z) in enumerate(passes):
                for copy in pass_copies(which, p, j, z):
                    copy.wait_send()


def whole_layer(head_dim, pad_cap, x, idx_t, slot_t, gate_t, attn_gain, moe_gain, qkv, proj, gate_w, up_w, down_w, experts):
    tokens, d_model = x.shape
    n_exp = gate_w.shape[0] // 2
    part_depth, ffn = gate_w.shape[1:]
    parts, n_src, block_cols = 4, 8, LANES
    n_sub = down_w.shape[2] // block_cols
    blocks = parts * n_sub
    chunks = n_exp + n_sub
    n_rows = n_src * pad_cap
    half = tokens // 2
    cos_tab, sin_tab = rope_tables(tokens, head_dim)
    dma = pltpu.SemaphoreType.DMA
    bf16, f32 = jnp.bfloat16, jnp.float32
    vmem, hbm = pl.BlockSpec(memory_space=pltpu.VMEM), pl.BlockSpec(memory_space=pl.ANY)
    return pl.pallas_call(
        functools.partial(layer_kernel, head_dim, pad_cap),
        out_shape=(jax.ShapeDtypeStruct(x.shape, bf16), jax.ShapeDtypeStruct((n_src, tokens + experts, d_model), bf16)),
        in_specs=[vmem] * 8 + [hbm] * 5,
        out_specs=(vmem, hbm),
        scratch_shapes=[
            pltpu.VMEM((n_exp, n_rows, d_model), bf16),
            pltpu.VMEM((parts, n_exp, 2, part_depth, ffn), bf16),
            pltpu.VMEM((parts, n_sub, n_exp, ffn, block_cols), bf16),
            pltpu.VMEM((4, tokens + experts, d_model), bf16),
            pltpu.VMEM((tokens + experts, d_model), bf16),
            pltpu.VMEM((tokens, d_model), bf16),
            pltpu.VMEM((n_exp, n_rows, ffn), bf16),
            pltpu.VMEM((n_src, tokens, n_exp * pad_cap), bf16),
            pltpu.VMEM((n_src, n_exp * pad_cap, block_cols), bf16),
            pltpu.VMEM((2, 4, tokens, block_cols), f32),
            pltpu.VMEM((2, 4, tokens, block_cols), f32),
            pltpu.VMEM((2, 4, tokens, block_cols), f32),
            pltpu.VMEM((3, 2, half, block_cols), f32),
            pltpu.VMEM((3, 2, half, block_cols), f32),
            pltpu.VMEM((3, 2, half, block_cols), f32),
            dma((42,)), dma((3, 4)), dma((3, 4)), dma((3, 4, 2, 2)), dma((4 + 2 * chunks,)),
            dma((14,)), dma((4, 2, 2)), dma, dma((2,)),
            dma((2, chunks, 2)), dma((3, chunks, 2)), dma((parts, chunks, 2)),
            dma((blocks, 4)), dma((blocks, 4)), dma((blocks, 2)), dma((blocks, 2)),
            dma((blocks, 2)), dma((blocks, 2)), dma((blocks, 2)), dma((blocks, 2)),
        ],
        compiler_params=pltpu.CompilerParams(collective_id=1, has_side_effects=True, vmem_limit_bytes=63 * 1024 * 1024),
        cost_estimate=pl.CostEstimate(flops=40_000_000_000, bytes_accessed=30_000_000, transcendentals=0),
        name='whole_layer',
    )(x, idx_t, slot_t, gate_t, attn_gain, moe_gain, cos_tab, sin_tab, qkv, proj, gate_w, up_w, down_w)[0]


def solution(mesh):
    tok_spec = P(('data', 'fsdp', 'ep'), None, None)
    ep_count = mesh.shape['ep']

    def local_step(x_blk, idx_blk, slot_blk, gate_blk, attn_gain, qkv_shard, out_shard, moe_gain, gate_shard, up_shard, down_shard):
        batch_rows, seq_len, d_model = x_blk.shape
        tokens = batch_rows * seq_len
        top_k = idx_blk.shape[-1]
        head_dim = qkv_shard.shape[3]
        experts = gate_shard.shape[0] * ep_count
        capacity = capacity_of(tokens, top_k, experts)
        pad_cap = 16 * ((capacity + 15) // 16)
        by_choice = [blk.reshape(tokens, top_k).T for blk in (idx_blk, slot_blk, gate_blk)]
        gains = [gain.astype(jnp.float32)[None, :] for gain in (attn_gain, moe_gain)]
        qkv = qkv_shard.reshape(qkv_shard.shape[0], -1)
        proj = out_shard.reshape(-1, d_model)
        result = whole_layer(head_dim, pad_cap, x_blk.reshape(tokens, d_model), *by_choice, *gains, qkv, proj, gate_shard, up_shard, down_shard, experts)
        return result.reshape(batch_rows, seq_len, d_model)

    return jax.shard_map(local_step, mesh=mesh, in_specs=(tok_spec, tok_spec, tok_spec, tok_spec, P(None), P('fsdp', None, None, None), P('fsdp', None, None), P(None), P('ep', 'fsdp', None), P('ep', 'fsdp', None), P('ep', None, 'fsdp')), out_specs=tok_spec, check_vma=False)
```

```python
import functools

import jax
import jax.numpy as jnp
import numpy as np
from jax import lax
from jax.experimental import pallas as pl
from jax.experimental.pallas import tpu as pltpu
from jax.sharding import PartitionSpec as P

NORM_EPS = 1e-6
ROPE_BASE = 10000.0
MESH_ID = pl.DeviceIdType.MESH
LANES = 128


def capacity_of(tok_count, top_k, experts):
    return 8 * ((5 * tok_count * top_k) // (32 * experts) + 1)


def rope_tables(seq_len, head_dim):
    half = head_dim // 2
    lane = np.arange(LANES)
    inv_freq = ROPE_BASE ** (-(lane % half) / half)
    angles = np.arange(seq_len)[:, None] * inv_freq[None, :]
    sign = np.where(lane % head_dim < half, -1.0, 1.0)
    return np.cos(angles).astype(np.float32), (np.sin(angles) * sign).astype(np.float32)


def layer_place():
    dx, dz, ep = lax.axis_index('data'), lax.axis_index('fsdp'), lax.axis_index('ep')
    return dx, dz, ep // 2, ep % 2


def flip(pos, bit):
    return (1 - pos) if bit else pos


def toggled(pos, bit):
    return pos + bit - 2 * pos * bit


def related(place, chip_rel, core_rel):
    dx, dz, dy, dc = place
    return flip(dx, chip_rel & 1), dz, flip(dy, chip_rel & 2), flip(dc, core_rel)


def slot_of(place):
    dx, _, dy, dc = place
    return dx * 4 + dy * 2 + dc


def dev_id(place):
    dx, dz, dy, dc = place
    return (dx, dz, dy * 2 + dc)


def remote(src, dst, send_sem, recv_sem, where):
    return pltpu.make_async_remote_copy(src_ref=src, dst_ref=dst, send_sem=send_sem, recv_sem=recv_sem, device_id=dev_id(where), device_id_type=MESH_ID)


def wait_in(ref, sem):
    pltpu.make_async_copy(ref, ref, sem).wait()


class Sender:
    def __init__(self, send_sems):
        self.send_sems = send_sems
        self.copies = []

    def send(self, src, dst, recv_sem, place):
        copy = remote(src, dst, self.send_sems.at[len(self.copies)], recv_sem, place)
        copy.start()
        self.copies.append(copy)

    def drain(self):
        for copy in self.copies:
            copy.wait_send()


def spread_in_layer(place, sender, own_src, part_ref, recv_sems):
    across_x, across_y, partner = related(place, 1, 0), related(place, 2, 0), related(place, 0, 1)

    def pass_on(chip_rel, half, target, rel_there, core_there, first=False):
        owner = slot_of(related(place, chip_rel, 0))
        src = own_src(half) if first else part_ref(owner, half)
        sender.send(src, part_ref(owner, half), recv_sems(rel_there, core_there, half), target)

    for half in (0, 1):
        pass_on(0, half, across_x, 1, 0, True)
        pass_on(0, 1 - half, across_y, 2, 0, True)
    for half in (0, 1):
        pass_on(0, half, partner, 0, 1, True)
    yield

    def arrived(chip_rel, core_rel, half):
        owner = slot_of(related(place, chip_rel, core_rel))
        wait_in(part_ref(owner, half), recv_sems(chip_rel, core_rel, half))

    arrived(1, 0, 0)
    pass_on(1, 0, across_y, 3, 0)
    pass_on(1, 0, partner, 1, 1)
    arrived(2, 0, 1)
    pass_on(2, 1, across_x, 3, 0)
    pass_on(2, 1, partner, 2, 1)
    yield
    arrived(1, 0, 1)
    pass_on(1, 1, partner, 1, 1)
    arrived(2, 0, 0)
    pass_on(2, 0, partner, 2, 1)
    yield
    arrived(3, 0, 0)
    pass_on(3, 0, partner, 3, 1)
    arrived(3, 0, 1)
    pass_on(3, 1, partner, 3, 1)
    yield
    for chip_rel in range(4):
        for half in (0, 1):
            arrived(chip_rel, 1, half)
    yield


def norm_rows(src, gain_ref, dst, rows):
    tile = 128

    def body(t, carry):
        at = pl.ds(pl.multiple_of(t * tile, tile), tile)
        wide = src[at].astype(jnp.float32)
        inv_rms = lax.rsqrt(jnp.mean(wide * wide, axis=-1, keepdims=True) + NORM_EPS)
        dst[at] = (wide * inv_rms * gain_ref[...]).astype(jnp.bfloat16)
        return carry

    lax.fori_loop(0, rows // tile, body, 0)


def attend(x_ref, normed, weights, cos_ref, sin_ref, qkv, hidden, head_dim):
    tokens, d_model = x_ref.shape
    lane = lax.broadcasted_iota(jnp.int32, (tokens, LANES), 1)
    low_half = lane % head_dim < head_dim // 2
    first_head = lax.broadcasted_iota(jnp.int32, (tokens // 2, LANES), 1) < head_dim
    group = 2 * LANES
    q_tile = tokens // 2
    scale = head_dim ** -0.5

    def rotate(val):
        swapped = jnp.where(low_half, pltpu.roll(val, LANES - head_dim // 2, 1), pltpu.roll(val, head_dim // 2, 1))
        return (val * cos_ref[...] + swapped * sin_ref[...]).astype(jnp.bfloat16)

    def project(b, cols):
        return jnp.dot(normed[:tokens], weights[b, :d_model, cols], preferred_element_type=jnp.float32)

    def group_body(g, carry):
        cols = pl.ds(pl.multiple_of(g * group, group), group)
        query, keys = project(0, cols), project(1, cols)
        values = project(2, cols).astype(jnp.bfloat16)
        for pair in (0, 1):
            at = slice(pair * LANES, (pair + 1) * LANES)
            qkv[0, :tokens, at] = rotate(query[:, at])
            qkv[1, :tokens, at] = rotate(keys[:, at])
            qkv[2, :tokens, at] = values[:, at]
        for pair in (0, 1):
            at = slice(pair * LANES, (pair + 1) * LANES)
            for tile in (0, 1):
                n_keys = (tile + 1) * q_tile
                q_pair = qkv[0, tile * q_tile:(tile + 1) * q_tile, at]
                k_pair, v_pair = qkv[1, :n_keys, at], qkv[2, :n_keys, at]
                row_id = lax.broadcasted_iota(jnp.int32, (q_tile, n_keys), 0) + tile * q_tile
                causal = row_id >= lax.broadcasted_iota(jnp.int32, (q_tile, n_keys), 1)
                outs = []
                for head in (0, 1):
                    q_head = jnp.where(first_head if head == 0 else ~first_head, q_pair, jnp.zeros((), jnp.bfloat16))
                    scores = lax.dot_general(q_head, k_pair, (((1,), (1,)), ((), ())), preferred_element_type=jnp.float32)
                    scores = jnp.where(causal, scores * scale, -1e30)
                    top = jnp.max(scores, axis=-1, keepdims=True)
                    weight = jnp.exp(scores - top)
                    probs = (weight * (1.0 / jnp.sum(weight, axis=-1, keepdims=True))).astype(jnp.bfloat16)
                    outs.append(jnp.dot(probs, v_pair, preferred_element_type=jnp.float32))
                out_cols = pl.ds(pl.multiple_of(g * group + pair * LANES, LANES), LANES)
                qkv[3, tile * q_tile:(tile + 1) * q_tile, out_cols] = jnp.where(first_head, outs[0], outs[1]).astype(jnp.bfloat16)
        return carry

    lax.fori_loop(0, d_model // group, group_body, 0)

    def out_body(g, carry):
        cols = pl.ds(pl.multiple_of(g * group, group), group)
        attn_out = jnp.dot(qkv[3, :tokens], weights[3, :d_model, cols], preferred_element_type=jnp.float32)
        hidden[:, cols] = (x_ref[:, cols].astype(jnp.float32) + attn_out).astype(jnp.bfloat16)
        return carry

    lax.fori_loop(0, d_model // group, out_body, 0)


def layer_kernel(head_dim, pad_cap,
                 x_ref, idx_ref, slot_ref, gate_ref, attn_gain_ref, moe_gain_ref, cos_ref, sin_ref,
                 qkv_hbm, proj_hbm, gate_hbm, up_hbm, down_hbm,
                 out_ref, tok_hbm,
                 big, gate_up, down_all, work, own_tok, hidden, inner, comb, y_buf, send_core, acc, got_core, got_x, got_y, got_last,
                 attn_send, attn_z_send, attn_z_recv, attn_recv, load_sems, tok_send, tok_recv, tok_sem, tok_load,
                 z_own, z_pass, z_recv, core_send, core_recv, x_send, x_recv, y_send, y_recv, last_send, last_recv):
    place = layer_place()
    dx, dz, dy, dc = place
    tokens, d_model = x_ref.shape
    experts = own_tok.shape[0] - tokens
    n_exp, n_rows, ffn = inner.shape
    n_src = comb.shape[0]
    block_cols = acc.shape[-1]
    half_tok = tokens // 2
    n_sub = down_all.shape[1]
    chunks = n_exp + n_sub
    across_x, across_y, partner = related(place, 1, 0), related(place, 2, 0), related(place, 0, 1)
    upper = dz // 2
    inside = (dz == 1) | (dz == 2)
    at_end = (dz == 0) | (dz == 3)
    first_exp = dx * n_exp
    mine = slot_of(place)

    def at_z(z):
        return (dx, z, dy, dc)

    barrier = pltpu.get_barrier_semaphore()
    for target in [at_z((dz + step) % 4) for step in (1, 2, 3)] + [across_x, across_y, partner]:
        pl.semaphore_signal(barrier, inc=1, device_id=dev_id(target), device_id_type=MESH_ID)
    pl.semaphore_wait(barrier, 6)

    shard_rows = qkv_hbm.shape[0]
    piece = shard_rows // 8

    def attn_src(b, rows):
        return proj_hbm.at[rows] if b == 3 else qkv_hbm.at[rows, pl.ds(b * d_model, d_model)]

    my_rows = pl.ds(pl.multiple_of(mine * piece, piece), piece)
    landing = pl.ds(pl.multiple_of(dz * shard_rows + mine * piece, piece), piece)
    z_copies = []
    for index, step in enumerate((1, 3, 2)):
        for b in range(4):
            copy = remote(attn_src(b, my_rows), big.at[b, landing], attn_z_send.at[index, b], attn_z_recv.at[index, b], at_z((dz + step) % 4))
            copy.start()
            z_copies.append(copy)

    def chunk_refs(p, j):
        if j < n_exp:
            return [gate_up.at[p, j, m] for m in (0, 1)]
        return [down_all.at[p, j - n_exp]]

    def chunk_srcs(j):
        if j < n_exp:
            return [gate_hbm.at[first_exp + j], up_hbm.at[first_exp + j]]
        return [down_hbm.at[pl.ds(first_exp, n_exp), :, pl.ds((j - n_exp) * block_cols, block_cols)]]

    def own_copies(side, j):
        target = at_z(dz - 1 if side == 0 else dz + 1)
        return [remote(src, dst, z_own.at[side, j, m], z_recv.at[dz, j, m], target) for m, (src, dst) in enumerate(zip(chunk_srcs(j), chunk_refs(dz, j)))]

    def pass_copies(which, p, j, z):
        return [remote(ref, ref, z_pass.at[which, j, m], z_recv.at[p, j, m], at_z(z)) for m, ref in enumerate(chunk_refs(p, j))]

    def wait_chunk(p, j):
        for m, ref in enumerate(chunk_refs(p, j)):
            wait_in(ref, z_recv.at[p, j, m])

    end_z, mid_z, far_z = 3 * (dz - 1), 3 - dz, 3 * (2 - dz)
    passes = ((end_z, mid_z), (mid_z, end_z), (far_z, end_z))

    def send_own(j):
        @pl.when(dz > 0)
        def _():
            for copy in own_copies(0, j):
                copy.start()

        @pl.when(dz < 3)
        def _():
            for copy in own_copies(1, j):
                copy.start()

    def forward(kinds, js):
        @pl.when(inside)
        def _():
            for j in js:
                for which in kinds:
                    p, z = passes[which]
                    wait_chunk(p, j)
                    for copy in pass_copies(which, p, j, z):
                        copy.start()

    near, far, expert_js, down_js = (0, 1), (2,), range(n_exp), range(n_exp, chunks)

    def need(j):
        @pl.when(at_end)
        def _():
            for k in range(3):
                wait_chunk(k + 1 - upper, j)

    for j in expert_js:
        send_own(j)
    own_loads = []
    for b in range(4):
        rows = pl.ds(pl.multiple_of(dz * shard_rows, shard_rows), shard_rows)
        own_loads.append(pltpu.make_async_copy(attn_src(b, pl.ds(0, shard_rows)), big.at[b, rows], load_sems.at[b]))
    for j in range(chunks):
        for m, (src, dst) in enumerate(zip(chunk_srcs(j), chunk_refs(dz, j))):
            own_loads.append(pltpu.make_async_copy(src, dst, load_sems.at[4 + 2 * j + m]))
    for copy in own_loads:
        copy.start()

    norm_rows(x_ref, attn_gain_ref, own_tok, tokens)

    expert_ids = lax.broadcasted_iota(jnp.int32, (experts, tokens), 0)
    slot_tab = jnp.zeros((experts, tokens), jnp.float32)
    gate_tab = jnp.zeros((experts, tokens), jnp.float32)
    for k in range(idx_ref.shape[0]):
        hit = expert_ids == idx_ref[k:k + 1, :]
        slot_tab = slot_tab + jnp.where(hit, slot_ref[k:k + 1, :].astype(jnp.float32) + 1.0, 0.0)
        gate_tab = gate_tab + jnp.where(hit, gate_ref[k:k + 1, :].astype(jnp.float32), 0.0)
    own_tok[tokens:, :tokens] = (slot_tab - 1.0).astype(jnp.bfloat16)
    own_tok[tokens:, tokens:] = gate_tab.astype(jnp.bfloat16)

    sender = Sender(attn_send)
    streams = []
    for index, step in enumerate((1, 3, 2)):
        source_z = (dz + 4 - step) % 4

        def part_ref(slot, half, source_z=source_z):
            start = source_z * shard_rows + slot * piece + half * (piece // 2)
            return big.at[:, pl.ds(pl.multiple_of(start, piece // 2), piece // 2)]

        def recv_sem(chip_rel, core_rel, half, index=index):
            return attn_recv.at[index, chip_rel, core_rel, half]

        arrival = pl.ds(pl.multiple_of(source_z * shard_rows + mine * piece, piece), piece)
        streams.append((arrival, index, spread_in_layer(place, sender, functools.partial(part_ref, mine), part_ref, recv_sem)))
    for arrival, index, stream in streams:
        for b in range(4):
            wait_in(big.at[b, arrival], attn_z_recv.at[index, b])
        next(stream)
    for _ in range(4):
        for _, _, stream in streams:
            next(stream)
    for copy in own_loads:
        copy.wait()

    attend(x_ref, own_tok, big, cos_ref, sin_ref, work, hidden, head_dim)
    norm_rows(hidden, moe_gain_ref, own_tok, tokens)
    sender.drain()
    for copy in z_copies:
        copy.wait_send()

    tok_sender = Sender(tok_send)
    half_rows = own_tok.shape[0] // 2

    def tok_part(slot, half):
        return tok_hbm.at[slot, pl.ds(half * half_rows, half_rows)]

    def tok_half(half):
        return own_tok.at[pl.ds(half * half_rows, half_rows)]

    stream = spread_in_layer(place, tok_sender, tok_half, tok_part, lambda chip_rel, core_rel, half: tok_recv.at[chip_rel, core_rel, half])
    next(stream)
    tok_copy = pltpu.make_async_copy(own_tok, tok_hbm.at[mine], tok_sem)
    tok_copy.start()
    forward(near, expert_js)
    for _ in range(4):
        next(stream)
    tok_copy.wait()
    tok_sender.drain()
    forward(far, expert_js)
    for j in down_js:
        send_own(j)

    def tok_in(s):
        return pltpu.make_async_copy(tok_hbm.at[s], work.at[s % 2], tok_load.at[s % 2])

    my_first = (lax.axis_index('ep') * 2 + dx) * n_exp
    pick_row = (lax.broadcasted_iota(jnp.int32, (8, experts), 1) == my_first + lax.broadcasted_iota(jnp.int32, (8, experts), 0)).astype(jnp.bfloat16)
    pick_col = (lax.broadcasted_iota(jnp.int32, (experts, LANES), 0) == my_first + lax.broadcasted_iota(jnp.int32, (experts, LANES), 1)).astype(jnp.bfloat16)
    tok_in(0).start()

    def dispatch_body(s, carry):
        @pl.when(s + 1 < n_src)
        def _():
            tok_in(s + 1).start()

        tok_in(s).wait()
        u = work[s % 2, :tokens]
        tables = work[s % 2, tokens:]
        slot_row = jnp.dot(pick_row, tables, preferred_element_type=jnp.float32)
        col_tab = lax.dot_general(tables, pick_col, (((0,), (0,)), ((), ())), preferred_element_type=jnp.float32)
        slot_ids = lax.broadcasted_iota(jnp.int32, (pad_cap, tokens), 0).astype(jnp.float32)
        rows = pl.ds(pl.multiple_of(s * pad_cap, pad_cap), pad_cap)
        for e in range(n_exp):
            one_hot = jnp.where(slot_ids == slot_row[e:e + 1, :tokens], 1.0, 0.0).astype(jnp.bfloat16)
            big[e, rows] = jnp.dot(one_hot, u, preferred_element_type=jnp.float32).astype(jnp.bfloat16)
        buf_ids = lax.broadcasted_iota(jnp.int32, (tokens, n_exp * pad_cap), 1).astype(jnp.float32)
        gates = jnp.zeros((tokens, n_exp * pad_cap), jnp.float32)
        for e in range(n_exp):
            slot_e = col_tab[:tokens, e:e + 1]
            dest_e = jnp.where(slot_e >= 0.0, slot_e + float(e * pad_cap), -1.0)
            gates = jnp.where(buf_ids == dest_e, col_tab[tokens:, e:e + 1], gates)
        comb[s] = gates.astype(jnp.bfloat16)
        return carry

    lax.fori_loop(0, n_src, dispatch_body, 0)

    row_tile = n_rows // 4

    def expert_inner(e):
        need(e)

        def tile_body(t, carry):
            at = pl.ds(pl.multiple_of(t * row_tile, row_tile), row_tile)
            rows = big[e, at]
            gate_act = jnp.dot(rows, gate_up[:, e, 0].reshape(d_model, ffn), preferred_element_type=jnp.float32)
            up_act = jnp.dot(rows, gate_up[:, e, 1].reshape(d_model, ffn), preferred_element_type=jnp.float32)
            inner[e, at] = (gate_act * jax.nn.sigmoid(gate_act) * up_act).astype(jnp.bfloat16)
            return carry

        lax.fori_loop(0, 4, tile_body, 0)

    for e in range(n_exp):
        expert_inner(e)

    def block_of(i):
        k, sub = i // n_sub, i % n_sub
        if isinstance(i, int) and k == 0:
            return dz, sub
        near_end = dz + upper * (3 - 2 * dz)
        low = k - near_end * ((3 - k) // 2)
        return low + upper * (3 - 2 * low), sub

    def rel_slot(rel, core_rel):
        return toggled(dx, rel % 2) * 4 + toggled(dy, rel // 2) * 2 + flip(dc, core_rel)

    halves = (pl.ds(0, half_tok), pl.ds(half_tok, half_tok))

    def core_copy(i, rel):
        return remote(send_core.at[i % 2, rel], got_core.at[i % 2, rel], core_send.at[i, rel], core_recv.at[i, rel], partner)

    def x_copy(i, rel):
        where = (3 - rel) // 2
        return remote(acc.at[i % 2, rel, halves[0]], got_x.at[i % 3, where], x_send.at[i, where], x_recv.at[i, where], across_x)

    def y_copy(i, rel):
        where = 3 - rel
        return remote(acc.at[i % 2, rel, halves[1]], got_y.at[i % 3, where], y_send.at[i, where], y_recv.at[i, where], across_y)

    def last_copy(i, which):
        rel, target = ((2, across_y), (1, across_x))[which]
        return remote(acc.at[i % 2, rel, halves[which]], got_last.at[i % 3, which], last_send.at[i, which], last_recv.at[i, which], target)

    def y_block(i):
        p, sub = block_of(i)
        if not (isinstance(i, int) and i < n_sub):
            @pl.when(at_end)
            def _():
                wait_in(down_all.at[p, sub], z_recv.at[p, n_exp + sub, 0])

        def y_body(e, carry):
            y_tall = jnp.dot(inner[e], down_all[p, sub, e], preferred_element_type=jnp.float32).astype(jnp.bfloat16)
            at = pl.ds(pl.multiple_of(e * pad_cap, pad_cap), pad_cap)
            for s in range(n_src):
                y_buf[s, at] = y_tall[s * pad_cap:(s + 1) * pad_cap]
            return carry

        lax.fori_loop(0, n_exp, y_body, 0)

    def sum_block(i):
        def partial(rel, core_rel):
            slot = rel_slot(rel, core_rel)
            return jnp.dot(comb[slot], y_buf[slot], preferred_element_type=jnp.float32)

        def core_body(k, carry):
            rel = 3 - k
            send_core[i % 2, rel] = partial(rel, 1)
            core_copy(i, rel).start()
            return carry

        def own_body(k, carry):
            rel = 3 - k
            own = partial(rel, 0)
            wait_in(got_core.at[i % 2, rel], core_recv.at[i, rel])
            acc[i % 2, rel] = own + got_core[i % 2, rel]

            @pl.when(rel % 2 == 1)
            def _():
                x_copy(i, rel).start()

            @pl.when(rel // 2 == 1)
            def _():
                y_copy(i, rel).start()

            return carry

        lax.fori_loop(0, 4, core_body, 0)
        lax.fori_loop(0, 4, own_body, 0)

    def turn_block(i):
        wait_in(got_x.at[i % 3, 0], x_recv.at[i, 0])
        acc[i % 2, 2, halves[0]] += got_x[i % 3, 0]
        last_copy(i, 0).start()
        wait_in(got_y.at[i % 3, 0], y_recv.at[i, 0])
        acc[i % 2, 1, halves[1]] += got_y[i % 3, 0]
        last_copy(i, 1).start()

    def end_block(i):
        p, sub = block_of(i)
        cols = pl.ds(pl.multiple_of((p * n_sub + sub) * block_cols, block_cols), block_cols)
        for half, got, got_sems in ((0, got_x, x_recv), (1, got_y, y_recv)):
            wait_in(got.at[i % 3, 1], got_sems.at[i, 1])
            wait_in(got_last.at[i % 3, half], last_recv.at[i, half])
            total = acc[i % 2, 0, halves[half]] + got[i % 3, 1] + got_last[i % 3, half]
            out_ref[halves[half], cols] = (hidden[halves[half], cols].astype(jnp.float32) + total).astype(jnp.bfloat16)
        for rel in range(4):
            core_copy(i, rel).wait_send()
        for rel in (3, 1):
            x_copy(i, rel).wait_send()
        for rel in (3, 2):
            y_copy(i, rel).wait_send()
        for which in (0, 1):
            last_copy(i, which).wait_send()

    blocks = 4 * n_sub
    y_block(0)
    sum_block(0)
    forward(near, down_js)
    y_block(1)
    turn_block(0)
    sum_block(1)
    end_block(0)
    y_block(2)
    turn_block(1)
    sum_block(2)
    forward(far, down_js)
    end_block(1)

    def block_body(i, carry):
        y_block(i + 1)
        turn_block(i)
        sum_block(i + 1)
        end_block(i)
        return carry

    lax.fori_loop(2, blocks - 3, block_body, 0)

    def late_body(i, carry):
        turn_block(i)
        y_block(i + 1)
        sum_block(i + 1)
        end_block(i)
        return carry

    lax.fori_loop(blocks - 3, blocks - 1, late_body, 0)
    turn_block(blocks - 1)
    end_block(blocks - 1)

    for j in range(chunks):
        @pl.when(dz > 0)
        def _():
            for copy in own_copies(0, j):
                copy.wait_send()

        @pl.when(dz < 3)
        def _():
            for copy in own_copies(1, j):
                copy.wait_send()

        @pl.when(inside)
        def _():
            for which, (p, z) in enumerate(passes):
                for copy in pass_copies(which, p, j, z):
                    copy.wait_send()


def whole_layer(head_dim, pad_cap, x, idx_t, slot_t, gate_t, attn_gain, moe_gain, qkv, proj, gate_w, up_w, down_w, experts):
    tokens, d_model = x.shape
    n_exp = gate_w.shape[0] // 2
    part_depth, ffn = gate_w.shape[1:]
    parts, n_src, block_cols = 4, 8, LANES
    n_sub = down_w.shape[2] // block_cols
    blocks = parts * n_sub
    chunks = n_exp + n_sub
    n_rows = n_src * pad_cap
    half = tokens // 2
    cos_tab, sin_tab = rope_tables(tokens, head_dim)
    dma = pltpu.SemaphoreType.DMA
    bf16, f32 = jnp.bfloat16, jnp.float32
    vmem, hbm = pl.BlockSpec(memory_space=pltpu.VMEM), pl.BlockSpec(memory_space=pl.ANY)
    return pl.pallas_call(
        functools.partial(layer_kernel, head_dim, pad_cap),
        out_shape=(jax.ShapeDtypeStruct(x.shape, bf16), jax.ShapeDtypeStruct((n_src, tokens + experts, d_model), bf16)),
        in_specs=[vmem] * 8 + [hbm] * 5,
        out_specs=(vmem, hbm),
        scratch_shapes=[
            pltpu.VMEM((n_exp, n_rows, d_model), bf16),
            pltpu.VMEM((parts, n_exp, 2, part_depth, ffn), bf16),
            pltpu.VMEM((parts, n_sub, n_exp, ffn, block_cols), bf16),
            pltpu.VMEM((4, tokens + experts, d_model), bf16),
            pltpu.VMEM((tokens + experts, d_model), bf16),
            pltpu.VMEM((tokens, d_model), bf16),
            pltpu.VMEM((n_exp, n_rows, ffn), bf16),
            pltpu.VMEM((n_src, tokens, n_exp * pad_cap), bf16),
            pltpu.VMEM((n_src, n_exp * pad_cap, block_cols), bf16),
            pltpu.VMEM((2, 4, tokens, block_cols), f32),
            pltpu.VMEM((2, 4, tokens, block_cols), f32),
            pltpu.VMEM((2, 4, tokens, block_cols), f32),
            pltpu.VMEM((3, 2, half, block_cols), f32),
            pltpu.VMEM((3, 2, half, block_cols), f32),
            pltpu.VMEM((3, 2, half, block_cols), f32),
            dma((42,)), dma((3, 4)), dma((3, 4)), dma((3, 4, 2, 2)), dma((4 + 2 * chunks,)),
            dma((14,)), dma((4, 2, 2)), dma, dma((2,)),
            dma((2, chunks, 2)), dma((3, chunks, 2)), dma((parts, chunks, 2)),
            dma((blocks, 4)), dma((blocks, 4)), dma((blocks, 2)), dma((blocks, 2)),
            dma((blocks, 2)), dma((blocks, 2)), dma((blocks, 2)), dma((blocks, 2)),
        ],
        compiler_params=pltpu.CompilerParams(collective_id=1, has_side_effects=True, vmem_limit_bytes=63 * 1024 * 1024),
        cost_estimate=pl.CostEstimate(flops=40_000_000_000, bytes_accessed=30_000_000, transcendentals=0),
        name='whole_layer',
    )(x, idx_t, slot_t, gate_t, attn_gain, moe_gain, cos_tab, sin_tab, qkv, proj, gate_w, up_w, down_w)[0]


def solution(mesh):
    tok_spec = P(('data', 'fsdp', 'ep'), None, None)
    ep_count = mesh.shape['ep']

    def local_step(x_blk, idx_blk, slot_blk, gate_blk, attn_gain, qkv_shard, out_shard, moe_gain, gate_shard, up_shard, down_shard):
        batch_rows, seq_len, d_model = x_blk.shape
        tokens = batch_rows * seq_len
        top_k = idx_blk.shape[-1]
        head_dim = qkv_shard.shape[3]
        experts = gate_shard.shape[0] * ep_count
        capacity = capacity_of(tokens, top_k, experts)
        pad_cap = 16 * ((capacity + 15) // 16)
        by_choice = [blk.reshape(tokens, top_k).T for blk in (idx_blk, slot_blk, gate_blk)]
        gains = [gain.astype(jnp.float32)[None, :] for gain in (attn_gain, moe_gain)]
        qkv = qkv_shard.reshape(qkv_shard.shape[0], -1)
        proj = out_shard.reshape(-1, d_model)
        result = whole_layer(head_dim, pad_cap, x_blk.reshape(tokens, d_model), *by_choice, *gains, qkv, proj, gate_shard, up_shard, down_shard, experts)
        return result.reshape(batch_rows, seq_len, d_model)

    return jax.shard_map(local_step, mesh=mesh, in_specs=(tok_spec, tok_spec, tok_spec, tok_spec, P(None), P('fsdp', None, None, None), P('fsdp', None, None), P(None), P('ep', 'fsdp', None), P('ep', 'fsdp', None), P('ep', None, 'fsdp')), out_specs=tok_spec, check_vma=False)
```

```python
import functools

import jax
import jax.numpy as jnp
import numpy as np
from jax import lax
from jax.experimental import pallas as pl
from jax.experimental.pallas import tpu as pltpu
from jax.sharding import PartitionSpec as P

NORM_EPS = 1e-6
ROPE_BASE = 10000.0
MESH_ID = pl.DeviceIdType.MESH
LANES = 128


def capacity_of(tok_count, top_k, experts):
    return 8 * ((5 * tok_count * top_k) // (32 * experts) + 1)


def rope_tables(seq_len, head_dim):
    half = head_dim // 2
    lane = np.arange(LANES)
    inv_freq = ROPE_BASE ** (-(lane % half) / half)
    angles = np.arange(seq_len)[:, None] * inv_freq[None, :]
    sign = np.where(lane % head_dim < half, -1.0, 1.0)
    return np.cos(angles).astype(np.float32), (np.sin(angles) * sign).astype(np.float32)


def layer_place():
    dx, dz, ep = lax.axis_index('data'), lax.axis_index('fsdp'), lax.axis_index('ep')
    return dx, dz, ep // 2, ep % 2


def flip(pos, bit):
    return (1 - pos) if bit else pos


def toggled(pos, bit):
    return pos + bit - 2 * pos * bit


def related(place, chip_rel, core_rel):
    dx, dz, dy, dc = place
    return flip(dx, chip_rel & 1), dz, flip(dy, chip_rel & 2), flip(dc, core_rel)


def slot_of(place):
    dx, _, dy, dc = place
    return dx * 4 + dy * 2 + dc


def dev_id(place):
    dx, dz, dy, dc = place
    return (dx, dz, dy * 2 + dc)


def remote(src, dst, send_sem, recv_sem, where):
    return pltpu.make_async_remote_copy(src_ref=src, dst_ref=dst, send_sem=send_sem, recv_sem=recv_sem, device_id=dev_id(where), device_id_type=MESH_ID)


def wait_in(ref, sem):
    pltpu.make_async_copy(ref, ref, sem).wait()


def spread_in_layer(place, own_refs, part_refs, send_sem, direct_sems, partner_sem, half_size, partner_size):
    across_x, across_y, partner = related(place, 1, 0), related(place, 2, 0), related(place, 0, 1)

    def pass_on(chip_rel, half, target, sem, first=False):
        owner = slot_of(related(place, chip_rel, 0))
        dsts = part_refs(owner, half)
        for src, dst in zip(own_refs(half) if first else dsts, dsts):
            remote(src, dst, send_sem, sem, target).start()

    def direct(rel_there, half):
        return direct_sems.at[rel_there - 1, half]

    for half in (0, 1):
        pass_on(0, half, across_x, direct(1, half), True)
        pass_on(0, 1 - half, across_y, direct(2, 1 - half), True)
    for half in (0, 1):
        pass_on(0, half, partner, partner_sem, True)
    yield

    def arrived(chip_rel, half):
        wait_in(half_size, direct(chip_rel, half))

    arrived(1, 0)
    pass_on(1, 0, across_y, direct(3, 0))
    pass_on(1, 0, partner, partner_sem)
    arrived(2, 1)
    pass_on(2, 1, across_x, direct(3, 1))
    pass_on(2, 1, partner, partner_sem)
    yield
    arrived(1, 1)
    pass_on(1, 1, partner, partner_sem)
    arrived(2, 0)
    pass_on(2, 0, partner, partner_sem)
    yield
    arrived(3, 0)
    pass_on(3, 0, partner, partner_sem)
    arrived(3, 1)
    pass_on(3, 1, partner, partner_sem)
    yield
    wait_in(partner_size, partner_sem)
    yield


def norm_rows(src, gain_ref, dst, rows):
    tile = 128
    gain = gain_ref[...].astype(jnp.float32).reshape(1, -1)

    def body(t, carry):
        at = pl.ds(pl.multiple_of(t * tile, tile), tile)
        wide = src[at].astype(jnp.float32)
        inv_rms = lax.rsqrt(jnp.mean(wide * wide, axis=-1, keepdims=True) + NORM_EPS)
        dst[at] = (wide * inv_rms * gain).astype(jnp.bfloat16)
        return carry

    lax.fori_loop(0, rows // tile, body, 0)


def attend(x_ref, normed, weights, rope, qkv, hidden, head_dim):
    tokens, d_model = x_ref.shape
    lane = lax.broadcasted_iota(jnp.int32, (tokens, LANES), 1)
    low_half = lane % head_dim < head_dim // 2
    first_head = lax.broadcasted_iota(jnp.int32, (tokens // 2, LANES), 1) < head_dim
    group = 2 * LANES
    q_tile = tokens // 2
    scale = head_dim ** -0.5

    def rotate(val):
        swapped = jnp.where(low_half, pltpu.roll(val, LANES - head_dim // 2, 1), pltpu.roll(val, head_dim // 2, 1))
        return (val * rope[0] + swapped * rope[1]).astype(jnp.bfloat16)

    def project(b, cols):
        return lax.dot_general(normed[:tokens], weights[b, cols, :], (((1,), (1,)), ((), ())), preferred_element_type=jnp.float32)

    def group_body(g, carry):
        cols = pl.ds(pl.multiple_of(g * group, group), group)
        query, keys = project(0, cols), project(1, cols)
        values = project(2, cols).astype(jnp.bfloat16)
        for pair in (0, 1):
            at = slice(pair * LANES, (pair + 1) * LANES)
            qkv[0, :tokens, at] = rotate(query[:, at])
            qkv[1, :tokens, at] = rotate(keys[:, at])
            qkv[2, :tokens, at] = values[:, at]
        for pair in (0, 1):
            at = slice(pair * LANES, (pair + 1) * LANES)
            for tile in (0, 1):
                n_keys = (tile + 1) * q_tile
                q_pair = qkv[0, tile * q_tile:(tile + 1) * q_tile, at]
                k_pair, v_pair = qkv[1, :n_keys, at], qkv[2, :n_keys, at]
                row_id = lax.broadcasted_iota(jnp.int32, (q_tile, n_keys), 0) + tile * q_tile
                causal = row_id >= lax.broadcasted_iota(jnp.int32, (q_tile, n_keys), 1)
                outs = []
                for head in (0, 1):
                    q_head = jnp.where(first_head if head == 0 else ~first_head, q_pair, jnp.zeros((), jnp.bfloat16))
                    scores = lax.dot_general(q_head, k_pair, (((1,), (1,)), ((), ())), preferred_element_type=jnp.float32)
                    scores = jnp.where(causal, scores * scale, -1e30)
                    top = jnp.max(scores, axis=-1, keepdims=True)
                    weight = jnp.exp(scores - top)
                    probs = (weight * (1.0 / jnp.sum(weight, axis=-1, keepdims=True))).astype(jnp.bfloat16)
                    outs.append(jnp.dot(probs, v_pair, preferred_element_type=jnp.float32))
                out_cols = pl.ds(pl.multiple_of(g * group + pair * LANES, LANES), LANES)
                qkv[3, tile * q_tile:(tile + 1) * q_tile, out_cols] = jnp.where(first_head, outs[0], outs[1]).astype(jnp.bfloat16)
        return carry

    lax.fori_loop(0, d_model // group, group_body, 0)

    def out_body(g, carry):
        cols = pl.ds(pl.multiple_of(g * group, group), group)
        attn_out = jnp.dot(qkv[3, :tokens], weights[3, :d_model, cols], preferred_element_type=jnp.float32)
        hidden[:, cols] = (x_ref[:, cols].astype(jnp.float32) + attn_out).astype(jnp.bfloat16)
        return carry

    lax.fori_loop(0, d_model // group, out_body, 0)


def layer_kernel(head_dim, pad_cap,
                 idx_ref, slot_ref, gate_ref, attn_gain_ref, moe_gain_ref,
                 x_hbm, rope_hbm, qkv_hbm, proj_hbm, gate_hbm, up_hbm, down_hbm,
                 out_ref, tok_hbm,
                 x_ref, rope, big, gate_up, down_all, work, own_tok, hidden, inner, comb, y_buf, send_core, acc, got_core, got_x, got_y, got_last,
                 attn_send, attn_z_send, attn_z_recv, attn_direct, attn_partner, load_sems, tok_send, tok_direct, tok_partner, tok_sem, tok_load,
                 z_own, z_pass, z_recv, core_send, core_recv, x_send, x_recv, y_send, y_recv, last_send, last_recv):
    place = layer_place()
    dx, dz, dy, dc = place
    tokens, d_model = x_ref.shape
    experts = own_tok.shape[0] - tokens
    n_exp, n_rows, ffn = inner.shape
    n_src = comb.shape[0]
    block_cols = acc.shape[-1]
    half_tok = tokens // 2
    n_sub = down_all.shape[1]
    chunks = n_exp + n_sub
    across_x, across_y, partner = related(place, 1, 0), related(place, 2, 0), related(place, 0, 1)
    upper = dz // 2
    inside = (dz == 1) | (dz == 2)
    at_end = (dz == 0) | (dz == 3)
    first_exp = dx * n_exp
    mine = slot_of(place)

    def at_z(z):
        return (dx, z, dy, dc)

    x_copy_in = pltpu.make_async_copy(x_hbm, x_ref, load_sems.at[0])
    rope_copy_in = pltpu.make_async_copy(rope_hbm, rope, load_sems.at[1])
    x_copy_in.start()
    rope_copy_in.start()
    barrier = pltpu.get_barrier_semaphore()
    for target in [at_z((dz + step) % 4) for step in (1, 2, 3)] + [across_x, across_y, partner]:
        pl.semaphore_signal(barrier, inc=1, device_id=dev_id(target), device_id_type=MESH_ID)
    pl.semaphore_wait(barrier, 6)

    shard_rows = proj_hbm.shape[0]
    row_piece, col_piece = shard_rows // 8, d_model // 8

    def qkv_rows(start, rows, col_z=None):
        at = pl.ds(pl.multiple_of(start, rows), rows)
        if col_z is None:
            return qkv_hbm.at[:, at]
        return big.at[pl.ds(0, 3), at, pl.ds(pl.multiple_of(col_z * shard_rows, shard_rows), shard_rows)]

    def proj_rows(start, rows):
        return big.at[3, pl.ds(pl.multiple_of(start, rows), rows)]

    def size_of(halves):
        return big.at[0, pl.ds(0, halves * row_piece * 2)]

    z_steps = (1, 3, 2)
    for index, step in enumerate(z_steps):
        proj_src = proj_hbm.at[pl.ds(pl.multiple_of(mine * row_piece, row_piece), row_piece)]
        for src, dst in ((qkv_rows(mine * col_piece, col_piece), qkv_rows(mine * col_piece, col_piece, dz)), (proj_src, proj_rows(dz * shard_rows + mine * row_piece, row_piece))):
            remote(src, dst, attn_z_send.at[index], attn_z_recv.at[index], at_z((dz + step) % 4)).start()

    def chunk_refs(p, j):
        if j < n_exp:
            return [gate_up.at[p, j, m] for m in (0, 1)]
        return [down_all.at[p, j - n_exp]]

    def chunk_srcs(j):
        if j < n_exp:
            return [gate_hbm.at[first_exp + j], up_hbm.at[first_exp + j]]
        return [down_hbm.at[pl.ds(first_exp, n_exp), :, pl.ds((j - n_exp) * block_cols, block_cols)]]

    def own_copies(side, j):
        target = at_z(dz - 1 if side == 0 else dz + 1)
        return [remote(src, dst, z_own.at[side, j // n_exp], z_recv.at[dz, j], target) for src, dst in zip(chunk_srcs(j), chunk_refs(dz, j))]

    def whole_chunk(p, j):
        return gate_up.at[p, j] if j < n_exp else down_all.at[p, j - n_exp]

    def pass_copy(which, p, j, z):
        return remote(whole_chunk(p, j), whole_chunk(p, j), z_pass.at[which, j // n_exp], z_recv.at[p, j], at_z(z))

    def wait_chunk(p, j):
        wait_in(whole_chunk(p, j), z_recv.at[p, j])

    end_z, mid_z, far_z = 3 * (dz - 1), 3 - dz, 3 * (2 - dz)
    passes = ((end_z, mid_z), (mid_z, end_z), (far_z, end_z))

    def send_own(j):
        @pl.when(dz > 0)
        def _():
            for copy in own_copies(0, j):
                copy.start()

        @pl.when(dz < 3)
        def _():
            for copy in own_copies(1, j):
                copy.start()

    def forward(kinds, js):
        @pl.when(inside)
        def _():
            for j in js:
                for which in kinds:
                    p, z = passes[which]
                    wait_chunk(p, j)
                    pass_copy(which, p, j, z).start()

    near, far, expert_js, down_js = (0, 1), (2,), range(n_exp), range(n_exp, chunks)

    def need(j):
        @pl.when(at_end)
        def _():
            for k in range(3):
                wait_chunk(k + 1 - upper, j)

    for j in expert_js:
        send_own(j)
    own_loads = [
        (qkv_hbm, big.at[pl.ds(0, 3), pl.ds(0, d_model), pl.ds(pl.multiple_of(dz * shard_rows, shard_rows), shard_rows)], 2),
        (proj_hbm, proj_rows(dz * shard_rows, shard_rows), 2),
    ]
    for j in range(chunks):
        own_loads += [(src, dst, 3 + j // n_exp) for src, dst in zip(chunk_srcs(j), chunk_refs(dz, j))]
    for src, dst, sem in own_loads:
        pltpu.make_async_copy(src, dst, load_sems.at[sem]).start()

    x_copy_in.wait()
    norm_rows(x_ref, attn_gain_ref, own_tok, tokens)

    expert_ids = lax.broadcasted_iota(jnp.int32, (experts, tokens), 0)
    slot_tab = jnp.zeros((experts, tokens), jnp.float32)
    gate_tab = jnp.zeros((experts, tokens), jnp.float32)
    for k in range(idx_ref.shape[0]):
        hit = expert_ids == idx_ref[k:k + 1, :]
        slot_tab = slot_tab + jnp.where(hit, slot_ref[k:k + 1, :].astype(jnp.float32) + 1.0, 0.0)
        gate_tab = gate_tab + jnp.where(hit, gate_ref[k:k + 1, :].astype(jnp.float32), 0.0)
    own_tok[tokens:, :tokens] = (slot_tab - 1.0).astype(jnp.bfloat16)
    own_tok[tokens:, tokens:] = gate_tab.astype(jnp.bfloat16)

    streams = []
    for index, step in enumerate(z_steps):
        source_z = (dz + 4 - step) % 4

        def part_refs(slot, half, source_z=source_z):
            cols, rows = col_piece // 2, row_piece // 2
            return [qkv_rows(slot * col_piece + half * cols, cols, source_z), proj_rows(source_z * shard_rows + slot * row_piece + half * rows, rows)]

        streams.append(spread_in_layer(place, functools.partial(part_refs, mine), part_refs, attn_send.at[index], attn_direct.at[index], attn_partner.at[index], size_of(1), size_of(8)))
    for index, stream in enumerate(streams):
        wait_in(size_of(2), attn_z_recv.at[index])
        next(stream)
    for _ in range(4):
        for stream in streams:
            next(stream)
    wait_in(size_of(16), load_sems.at[2])
    rope_copy_in.wait()

    attend(x_ref, own_tok, big, rope, work, hidden, head_dim)
    norm_rows(hidden, moe_gain_ref, own_tok, tokens)
    for index in range(3):
        wait_in(size_of(14), attn_send.at[index])
        wait_in(size_of(2), attn_z_send.at[index])

    half_rows = own_tok.shape[0] // 2

    def tok_part(slot, half):
        return [tok_hbm.at[slot, pl.ds(half * half_rows, half_rows)]]

    def tok_half(half):
        return [own_tok.at[pl.ds(half * half_rows, half_rows)]]

    stream = spread_in_layer(place, tok_half, tok_part, tok_send, tok_direct, tok_partner, tok_part(0, 0)[0], tok_hbm.at[pl.ds(0, 4)])
    next(stream)
    tok_copy = pltpu.make_async_copy(own_tok, tok_hbm.at[mine], tok_sem)
    tok_copy.start()
    forward(near, expert_js)
    for _ in range(4):
        next(stream)
    tok_copy.wait()
    wait_in(tok_hbm.at[pl.ds(0, 7)], tok_send)
    forward(far, expert_js)
    for j in down_js:
        send_own(j)

    def tok_in(s):
        return pltpu.make_async_copy(tok_hbm.at[s], work.at[s % 2], tok_load.at[s % 2])

    my_first = (lax.axis_index('ep') * 2 + dx) * n_exp
    pick_row = (lax.broadcasted_iota(jnp.int32, (8, experts), 1) == my_first + lax.broadcasted_iota(jnp.int32, (8, experts), 0)).astype(jnp.bfloat16)
    pick_col = (lax.broadcasted_iota(jnp.int32, (experts, LANES), 0) == my_first + lax.broadcasted_iota(jnp.int32, (experts, LANES), 1)).astype(jnp.bfloat16)
    tok_in(0).start()

    def dispatch_body(s, carry):
        @pl.when(s + 1 < n_src)
        def _():
            tok_in(s + 1).start()

        tok_in(s).wait()
        u = work[s % 2, :tokens]
        tables = work[s % 2, tokens:]
        slot_row = jnp.dot(pick_row, tables, preferred_element_type=jnp.float32)
        col_tab = lax.dot_general(tables, pick_col, (((0,), (0,)), ((), ())), preferred_element_type=jnp.float32)
        slot_ids = lax.broadcasted_iota(jnp.int32, (pad_cap, tokens), 0).astype(jnp.float32)
        rows = pl.ds(pl.multiple_of(s * pad_cap, pad_cap), pad_cap)
        for e in range(n_exp):
            one_hot = jnp.where(slot_ids == slot_row[e:e + 1, :tokens], 1.0, 0.0).astype(jnp.bfloat16)
            big[e, rows] = jnp.dot(one_hot, u, preferred_element_type=jnp.float32).astype(jnp.bfloat16)
        buf_ids = lax.broadcasted_iota(jnp.int32, (tokens, n_exp * pad_cap), 1).astype(jnp.float32)
        gates = jnp.zeros((tokens, n_exp * pad_cap), jnp.float32)
        for e in range(n_exp):
            slot_e = col_tab[:tokens, e:e + 1]
            dest_e = jnp.where(slot_e >= 0.0, slot_e + float(e * pad_cap), -1.0)
            gates = jnp.where(buf_ids == dest_e, col_tab[tokens:, e:e + 1], gates)
        comb[s] = gates.astype(jnp.bfloat16)
        return carry

    lax.fori_loop(0, n_src, dispatch_body, 0)

    row_tile = n_rows // 4

    def expert_inner(e):
        need(e)

        def tile_body(t, carry):
            at = pl.ds(pl.multiple_of(t * row_tile, row_tile), row_tile)
            rows = big[e, at]
            gate_act = jnp.dot(rows, gate_up[:, e, 0].reshape(d_model, ffn), preferred_element_type=jnp.float32)
            up_act = jnp.dot(rows, gate_up[:, e, 1].reshape(d_model, ffn), preferred_element_type=jnp.float32)
            inner[e, at] = (gate_act * jax.nn.sigmoid(gate_act) * up_act).astype(jnp.bfloat16)
            return carry

        lax.fori_loop(0, 4, tile_body, 0)

    wait_in(gate_up.at[0], load_sems.at[3])
    wait_in(down_all.at[0], load_sems.at[4])
    for e in range(n_exp):
        expert_inner(e)

    def block_of(i):
        k, sub = i // n_sub, i % n_sub
        if isinstance(i, int) and k == 0:
            return dz, sub
        near_end = dz + upper * (3 - 2 * dz)
        low = k - near_end * ((3 - k) // 2)
        return low + upper * (3 - 2 * low), sub

    def rel_slot(rel, core_rel):
        return toggled(dx, rel % 2) * 4 + toggled(dy, rel // 2) * 2 + flip(dc, core_rel)

    halves = (pl.ds(0, half_tok), pl.ds(half_tok, half_tok))

    def core_copy(i, rel):
        return remote(send_core.at[i % 2, rel], got_core.at[i % 2, rel], core_send.at[i % 2, rel], core_recv.at[i % 2, rel], partner)

    def x_copy(i, rel):
        where = (3 - rel) // 2
        return remote(acc.at[i % 2, rel, halves[0]], got_x.at[i % 3, where], x_send.at[i % 3, where], x_recv.at[i % 3, where], across_x)

    def y_copy(i, rel):
        where = 3 - rel
        return remote(acc.at[i % 2, rel, halves[1]], got_y.at[i % 3, where], y_send.at[i % 3, where], y_recv.at[i % 3, where], across_y)

    def last_copy(i, which):
        rel, target = ((2, across_y), (1, across_x))[which]
        return remote(acc.at[i % 2, rel, halves[which]], got_last.at[i % 3, which], last_send.at[i % 3, which], last_recv.at[i % 3, which], target)

    def y_block(i):
        p, sub = block_of(i)
        if not (isinstance(i, int) and i < n_sub):
            @pl.when(at_end)
            def _():
                wait_in(down_all.at[p, sub], z_recv.at[p, n_exp + sub])

        def y_body(e, carry):
            y_tall = jnp.dot(inner[e], down_all[p, sub, e], preferred_element_type=jnp.float32).astype(jnp.bfloat16)
            at = pl.ds(pl.multiple_of(e * pad_cap, pad_cap), pad_cap)
            for s in range(n_src):
                y_buf[s, at] = y_tall[s * pad_cap:(s + 1) * pad_cap]
            return carry

        lax.fori_loop(0, n_exp, y_body, 0)

    def sum_block(i):
        def partial(rel, core_rel):
            slot = rel_slot(rel, core_rel)
            return jnp.dot(comb[slot], y_buf[slot], preferred_element_type=jnp.float32)

        def core_body(k, carry):
            rel = 3 - k
            send_core[i % 2, rel] = partial(rel, 1)
            core_copy(i, rel).start()
            return carry

        def own_body(k, carry):
            rel = 3 - k
            own = partial(rel, 0)
            wait_in(got_core.at[i % 2, rel], core_recv.at[i % 2, rel])
            acc[i % 2, rel] = own + got_core[i % 2, rel]

            @pl.when(rel % 2 == 1)
            def _():
                x_copy(i, rel).start()

            @pl.when(rel // 2 == 1)
            def _():
                y_copy(i, rel).start()

            return carry

        lax.fori_loop(0, 4, core_body, 0)
        lax.fori_loop(0, 4, own_body, 0)

    def turn_block(i):
        wait_in(got_x.at[i % 3, 0], x_recv.at[i % 3, 0])
        acc[i % 2, 2, halves[0]] += got_x[i % 3, 0]
        last_copy(i, 0).start()
        wait_in(got_y.at[i % 3, 0], y_recv.at[i % 3, 0])
        acc[i % 2, 1, halves[1]] += got_y[i % 3, 0]
        last_copy(i, 1).start()

    def end_block(i):
        p, sub = block_of(i)
        cols = pl.ds(pl.multiple_of((p * n_sub + sub) * block_cols, block_cols), block_cols)
        for half, got, got_sems in ((0, got_x, x_recv), (1, got_y, y_recv)):
            wait_in(got.at[i % 3, 1], got_sems.at[i % 3, 1])
            wait_in(got_last.at[i % 3, half], last_recv.at[i % 3, half])
            total = acc[i % 2, 0, halves[half]] + got[i % 3, 1] + got_last[i % 3, half]
            out_ref[halves[half], cols] = (hidden[halves[half], cols].astype(jnp.float32) + total).astype(jnp.bfloat16)
        for rel in range(4):
            core_copy(i, rel).wait_send()
        for rel in (3, 1):
            x_copy(i, rel).wait_send()
        for rel in (3, 2):
            y_copy(i, rel).wait_send()
        for which in (0, 1):
            last_copy(i, which).wait_send()

    blocks = 4 * n_sub
    y_block(0)
    sum_block(0)
    forward(near, down_js)
    y_block(1)
    turn_block(0)
    sum_block(1)
    end_block(0)
    y_block(2)
    turn_block(1)
    sum_block(2)
    forward(far, down_js)
    end_block(1)

    def block_body(i, carry):
        y_block(i + 1)
        turn_block(i)
        sum_block(i + 1)
        end_block(i)
        return carry

    lax.fori_loop(2, blocks - 3, block_body, 0)

    def late_body(i, carry):
        turn_block(i)
        y_block(i + 1)
        sum_block(i + 1)
        end_block(i)
        return carry

    lax.fori_loop(blocks - 3, blocks - 1, late_body, 0)
    turn_block(blocks - 1)
    end_block(blocks - 1)

    for kind, size in ((0, gate_up.at[0]), (1, down_all.at[0])):
        @pl.when(dz > 0)
        def _():
            wait_in(size, z_own.at[0, kind])

        @pl.when(dz < 3)
        def _():
            wait_in(size, z_own.at[1, kind])

        @pl.when(inside)
        def _():
            for which in range(3):
                wait_in(size, z_pass.at[which, kind])


def whole_layer(head_dim, pad_cap, x, idx_t, slot_t, gate_t, attn_gain, moe_gain, qkv, proj, gate_w, up_w, down_w, experts):
    tokens, d_model = x.shape
    n_exp = gate_w.shape[0] // 2
    part_depth, ffn = gate_w.shape[1:]
    parts, n_src, block_cols = 4, 8, LANES
    n_sub = down_w.shape[2] // block_cols
    chunks = n_exp + n_sub
    n_rows = n_src * pad_cap
    half = tokens // 2
    rope = np.stack(rope_tables(tokens, head_dim))
    dma = pltpu.SemaphoreType.DMA
    bf16, f32 = jnp.bfloat16, jnp.float32
    vmem, hbm = pl.BlockSpec(memory_space=pltpu.VMEM), pl.BlockSpec(memory_space=pl.ANY)
    return pl.pallas_call(
        functools.partial(layer_kernel, head_dim, pad_cap),
        out_shape=(jax.ShapeDtypeStruct(x.shape, bf16), jax.ShapeDtypeStruct((n_src, tokens + experts, d_model), bf16)),
        in_specs=[vmem] * 5 + [hbm] * 7,
        out_specs=(vmem, hbm),
        scratch_shapes=[
            pltpu.VMEM((tokens, d_model), bf16),
            pltpu.VMEM(rope.shape, f32),
            pltpu.VMEM((n_exp, n_rows, d_model), bf16),
            pltpu.VMEM((parts, n_exp, 2, part_depth, ffn), bf16),
            pltpu.VMEM((parts, n_sub, n_exp, ffn, block_cols), bf16),
            pltpu.VMEM((4, tokens + experts, d_model), bf16),
            pltpu.VMEM((tokens + experts, d_model), bf16),
            pltpu.VMEM((tokens, d_model), bf16),
            pltpu.VMEM((n_exp, n_rows, ffn), bf16),
            pltpu.VMEM((n_src, tokens, n_exp * pad_cap), bf16),
            pltpu.VMEM((n_src, n_exp * pad_cap, block_cols), bf16),
            pltpu.VMEM((2, 4, tokens, block_cols), f32),
            pltpu.VMEM((2, 4, tokens, block_cols), f32),
            pltpu.VMEM((2, 4, tokens, block_cols), f32),
            pltpu.VMEM((3, 2, half, block_cols), f32),
            pltpu.VMEM((3, 2, half, block_cols), f32),
            pltpu.VMEM((3, 2, half, block_cols), f32),
            dma((3,)), dma((3,)), dma((3,)), dma((3, 3, 2)), dma((3,)), dma((5,)),
            dma, dma((3, 2)), dma, dma, dma((2,)),
            dma((2, 2)), dma((3, 2)), dma((parts, chunks)), dma((2, 4)), dma((2, 4)),
            dma((3, 2)), dma((3, 2)), dma((3, 2)), dma((3, 2)), dma((3, 2)), dma((3, 2)),
        ],
        compiler_params=pltpu.CompilerParams(collective_id=1, has_side_effects=True, vmem_limit_bytes=63 * 1024 * 1024),
        cost_estimate=pl.CostEstimate(flops=40_000_000_000, bytes_accessed=30_000_000, transcendentals=0),
        name='whole_layer',
    )(idx_t, slot_t, gate_t, attn_gain, moe_gain, x, rope, qkv, proj, gate_w, up_w, down_w)[0]


def solution(mesh):
    tok_spec = P(('data', 'fsdp', 'ep'), None, None)
    ep_count = mesh.shape['ep']

    def local_step(x_blk, idx_blk, slot_blk, gate_blk, attn_gain, qkv_shard, out_shard, moe_gain, gate_shard, up_shard, down_shard):
        batch_rows, seq_len, d_model = x_blk.shape
        tokens = batch_rows * seq_len
        top_k = idx_blk.shape[-1]
        head_dim = qkv_shard.shape[3]
        experts = gate_shard.shape[0] * ep_count
        capacity = capacity_of(tokens, top_k, experts)
        pad_cap = 16 * ((capacity + 15) // 16)
        by_choice = [blk.reshape(tokens, top_k).T for blk in (idx_blk, slot_blk, gate_blk)]
        qkv = qkv_shard.transpose(1, 2, 3, 0).reshape(3, d_model, -1)
        proj = out_shard.reshape(-1, d_model)
        result = whole_layer(head_dim, pad_cap, x_blk.reshape(tokens, d_model), *by_choice, attn_gain, moe_gain, qkv, proj, gate_shard, up_shard, down_shard, experts)
        return result.reshape(batch_rows, seq_len, d_model)

    return jax.shard_map(local_step, mesh=mesh, in_specs=(tok_spec, tok_spec, tok_spec, tok_spec, P(None), P('fsdp', None, None, None), P('fsdp', None, None), P(None), P('ep', 'fsdp', None), P('ep', 'fsdp', None), P('ep', None, 'fsdp')), out_specs=tok_spec, check_vma=False)
```

```python
import functools

import jax
import jax.numpy as jnp
import numpy as np
from jax import lax
from jax.experimental import pallas as pl
from jax.experimental.pallas import tpu as pltpu
from jax.sharding import PartitionSpec as P

NORM_EPS = 1e-6
ROPE_BASE = 10000.0
MESH_ID = pl.DeviceIdType.MESH
LANES = 128
BOTH = (0, 1)
LANES_BOTH = (((1,), (1,)), ((), ()))


def capacity_of(tok_count, top_k, experts):
    return 8 * ((5 * tok_count * top_k) // (32 * experts) + 1)


def rope_tables(seq_len, head_dim):
    half = head_dim // 2
    lane = np.arange(LANES)
    inv_freq = ROPE_BASE ** (-(lane % half) / half)
    angles = np.arange(seq_len)[:, None] * inv_freq[None, :]
    sign = np.where(lane % head_dim < half, -1.0, 1.0)
    return np.cos(angles).astype(np.float32), (np.sin(angles) * sign).astype(np.float32)


def two(i):
    return i % 2


def three(i):
    return i % 3


def layer_place():
    dx, dz, ep = lax.axis_index('data'), lax.axis_index('fsdp'), lax.axis_index('ep')
    return dx, dz, ep // 2, ep % 2


def flip(pos, bit):
    return (1 - pos) if bit else pos


def toggled(pos, bit):
    return pos + bit - 2 * pos * bit


def related(place, chip_rel, core_rel):
    dx, dz, dy, dc = place
    return flip(dx, chip_rel & 1), dz, flip(dy, chip_rel & 2), flip(dc, core_rel)


def slot_of(place):
    dx, _, dy, dc = place
    return dx * 4 + dy * 2 + dc


def dev_id(place):
    dx, dz, dy, dc = place
    return (dx, dz, dy * 2 + dc)


def remote(src, dst, send_sem, recv_sem, where):
    return pltpu.make_async_remote_copy(src_ref=src, dst_ref=dst, send_sem=send_sem, recv_sem=recv_sem, device_id=dev_id(where), device_id_type=MESH_ID)


def wait_in(ref, sem):
    pltpu.make_async_copy(ref, ref, sem).wait()


def spread_in_layer(place, own_refs, part_refs, send_sem, direct_sems, partner_sem, half_size, partner_size):
    across_x, across_y, partner = related(place, 1, 0), related(place, 2, 0), related(place, 0, 1)

    def pass_on(chip_rel, half, target, sem, first=False):
        owner = slot_of(related(place, chip_rel, 0))
        dsts = part_refs(owner, half)
        for src, dst in zip(own_refs(half) if first else dsts, dsts):
            remote(src, dst, send_sem, sem, target).start()

    def direct(rel_there, half):
        return direct_sems.at[rel_there - 1, half]

    for half in BOTH:
        pass_on(0, half, across_x, direct(1, half), True)
        pass_on(0, 1 - half, across_y, direct(2, 1 - half), True)
    for half in BOTH:
        pass_on(0, half, partner, partner_sem, True)
    yield

    def arrived(chip_rel, half):
        wait_in(half_size, direct(chip_rel, half))

    arrived(1, 0)
    pass_on(1, 0, across_y, direct(3, 0))
    pass_on(1, 0, partner, partner_sem)
    arrived(2, 1)
    pass_on(2, 1, across_x, direct(3, 1))
    pass_on(2, 1, partner, partner_sem)
    yield
    arrived(1, 1)
    pass_on(1, 1, partner, partner_sem)
    arrived(2, 0)
    pass_on(2, 0, partner, partner_sem)
    yield
    arrived(3, 0)
    pass_on(3, 0, partner, partner_sem)
    arrived(3, 1)
    pass_on(3, 1, partner, partner_sem)
    yield
    wait_in(partner_size, partner_sem)
    yield


def norm_rows(src, gain_ref, dst, rows):
    tile = 128
    gain = gain_ref[...].astype(jnp.float32).reshape(1, -1)

    def body(t, carry):
        at = pl.ds(pl.multiple_of(t * tile, tile), tile)
        wide = src[at].astype(jnp.float32)
        inv_rms = lax.rsqrt(jnp.mean(wide * wide, axis=-1, keepdims=True) + NORM_EPS)
        dst[at] = (wide * inv_rms * gain).astype(jnp.bfloat16)
        return carry

    lax.fori_loop(0, rows // tile, body, 0)


def attend(x_ref, normed, weights, rope, qkv, hidden, head_dim):
    tokens, d_model = x_ref.shape
    lane = lax.broadcasted_iota(jnp.int32, (tokens, LANES), 1)
    low_half = lane % head_dim < head_dim // 2
    first_head = lax.broadcasted_iota(jnp.int32, (tokens // 2, LANES), 1) < head_dim
    group = 2 * LANES
    q_tile = tokens // 2
    scale = head_dim ** -0.5

    def rotate(val):
        swapped = jnp.where(low_half, pltpu.roll(val, LANES - head_dim // 2, 1), pltpu.roll(val, head_dim // 2, 1))
        return (val * rope[0] + swapped * rope[1]).astype(jnp.bfloat16)

    def project(b, cols):
        return lax.dot_general(normed[:tokens], weights[b, cols, :], LANES_BOTH, preferred_element_type=jnp.float32)

    def group_body(g, carry):
        cols = pl.ds(pl.multiple_of(g * group, group), group)
        query, keys = project(0, cols), project(1, cols)
        values = project(2, cols).astype(jnp.bfloat16)
        for pair in BOTH:
            at = slice(pair * LANES, (pair + 1) * LANES)
            qkv[0, :tokens, at] = rotate(query[:, at])
            qkv[1, :tokens, at] = rotate(keys[:, at])
            qkv[2, :tokens, at] = values[:, at]
        for pair in BOTH:
            at = slice(pair * LANES, (pair + 1) * LANES)
            for tile in BOTH:
                n_keys = (tile + 1) * q_tile
                q_pair = qkv[0, tile * q_tile:(tile + 1) * q_tile, at]
                k_pair, v_pair = qkv[1, :n_keys, at], qkv[2, :n_keys, at]
                row_id = lax.broadcasted_iota(jnp.int32, (q_tile, n_keys), 0) + tile * q_tile
                causal = row_id >= lax.broadcasted_iota(jnp.int32, (q_tile, n_keys), 1)
                outs = []
                for head in BOTH:
                    q_head = jnp.where(first_head if head == 0 else ~first_head, q_pair, jnp.zeros((), jnp.bfloat16))
                    scores = lax.dot_general(q_head, k_pair, LANES_BOTH, preferred_element_type=jnp.float32)
                    scores = jnp.where(causal, scores * scale, -1e30)
                    top = jnp.max(scores, axis=-1, keepdims=True)
                    weight = jnp.exp(scores - top)
                    probs = (weight * (1.0 / jnp.sum(weight, axis=-1, keepdims=True))).astype(jnp.bfloat16)
                    outs.append(jnp.dot(probs, v_pair, preferred_element_type=jnp.float32))
                out_cols = pl.ds(pl.multiple_of(g * group + pair * LANES, LANES), LANES)
                qkv[3, tile * q_tile:(tile + 1) * q_tile, out_cols] = jnp.where(first_head, outs[0], outs[1]).astype(jnp.bfloat16)
        return carry

    lax.fori_loop(0, d_model // group, group_body, 0)

    def out_body(g, carry):
        cols = pl.ds(pl.multiple_of(g * group, group), group)
        attn_out = jnp.dot(qkv[3, :tokens], weights[3, :d_model, cols], preferred_element_type=jnp.float32)
        hidden[:, cols] = (x_ref[:, cols].astype(jnp.float32) + attn_out).astype(jnp.bfloat16)
        return carry

    lax.fori_loop(0, d_model // group, out_body, 0)


def layer_kernel(head_dim, pad_cap,
                 idx_hbm, slot_hbm, gate_idx_hbm, attn_gain_hbm, moe_gain_hbm, x_hbm, rope_hbm, qkv_hbm, proj_hbm, gate_hbm, up_hbm, down_hbm,
                 out_ref, tok_hbm,
                 idx_ref, slot_ref, gate_ref, attn_gain_ref, moe_gain_ref, x_ref, rope, gate_act, big, gate_up, down_all, work, own_tok, hidden, inner, comb, y_buf, send_core, acc, got_core, got_x, got_y, got_last,
                 attn_send, attn_z_send, attn_z_recv, attn_direct, attn_partner, load_sems, tok_send, tok_direct, tok_partner, tok_sem, tok_load, small_sems,
                 z_own, z_pass, z_recv, core_send, core_recv, x_send, x_recv, y_send, y_recv, last_send, last_recv):
    place = layer_place()
    dx, dz, dy, dc = place
    tokens, d_model = x_ref.shape
    experts = own_tok.shape[0] - tokens
    n_exp, n_rows, ffn = inner.shape
    n_src = comb.shape[0]
    block_cols = acc.shape[-1]
    half_tok = tokens // 2
    n_sub = down_all.shape[1]
    chunks = n_exp + 1 + n_sub
    across_x, across_y, partner = related(place, 1, 0), related(place, 2, 0), related(place, 0, 1)
    upper = dz // 2
    inside = (dz == 1) | (dz == 2)
    at_end = (dz == 0) | (dz == 3)
    first_exp = dx * n_exp
    mine = slot_of(place)

    def at_z(z):
        return (dx, z, dy, dc)

    x_copy_in = pltpu.make_async_copy(x_hbm, x_ref, load_sems.at[0])
    rope_copy_in = pltpu.make_async_copy(rope_hbm, rope, load_sems.at[1])
    small_copies = [pltpu.make_async_copy(src, dst, small_sems.at[n]) for n, (src, dst) in enumerate(((idx_hbm, idx_ref), (slot_hbm, slot_ref), (gate_idx_hbm, gate_ref), (attn_gain_hbm, attn_gain_ref), (moe_gain_hbm, moe_gain_ref)))]
    for copy in [x_copy_in, rope_copy_in] + small_copies:
        copy.start()
    barrier = pltpu.get_barrier_semaphore()
    for target in [at_z((dz + step) % 4) for step in (1, 2, 3)] + [across_x, across_y, partner]:
        pl.semaphore_signal(barrier, inc=1, device_id=dev_id(target), device_id_type=MESH_ID)
    pl.semaphore_wait(barrier, 6)

    shard_rows = proj_hbm.shape[0]
    row_piece, col_piece = shard_rows // 8, d_model // 8

    def qkv_rows(start, rows, col_z=None):
        at = pl.ds(pl.multiple_of(start, rows), rows)
        if col_z is None:
            return qkv_hbm.at[:, at]
        return big.at[pl.ds(0, 3), at, pl.ds(pl.multiple_of(col_z * shard_rows, shard_rows), shard_rows)]

    def proj_rows(start, rows):
        return big.at[3, pl.ds(pl.multiple_of(start, rows), rows)]

    def size_of(halves):
        return big.at[0, pl.ds(0, halves * row_piece * 2)]

    z_steps = (1, 3, 2)
    for index, step in enumerate(z_steps):
        proj_src = proj_hbm.at[pl.ds(pl.multiple_of(mine * row_piece, row_piece), row_piece)]
        for src, dst in ((qkv_rows(mine * col_piece, col_piece), qkv_rows(mine * col_piece, col_piece, dz)), (proj_src, proj_rows(dz * shard_rows + mine * row_piece, row_piece))):
            remote(src, dst, attn_z_send.at[index], attn_z_recv.at[index], at_z((dz + step) % 4)).start()

    last_exp = n_exp - 1

    def chunk_refs(p, j):
        if j < last_exp:
            return [gate_up.at[p, j, m] for m in BOTH]
        if j <= n_exp:
            return [gate_up.at[p, last_exp, j - last_exp]]
        return [down_all.at[p, j - n_exp - 1]]

    def chunk_srcs(j):
        if j < last_exp:
            return [gate_hbm.at[first_exp + j], up_hbm.at[first_exp + j]]
        if j <= n_exp:
            return [(gate_hbm, up_hbm)[j - last_exp].at[first_exp + last_exp]]
        return [down_hbm.at[pl.ds(first_exp, n_exp), :, pl.ds((j - n_exp - 1) * block_cols, block_cols)]]

    def kind_of(j):
        return 0 if j <= n_exp else 1

    def own_copies(side, j):
        target = at_z(dz - 1 if side == 0 else dz + 1)
        return [remote(src, dst, z_own.at[side, kind_of(j)], z_recv.at[dz, j], target) for src, dst in zip(chunk_srcs(j), chunk_refs(dz, j))]

    def whole_chunk(p, j):
        return gate_up.at[p, j] if j < last_exp else chunk_refs(p, j)[0]

    def pass_copy(which, p, j, z):
        return remote(whole_chunk(p, j), whole_chunk(p, j), z_pass.at[which, kind_of(j)], z_recv.at[p, j], at_z(z))

    def wait_chunk(p, j):
        wait_in(whole_chunk(p, j), z_recv.at[p, j])

    end_z, mid_z, far_z = 3 * (dz - 1), 3 - dz, 3 * (2 - dz)
    passes = ((end_z, mid_z), (mid_z, end_z), (far_z, end_z))

    def send_own(j):
        @pl.when(dz > 0)
        def _():
            for copy in own_copies(0, j):
                copy.start()

        @pl.when(dz < 3)
        def _():
            for copy in own_copies(1, j):
                copy.start()

    def forward(kinds, js):
        @pl.when(inside)
        def _():
            for j in js:
                for which in kinds:
                    p, z = passes[which]
                    wait_chunk(p, j)
                    pass_copy(which, p, j, z).start()

    near, far, expert_js, down_js = BOTH, (2,), range(n_exp + 1), range(n_exp + 1, chunks)

    def need(j):
        @pl.when(at_end)
        def _():
            for k in range(3):
                wait_chunk(k + 1 - upper, j)

    for j in expert_js:
        send_own(j)
    own_loads = [
        (qkv_hbm, big.at[pl.ds(0, 3), pl.ds(0, d_model), pl.ds(pl.multiple_of(dz * shard_rows, shard_rows), shard_rows)], 2),
        (proj_hbm, proj_rows(dz * shard_rows, shard_rows), 2),
    ]
    for j in range(chunks):
        own_loads += [(src, dst, 3 + kind_of(j)) for src, dst in zip(chunk_srcs(j), chunk_refs(dz, j))]
    for src, dst, sem in own_loads:
        pltpu.make_async_copy(src, dst, load_sems.at[sem]).start()

    for copy in [x_copy_in] + small_copies:
        copy.wait()
    norm_rows(x_ref, attn_gain_ref, own_tok, tokens)

    expert_ids = lax.broadcasted_iota(jnp.int32, (experts, tokens), 0)
    slot_tab = jnp.zeros((experts, tokens), jnp.float32)
    gate_tab = jnp.zeros((experts, tokens), jnp.float32)
    for k in range(idx_ref.shape[0]):
        hit = expert_ids == idx_ref[k:k + 1, :]
        slot_tab = slot_tab + jnp.where(hit, slot_ref[k:k + 1, :].astype(jnp.float32) + 1.0, 0.0)
        gate_tab = gate_tab + jnp.where(hit, gate_ref[k:k + 1, :].astype(jnp.float32), 0.0)
    own_tok[tokens:, :tokens] = (slot_tab - 1.0).astype(jnp.bfloat16)
    own_tok[tokens:, tokens:] = gate_tab.astype(jnp.bfloat16)

    streams = []
    for index, step in enumerate(z_steps):
        source_z = (dz + 4 - step) % 4

        def part_refs(slot, half, source_z=source_z):
            cols, rows = col_piece // 2, row_piece // 2
            return [qkv_rows(slot * col_piece + half * cols, cols, source_z), proj_rows(source_z * shard_rows + slot * row_piece + half * rows, rows)]

        streams.append(spread_in_layer(place, functools.partial(part_refs, mine), part_refs, attn_send.at[index], attn_direct.at[index], attn_partner.at[index], size_of(1), size_of(8)))
    for index, stream in enumerate(streams):
        wait_in(size_of(2), attn_z_recv.at[index])
        next(stream)
    for _ in range(4):
        for stream in streams:
            next(stream)
    wait_in(size_of(16), load_sems.at[2])
    rope_copy_in.wait()

    attend(x_ref, own_tok, big, rope, work, hidden, head_dim)
    norm_rows(hidden, moe_gain_ref, own_tok, tokens)
    for index in range(3):
        wait_in(size_of(14), attn_send.at[index])
        wait_in(size_of(2), attn_z_send.at[index])

    half_rows = own_tok.shape[0] // 2

    def tok_part(slot, half):
        return [tok_hbm.at[slot, pl.ds(half * half_rows, half_rows)]]

    def tok_half(half):
        return [own_tok.at[pl.ds(half * half_rows, half_rows)]]

    stream = spread_in_layer(place, tok_half, tok_part, tok_send, tok_direct, tok_partner, tok_part(0, 0)[0], tok_hbm.at[pl.ds(0, 4)])
    next(stream)
    tok_copy = pltpu.make_async_copy(own_tok, tok_hbm.at[mine], tok_sem)
    tok_copy.start()
    forward(near, expert_js)
    for _ in range(4):
        next(stream)
    tok_copy.wait()
    wait_in(tok_hbm.at[pl.ds(0, 7)], tok_send)
    forward(far, expert_js)
    for j in down_js:
        send_own(j)

    def tok_in(s):
        return pltpu.make_async_copy(tok_hbm.at[s], work.at[s % 2], tok_load.at[s % 2])

    my_first = (lax.axis_index('ep') * 2 + dx) * n_exp
    pick_row = (lax.broadcasted_iota(jnp.int32, (8, experts), 1) == my_first + lax.broadcasted_iota(jnp.int32, (8, experts), 0)).astype(jnp.bfloat16)
    pick_col = (lax.broadcasted_iota(jnp.int32, (experts, LANES), 0) == my_first + lax.broadcasted_iota(jnp.int32, (experts, LANES), 1)).astype(jnp.bfloat16)
    tok_in(0).start()

    def dispatch_body(s, carry):
        @pl.when(s + 1 < n_src)
        def _():
            tok_in(s + 1).start()

        tok_in(s).wait()
        u = work[s % 2, :tokens]
        tables = work[s % 2, tokens:]
        slot_row = jnp.dot(pick_row, tables, preferred_element_type=jnp.float32)
        col_tab = lax.dot_general(tables, pick_col, (((0,), (0,)), ((), ())), preferred_element_type=jnp.float32)
        slot_ids = lax.broadcasted_iota(jnp.int32, (pad_cap, tokens), 0).astype(jnp.float32)
        rows = pl.ds(pl.multiple_of(s * pad_cap, pad_cap), pad_cap)
        for e in range(n_exp):
            one_hot = jnp.where(slot_ids == slot_row[e:e + 1, :tokens], 1.0, 0.0).astype(jnp.bfloat16)
            big[e, rows] = jnp.dot(one_hot, u, preferred_element_type=jnp.float32).astype(jnp.bfloat16)
        buf_ids = lax.broadcasted_iota(jnp.int32, (tokens, n_exp * pad_cap), 1).astype(jnp.float32)
        gates = jnp.zeros((tokens, n_exp * pad_cap), jnp.float32)
        for e in range(n_exp):
            slot_e = col_tab[:tokens, e:e + 1]
            dest_e = jnp.where(slot_e >= 0.0, slot_e + float(e * pad_cap), -1.0)
            gates = jnp.where(buf_ids == dest_e, col_tab[tokens:, e:e + 1], gates)
        comb[s] = gates.astype(jnp.bfloat16)
        return carry

    lax.fori_loop(0, n_src, dispatch_body, 0)

    row_tile = n_rows // 4

    def tile_loop(body):
        def tile_body(t, carry):
            body(pl.ds(pl.multiple_of(t * row_tile, row_tile), row_tile))
            return carry

        lax.fori_loop(0, 4, tile_body, 0)

    def product(e, m, at):
        return jnp.dot(big[e, at], gate_up[:, e, m].reshape(d_model, ffn), preferred_element_type=jnp.float32)

    def expert_inner(e):
        def body(at):
            gate = product(e, 0, at)
            inner[e, at] = (gate * jax.nn.sigmoid(gate) * product(e, 1, at)).astype(jnp.bfloat16)

        need(e)
        tile_loop(body)

    def last_gate(at):
        gate = product(last_exp, 0, at)
        gate_act[at] = gate * jax.nn.sigmoid(gate)

    def last_up(at):
        inner[last_exp, at] = (gate_act[at] * product(last_exp, 1, at)).astype(jnp.bfloat16)

    def block_of(i):
        k, sub = i // n_sub, i % n_sub
        if isinstance(i, int) and k == 0:
            return dz, sub
        near_end = dz + upper * (3 - 2 * dz)
        low = k - near_end * ((3 - k) // 2)
        return low + upper * (3 - 2 * low), sub

    def rel_slot(rel, core_rel):
        return toggled(dx, rel % 2) * 4 + toggled(dy, rel // 2) * 2 + flip(dc, core_rel)

    halves = (pl.ds(0, half_tok), pl.ds(half_tok, half_tok))

    def core_copy(i, rel):
        return remote(send_core.at[two(i), rel], got_core.at[two(i), rel], core_send.at[two(i), rel], core_recv.at[two(i), rel], partner)

    def x_copy(i, rel):
        where = (3 - rel) // 2
        return remote(acc.at[two(i), rel, halves[0]], got_x.at[three(i), where], x_send.at[three(i), where], x_recv.at[three(i), where], across_x)

    def y_copy(i, rel):
        where = 3 - rel
        return remote(acc.at[two(i), rel, halves[1]], got_y.at[three(i), where], y_send.at[three(i), where], y_recv.at[three(i), where], across_y)

    def last_copy(i, which):
        rel, target = ((2, across_y), (1, across_x))[which]
        return remote(acc.at[two(i), rel, halves[which]], got_last.at[three(i), which], last_send.at[three(i), which], last_recv.at[three(i), which], target)

    def wait_down(i):
        p, sub = block_of(i)
        if not (isinstance(i, int) and i < n_sub):
            @pl.when(at_end)
            def _():
                wait_in(down_all.at[p, sub], z_recv.at[p, n_exp + 1 + sub])

    def y_block(i, low=0, high=n_exp):
        p, sub = block_of(i)
        wait_down(i)

        def y_body(e, carry):
            y_tall = jnp.dot(inner[e], down_all[p, sub, e], preferred_element_type=jnp.float32).astype(jnp.bfloat16)
            at = pl.ds(pl.multiple_of(e * pad_cap, pad_cap), pad_cap)
            for s in range(n_src):
                y_buf[s, at] = y_tall[s * pad_cap:(s + 1) * pad_cap]
            return carry

        lax.fori_loop(low, high, y_body, 0)

    def sum_block(i, with_y=False):
        p, sub = block_of(i)

        def partial(rel, core_rel):
            slot = rel_slot(rel, core_rel)
            if with_y:
                rows = pl.ds(pl.multiple_of(slot * pad_cap, pad_cap), pad_cap)
                for e in range(n_exp):
                    y_buf[slot, e * pad_cap:(e + 1) * pad_cap] = jnp.dot(inner[e, rows], down_all[p, sub, e], preferred_element_type=jnp.float32).astype(jnp.bfloat16)
            return jnp.dot(comb[slot], y_buf[slot], preferred_element_type=jnp.float32)

        def core_body(k, carry):
            rel = 3 - k
            send_core[two(i), rel] = partial(rel, 1)
            core_copy(i, rel).start()
            return carry

        def own_body(k, carry):
            rel = 3 - k
            own = partial(rel, 0)
            wait_in(got_core.at[two(i), rel], core_recv.at[two(i), rel])
            acc[two(i), rel] = own + got_core[two(i), rel]

            @pl.when(rel % 2 == 1)
            def _():
                x_copy(i, rel).start()

            @pl.when(rel // 2 == 1)
            def _():
                y_copy(i, rel).start()

            return carry

        lax.fori_loop(0, 4, core_body, 0)
        lax.fori_loop(0, 4, own_body, 0)

    def turn_block(i):
        wait_in(got_x.at[three(i), 0], x_recv.at[three(i), 0])
        acc[two(i), 2, halves[0]] += got_x[three(i), 0]
        last_copy(i, 0).start()
        wait_in(got_y.at[three(i), 0], y_recv.at[three(i), 0])
        acc[two(i), 1, halves[1]] += got_y[three(i), 0]
        last_copy(i, 1).start()

    def end_block(i):
        p, sub = block_of(i)
        cols = pl.ds(pl.multiple_of((p * n_sub + sub) * block_cols, block_cols), block_cols)
        for half, got, got_sems in ((0, got_x, x_recv), (1, got_y, y_recv)):
            wait_in(got.at[three(i), 1], got_sems.at[three(i), 1])
            wait_in(got_last.at[three(i), half], last_recv.at[three(i), half])
            total = acc[two(i), 0, halves[half]] + got[three(i), 1] + got_last[three(i), half]
            out_ref[halves[half], cols] = (hidden[halves[half], cols].astype(jnp.float32) + total).astype(jnp.bfloat16)
        for rel in range(4):
            core_copy(i, rel).wait_send()
        for rel in (3, 1):
            x_copy(i, rel).wait_send()
        for rel in (3, 2):
            y_copy(i, rel).wait_send()
        for which in BOTH:
            last_copy(i, which).wait_send()

    wait_in(gate_up.at[0], load_sems.at[3])
    wait_in(down_all.at[0], load_sems.at[4])
    for e in range(last_exp):
        expert_inner(e)
    y_block(0, 0, last_exp)
    need(last_exp)
    tile_loop(last_gate)
    need(n_exp)
    tile_loop(last_up)

    blocks = 4 * n_sub
    y_block(0, last_exp, n_exp)
    sum_block(0)
    forward(near, down_js)
    y_block(1)
    turn_block(0)
    sum_block(1)
    end_block(0)
    y_block(2)
    turn_block(1)
    sum_block(2)
    forward(far, down_js)
    end_block(1)

    def block_body(i, carry):
        y_block(i + 1)
        turn_block(i)
        sum_block(i + 1)
        end_block(i)
        return carry

    lax.fori_loop(2, blocks - 3, block_body, 0)

    turn_block(blocks - 3)
    y_block(blocks - 2)
    sum_block(blocks - 2)
    end_block(blocks - 3)
    turn_block(blocks - 2)
    wait_down(blocks - 1)
    sum_block(blocks - 1, with_y=True)
    end_block(blocks - 2)
    turn_block(blocks - 1)
    end_block(blocks - 1)

    for kind, size in ((0, gate_up.at[0]), (1, down_all.at[0])):
        @pl.when(dz > 0)
        def _():
            wait_in(size, z_own.at[0, kind])

        @pl.when(dz < 3)
        def _():
            wait_in(size, z_own.at[1, kind])

        @pl.when(inside)
        def _():
            for which in range(3):
                wait_in(size, z_pass.at[which, kind])


def whole_layer(head_dim, pad_cap, x, idx_t, slot_t, gate_t, attn_gain, moe_gain, qkv, proj, gate_w, up_w, down_w, experts):
    tokens, d_model = x.shape
    n_exp = gate_w.shape[0] // 2
    part_depth, ffn = gate_w.shape[1:]
    parts, n_src, block_cols = 4, 8, LANES
    n_sub = down_w.shape[2] // block_cols
    chunks = n_exp + 1 + n_sub
    n_rows = n_src * pad_cap
    half = tokens // 2
    rope = np.stack(rope_tables(tokens, head_dim))
    dma = pltpu.SemaphoreType.DMA
    bf16, f32 = jnp.bfloat16, jnp.float32
    hbm = pl.BlockSpec(memory_space=pl.ANY)
    return pl.pallas_call(
        functools.partial(layer_kernel, head_dim, pad_cap),
        out_shape=(pltpu.VMEM(x.shape, bf16), jax.ShapeDtypeStruct((n_src, tokens + experts, d_model), bf16)),
        in_specs=[hbm] * 12,
        out_specs=(pl.BlockSpec(memory_space=pltpu.VMEM), hbm),
        scratch_shapes=[
            *(pltpu.VMEM(small.shape, small.dtype) for small in (idx_t, slot_t, gate_t, attn_gain, moe_gain)),
            pltpu.VMEM((tokens, d_model), bf16),
            pltpu.VMEM(rope.shape, f32),
            pltpu.VMEM((n_rows, ffn), f32),
            pltpu.VMEM((n_exp, n_rows, d_model), bf16),
            pltpu.VMEM((parts, n_exp, 2, part_depth, ffn), bf16),
            pltpu.VMEM((parts, n_sub, n_exp, ffn, block_cols), bf16),
            pltpu.VMEM((4, tokens + experts, d_model), bf16),
            pltpu.VMEM((tokens + experts, d_model), bf16),
            pltpu.VMEM((tokens, d_model), bf16),
            pltpu.VMEM((n_exp, n_rows, ffn), bf16),
            pltpu.VMEM((n_src, tokens, n_exp * pad_cap), bf16),
            pltpu.VMEM((n_src, n_exp * pad_cap, block_cols), bf16),
            *[pltpu.VMEM((2, 4, tokens, block_cols), f32)] * 3,
            *[pltpu.VMEM((3, 2, half, block_cols), f32)] * 3,
            *[dma((3,))] * 3, dma((3, 3, 2)), dma((3,)), dma((5,)),
            dma, dma((3, 2)), dma, dma, dma((2,)), dma((5,)),
            dma((2, 2)), dma((3, 2)), dma((parts, chunks)), dma((2, 4)), dma((2, 4)),
            *[dma((3, 2))] * 6,
        ],
        compiler_params=pltpu.CompilerParams(collective_id=1, has_side_effects=True, vmem_limit_bytes=60 * 1024 * 1024),
        cost_estimate=pl.CostEstimate(flops=40_000_000_000, bytes_accessed=30_000_000, transcendentals=0),
        name='whole_layer',
    )(idx_t, slot_t, gate_t, attn_gain, moe_gain, x, rope, qkv, proj, gate_w, up_w, down_w)[0]


def solution(mesh):
    tok_spec = P(('data', 'fsdp', 'ep'), None, None)
    ep_count = mesh.shape['ep']

    def local_step(x_blk, idx_blk, slot_blk, gate_blk, attn_gain, qkv_shard, out_shard, moe_gain, gate_shard, up_shard, down_shard):
        batch_rows, seq_len, d_model = x_blk.shape
        tokens = batch_rows * seq_len
        top_k = idx_blk.shape[-1]
        head_dim = qkv_shard.shape[3]
        experts = gate_shard.shape[0] * ep_count
        capacity = capacity_of(tokens, top_k, experts)
        pad_cap = 16 * ((capacity + 15) // 16)
        by_choice = [blk.reshape(tokens, top_k).T for blk in (idx_blk, slot_blk, gate_blk)]
        qkv = qkv_shard.transpose(1, 2, 3, 0).reshape(3, d_model, -1)
        proj = out_shard.reshape(-1, d_model)
        result = whole_layer(head_dim, pad_cap, x_blk.reshape(tokens, d_model), *by_choice, attn_gain, moe_gain, qkv, proj, gate_shard, up_shard, down_shard, experts)
        return result.reshape(batch_rows, seq_len, d_model)

    return jax.shard_map(local_step, mesh=mesh, in_specs=(tok_spec, tok_spec, tok_spec, tok_spec, P(None), P('fsdp', None, None, None), P('fsdp', None, None), P(None), P('ep', 'fsdp', None), P('ep', 'fsdp', None), P('ep', None, 'fsdp')), out_specs=tok_spec, check_vma=False)
```

```python
import functools

import jax
import jax.numpy as jnp
import numpy as np
from jax import lax
from jax.experimental import pallas as pl
from jax.experimental.pallas import tpu as pltpu
from jax.sharding import PartitionSpec as P

NORM_EPS = 1e-6
ROPE_BASE = 10000.0
MESH_ID = pl.DeviceIdType.MESH
LANES = 128
BOTH = (0, 1)
LANES_BOTH = (((1,), (1,)), ((), ()))


def capacity_of(tok_count, top_k, experts):
    return 8 * ((5 * tok_count * top_k) // (32 * experts) + 1)


def rope_tables(seq_len, head_dim):
    half = head_dim // 2
    lane = np.arange(LANES)
    inv_freq = ROPE_BASE ** (-(lane % half) / half)
    angles = np.arange(seq_len)[:, None] * inv_freq[None, :]
    sign = np.where(lane % head_dim < half, -1.0, 1.0)
    return np.cos(angles).astype(np.float32), (np.sin(angles) * sign).astype(np.float32)


def two(i):
    return i % 2


def three(i):
    return i % 3


def layer_place():
    dx, dz, ep = lax.axis_index('data'), lax.axis_index('fsdp'), lax.axis_index('ep')
    return dx, dz, ep // 2, ep % 2


def flip(pos, bit):
    return (1 - pos) if bit else pos


def toggled(pos, bit):
    return pos + bit - 2 * pos * bit


def related(place, chip_rel, core_rel):
    dx, dz, dy, dc = place
    return flip(dx, chip_rel & 1), dz, flip(dy, chip_rel & 2), flip(dc, core_rel)


def slot_of(place):
    dx, _, dy, dc = place
    return dx * 4 + dy * 2 + dc


def dev_id(place):
    dx, dz, dy, dc = place
    return (dx, dz, dy * 2 + dc)


def remote(src, dst, send_sem, recv_sem, where):
    return pltpu.make_async_remote_copy(src_ref=src, dst_ref=dst, send_sem=send_sem, recv_sem=recv_sem, device_id=dev_id(where), device_id_type=MESH_ID)


def run_if(cond, body):
    if not isinstance(cond, bool):
        pl.when(cond)(body)
    elif cond:
        body()


def wait_in(ref, sem):
    pltpu.make_async_copy(ref, ref, sem).wait()


def spread_in_layer(place, own_refs, part_refs, send_sem, direct_sems, partner_sem, half_size, partner_size):
    across_x, across_y, partner = related(place, 1, 0), related(place, 2, 0), related(place, 0, 1)

    def pass_on(chip_rel, half, target, sem, first=False):
        owner = slot_of(related(place, chip_rel, 0))
        dsts = part_refs(owner, half)
        for src, dst in zip(own_refs(half) if first else dsts, dsts):
            remote(src, dst, send_sem, sem, target).start()

    def direct(rel_there, half):
        return direct_sems.at[rel_there - 1, half]

    for half in BOTH:
        pass_on(0, half, across_x, direct(1, half), True)
        pass_on(0, 1 - half, across_y, direct(2, 1 - half), True)
    for half in BOTH:
        pass_on(0, half, partner, partner_sem, True)
    yield

    def arrived(chip_rel, half):
        wait_in(half_size, direct(chip_rel, half))

    arrived(1, 0)
    pass_on(1, 0, across_y, direct(3, 0))
    pass_on(1, 0, partner, partner_sem)
    arrived(2, 1)
    pass_on(2, 1, across_x, direct(3, 1))
    pass_on(2, 1, partner, partner_sem)
    yield
    arrived(1, 1)
    pass_on(1, 1, partner, partner_sem)
    arrived(2, 0)
    pass_on(2, 0, partner, partner_sem)
    yield
    arrived(3, 0)
    pass_on(3, 0, partner, partner_sem)
    arrived(3, 1)
    pass_on(3, 1, partner, partner_sem)
    yield
    wait_in(partner_size, partner_sem)
    yield


def norm_rows(src, gain_ref, dst, rows):
    tile = 128
    gain = gain_ref[...].astype(jnp.float32).reshape(1, -1)

    def body(t, carry):
        at = pl.ds(pl.multiple_of(t * tile, tile), tile)
        wide = src[at].astype(jnp.float32)
        inv_rms = lax.rsqrt(jnp.mean(wide * wide, axis=-1, keepdims=True) + NORM_EPS)
        dst[at] = (wide * inv_rms * gain).astype(jnp.bfloat16)
        return carry

    lax.fori_loop(0, rows // tile, body, 0)


def attend(x_ref, normed, weights, rope, qkv, hidden, head_dim):
    tokens, d_model = x_ref.shape
    lane = lax.broadcasted_iota(jnp.int32, (tokens, LANES), 1)
    low_half = lane % head_dim < head_dim // 2
    first_head = lax.broadcasted_iota(jnp.int32, (tokens // 2, LANES), 1) < head_dim
    group = 2 * LANES
    q_tile = tokens // 2
    scale = head_dim ** -0.5

    def rotate(val):
        swapped = jnp.where(low_half, pltpu.roll(val, LANES - head_dim // 2, 1), pltpu.roll(val, head_dim // 2, 1))
        return (val * rope[0] + swapped * rope[1]).astype(jnp.bfloat16)

    def project(b, cols):
        return lax.dot_general(normed[:tokens], weights[b, cols, :], LANES_BOTH, preferred_element_type=jnp.float32)

    def group_body(g, carry):
        cols = pl.ds(pl.multiple_of(g * group, group), group)
        query, keys = project(0, cols), project(1, cols)
        values = project(2, cols).astype(jnp.bfloat16)
        for pair in BOTH:
            at = slice(pair * LANES, (pair + 1) * LANES)
            qkv[0, :tokens, at] = rotate(query[:, at])
            qkv[1, :tokens, at] = rotate(keys[:, at])
            qkv[2, :tokens, at] = values[:, at]
        for pair in BOTH:
            at = slice(pair * LANES, (pair + 1) * LANES)
            for tile in BOTH:
                n_keys = (tile + 1) * q_tile
                q_pair = qkv[0, tile * q_tile:(tile + 1) * q_tile, at]
                k_pair, v_pair = qkv[1, :n_keys, at], qkv[2, :n_keys, at]
                row_id = lax.broadcasted_iota(jnp.int32, (q_tile, n_keys), 0) + tile * q_tile
                causal = row_id >= lax.broadcasted_iota(jnp.int32, (q_tile, n_keys), 1)
                outs = []
                for head in BOTH:
                    q_head = jnp.where(first_head if head == 0 else ~first_head, q_pair, jnp.zeros((), jnp.bfloat16))
                    scores = lax.dot_general(q_head, k_pair, LANES_BOTH, preferred_element_type=jnp.float32)
                    scores = jnp.where(causal, scores * scale, -1e30)
                    top = jnp.max(scores, axis=-1, keepdims=True)
                    weight = jnp.exp(scores - top)
                    probs = (weight * (1.0 / jnp.sum(weight, axis=-1, keepdims=True))).astype(jnp.bfloat16)
                    outs.append(jnp.dot(probs, v_pair, preferred_element_type=jnp.float32))
                out_cols = pl.ds(pl.multiple_of(g * group + pair * LANES, LANES), LANES)
                qkv[3, tile * q_tile:(tile + 1) * q_tile, out_cols] = jnp.where(first_head, outs[0], outs[1]).astype(jnp.bfloat16)
        return carry

    lax.fori_loop(0, d_model // group, group_body, 0)

    def out_body(g, carry):
        cols = pl.ds(pl.multiple_of(g * group, group), group)
        attn_out = jnp.dot(qkv[3, :tokens], weights[3, :d_model, cols], preferred_element_type=jnp.float32)
        hidden[:, cols] = (x_ref[:, cols].astype(jnp.float32) + attn_out).astype(jnp.bfloat16)
        return carry

    lax.fori_loop(0, d_model // group, out_body, 0)


def layer_kernel(head_dim, pad_cap,
                 idx_hbm, slot_hbm, gate_idx_hbm, attn_gain_hbm, moe_gain_hbm, x_hbm, rope_hbm, qkv_hbm, proj_hbm, gate_hbm, up_hbm, down_hbm,
                 out_ref, tok_hbm,
                 idx_ref, slot_ref, gate_ref, attn_gain_ref, moe_gain_ref, x_ref, rope, gate_act, big, gate_up, down_all, work, own_tok, hidden, inner, comb, y_buf, send_core, acc, got_core, got_x, got_y, got_last,
                 attn_z_recv, attn_direct, attn_partner, tok_direct, tok_partner,
                 z_own, z_pass, z_recv, core_send, core_recv, x_send, y_send, last_send):
    place = layer_place()
    dx, dz, dy, dc = place
    tokens, d_model = x_ref.shape
    x_recv, y_recv, last_recv = [attn_direct.at[n] for n in range(3)]
    load_sems = [x_send.at[n // 2, n % 2] for n in range(5)]
    small_sems = [core_send.at[n // 4, n % 4] for n in range(5)]
    attn_send, attn_z_send = [[last_send.at[n, m] for n in range(3)] for m in BOTH]
    tok_send, tok_sem, tok_load = y_send.at[0, 0], y_send.at[0, 1], y_send.at[1]
    experts = own_tok.shape[0] - tokens
    n_exp, n_rows, ffn = inner.shape
    n_src = comb.shape[0]
    block_cols = acc.shape[-1]
    half_tok = tokens // 2
    n_sub = down_all.shape[1]
    chunks = n_exp + 1 + n_sub
    across_x, across_y, partner = related(place, 1, 0), related(place, 2, 0), related(place, 0, 1)
    upper = dz // 2
    inside = (dz == 1) | (dz == 2)
    at_end = (dz == 0) | (dz == 3)
    first_exp = dx * n_exp
    mine = slot_of(place)

    def at_z(z):
        return (dx, z, dy, dc)

    x_copy_in = pltpu.make_async_copy(x_hbm, x_ref, load_sems[0])
    rope_copy_in = pltpu.make_async_copy(rope_hbm, rope, load_sems[1])
    small_copies = [pltpu.make_async_copy(src, dst, small_sems[n]) for n, (src, dst) in enumerate(((idx_hbm, idx_ref), (slot_hbm, slot_ref), (gate_idx_hbm, gate_ref), (attn_gain_hbm, attn_gain_ref), (moe_gain_hbm, moe_gain_ref)))]
    for copy in [x_copy_in, rope_copy_in] + small_copies:
        copy.start()
    barrier = pltpu.get_barrier_semaphore()
    for target in [at_z((dz + step) % 4) for step in (1, 2, 3)] + [across_x, across_y, partner]:
        pl.semaphore_signal(barrier, inc=1, device_id=dev_id(target), device_id_type=MESH_ID)
    pl.semaphore_wait(barrier, 6)

    shard_rows = proj_hbm.shape[0]
    row_piece, col_piece = shard_rows // 8, d_model // 8

    def qkv_rows(start, rows, col_z=None):
        at = pl.ds(pl.multiple_of(start, rows), rows)
        if col_z is None:
            return qkv_hbm.at[:, at]
        return big.at[pl.ds(0, 3), at, pl.ds(pl.multiple_of(col_z * shard_rows, shard_rows), shard_rows)]

    def proj_rows(start, rows):
        return big.at[3, pl.ds(pl.multiple_of(start, rows), rows)]

    def size_of(halves):
        return big.at[0, pl.ds(0, halves * row_piece * 2)]

    z_steps = (1, 3, 2)
    for index, step in enumerate(z_steps):
        proj_src = proj_hbm.at[pl.ds(pl.multiple_of(mine * row_piece, row_piece), row_piece)]
        for src, dst in ((qkv_rows(mine * col_piece, col_piece), qkv_rows(mine * col_piece, col_piece, dz)), (proj_src, proj_rows(dz * shard_rows + mine * row_piece, row_piece))):
            remote(src, dst, attn_z_send[index], attn_z_recv.at[index], at_z((dz + step) % 4)).start()

    last_exp = n_exp - 1

    def chunk_refs(p, j):
        if j < last_exp:
            return [gate_up.at[p, j, m] for m in BOTH]
        if j <= n_exp:
            return [gate_up.at[p, last_exp, j - last_exp]]
        return [down_all.at[p, j - n_exp - 1]]

    def chunk_srcs(j):
        if j < last_exp:
            return [gate_hbm.at[first_exp + j], up_hbm.at[first_exp + j]]
        if j <= n_exp:
            return [(gate_hbm, up_hbm)[j - last_exp].at[first_exp + last_exp]]
        return [down_hbm.at[pl.ds(first_exp, n_exp), :, pl.ds((j - n_exp - 1) * block_cols, block_cols)]]

    def kind_of(j):
        return 0 if j <= n_exp else 1

    def own_copies(side, j):
        target = at_z(dz - 1 if side == 0 else dz + 1)
        return [remote(src, dst, z_own.at[side, kind_of(j)], z_recv.at[dz, j], target) for src, dst in zip(chunk_srcs(j), chunk_refs(dz, j))]

    def whole_chunk(p, j):
        return gate_up.at[p, j] if j < last_exp else chunk_refs(p, j)[0]

    def pass_copy(which, p, j, z):
        return remote(whole_chunk(p, j), whole_chunk(p, j), z_pass.at[which, kind_of(j)], z_recv.at[p, j], at_z(z))

    def wait_chunk(p, j):
        wait_in(whole_chunk(p, j), z_recv.at[p, j])

    end_z, mid_z, far_z = 3 * (dz - 1), 3 - dz, 3 * (2 - dz)
    passes = ((end_z, mid_z), (mid_z, end_z), (far_z, end_z))

    def send_own(j):
        @pl.when(dz > 0)
        def _():
            for copy in own_copies(0, j):
                copy.start()

        @pl.when(dz < 3)
        def _():
            for copy in own_copies(1, j):
                copy.start()

    def forward(kinds, js):
        @pl.when(inside)
        def _():
            for j in js:
                for which in kinds:
                    p, z = passes[which]
                    wait_chunk(p, j)
                    pass_copy(which, p, j, z).start()

    near, far, expert_js, down_js = BOTH, (2,), range(n_exp + 1), range(n_exp + 1, chunks)

    def need(j):
        @pl.when(at_end)
        def _():
            for k in range(3):
                wait_chunk(k + 1 - upper, j)

    for j in expert_js:
        send_own(j)
    own_loads = [
        (qkv_hbm, big.at[pl.ds(0, 3), pl.ds(0, d_model), pl.ds(pl.multiple_of(dz * shard_rows, shard_rows), shard_rows)], 2),
        (proj_hbm, proj_rows(dz * shard_rows, shard_rows), 2),
    ]
    for j in range(chunks):
        own_loads += [(src, dst, 3 + kind_of(j)) for src, dst in zip(chunk_srcs(j), chunk_refs(dz, j))]
    for src, dst, sem in own_loads:
        pltpu.make_async_copy(src, dst, load_sems[sem]).start()

    for copy in [x_copy_in] + small_copies:
        copy.wait()
    norm_rows(x_ref, attn_gain_ref, own_tok, tokens)

    expert_ids = lax.broadcasted_iota(jnp.int32, (experts, tokens), 0)
    slot_tab = jnp.zeros((experts, tokens), jnp.float32)
    gate_tab = jnp.zeros((experts, tokens), jnp.float32)
    for k in range(idx_ref.shape[0]):
        hit = expert_ids == idx_ref[k:k + 1, :]
        slot_tab = slot_tab + jnp.where(hit, slot_ref[k:k + 1, :].astype(jnp.float32) + 1.0, 0.0)
        gate_tab = gate_tab + jnp.where(hit, gate_ref[k:k + 1, :].astype(jnp.float32), 0.0)
    own_tok[tokens:, :tokens] = (slot_tab - 1.0).astype(jnp.bfloat16)
    own_tok[tokens:, tokens:] = gate_tab.astype(jnp.bfloat16)

    streams = []
    for index, step in enumerate(z_steps):
        source_z = (dz + 4 - step) % 4

        def part_refs(slot, half, source_z=source_z):
            cols, rows = col_piece // 2, row_piece // 2
            return [qkv_rows(slot * col_piece + half * cols, cols, source_z), proj_rows(source_z * shard_rows + slot * row_piece + half * rows, rows)]

        streams.append(spread_in_layer(place, functools.partial(part_refs, mine), part_refs, attn_send[index], attn_direct.at[index], attn_partner.at[index], size_of(1), size_of(8)))
    for index, stream in enumerate(streams):
        wait_in(size_of(2), attn_z_recv.at[index])
        next(stream)
    for _ in range(4):
        for stream in streams:
            next(stream)
    wait_in(size_of(16), load_sems[2])
    rope_copy_in.wait()

    attend(x_ref, own_tok, big, rope, work, hidden, head_dim)
    norm_rows(hidden, moe_gain_ref, own_tok, tokens)
    for index in range(3):
        wait_in(size_of(14), attn_send[index])
        wait_in(size_of(2), attn_z_send[index])

    half_rows = own_tok.shape[0] // 2

    def tok_part(slot, half):
        return [tok_hbm.at[slot, pl.ds(half * half_rows, half_rows)]]

    def tok_half(half):
        return [own_tok.at[pl.ds(half * half_rows, half_rows)]]

    stream = spread_in_layer(place, tok_half, tok_part, tok_send, tok_direct, tok_partner, tok_part(0, 0)[0], tok_hbm.at[pl.ds(0, 4)])
    next(stream)
    tok_copy = pltpu.make_async_copy(own_tok, tok_hbm.at[mine], tok_sem)
    tok_copy.start()
    forward(near, expert_js)
    for _ in range(4):
        next(stream)
    tok_copy.wait()
    wait_in(tok_hbm.at[pl.ds(0, 7)], tok_send)
    forward(far, expert_js)
    for j in down_js:
        send_own(j)

    def tok_in(s):
        return pltpu.make_async_copy(tok_hbm.at[s], work.at[s % 2], tok_load.at[s % 2])

    my_first = (lax.axis_index('ep') * 2 + dx) * n_exp
    pick_row = (lax.broadcasted_iota(jnp.int32, (8, experts), 1) == my_first + lax.broadcasted_iota(jnp.int32, (8, experts), 0)).astype(jnp.bfloat16)
    pick_col = (lax.broadcasted_iota(jnp.int32, (experts, LANES), 0) == my_first + lax.broadcasted_iota(jnp.int32, (experts, LANES), 1)).astype(jnp.bfloat16)
    tok_in(0).start()

    def dispatch_body(s, carry):
        @pl.when(s + 1 < n_src)
        def _():
            tok_in(s + 1).start()

        tok_in(s).wait()
        u = work[s % 2, :tokens]
        tables = work[s % 2, tokens:]
        slot_row = jnp.dot(pick_row, tables, preferred_element_type=jnp.float32)
        col_tab = lax.dot_general(tables, pick_col, (((0,), (0,)), ((), ())), preferred_element_type=jnp.float32)
        slot_ids = lax.broadcasted_iota(jnp.int32, (pad_cap, tokens), 0).astype(jnp.float32)
        rows = pl.ds(pl.multiple_of(s * pad_cap, pad_cap), pad_cap)
        for e in range(n_exp):
            one_hot = jnp.where(slot_ids == slot_row[e:e + 1, :tokens], 1.0, 0.0).astype(jnp.bfloat16)
            big[e, rows] = jnp.dot(one_hot, u, preferred_element_type=jnp.float32).astype(jnp.bfloat16)
        buf_ids = lax.broadcasted_iota(jnp.int32, (tokens, n_exp * pad_cap), 1).astype(jnp.float32)
        gates = jnp.zeros((tokens, n_exp * pad_cap), jnp.float32)
        for e in range(n_exp):
            slot_e = col_tab[:tokens, e:e + 1]
            dest_e = jnp.where(slot_e >= 0.0, slot_e + float(e * pad_cap), -1.0)
            gates = jnp.where(buf_ids == dest_e, col_tab[tokens:, e:e + 1], gates)
        comb[s] = gates.astype(jnp.bfloat16)
        return carry

    lax.fori_loop(0, n_src, dispatch_body, 0)

    row_tile = n_rows // 4

    def tile_loop(body):
        def tile_body(t, carry):
            body(pl.ds(pl.multiple_of(t * row_tile, row_tile), row_tile))
            return carry

        lax.fori_loop(0, 4, tile_body, 0)

    def product(e, m, at):
        return jnp.dot(big[e, at], gate_up[:, e, m].reshape(d_model, ffn), preferred_element_type=jnp.float32)

    def expert_inner(e):
        def body(at):
            gate = product(e, 0, at)
            inner[e, at] = (gate * jax.nn.sigmoid(gate) * product(e, 1, at)).astype(jnp.bfloat16)

        need(e)
        tile_loop(body)

    def last_gate(at):
        gate = product(last_exp, 0, at)
        gate_act[at] = gate * jax.nn.sigmoid(gate)

    def last_up(at):
        inner[last_exp, at] = (gate_act[at] * product(last_exp, 1, at)).astype(jnp.bfloat16)

    def block_of(i):
        k, sub = i // n_sub, i % n_sub
        if isinstance(i, int) and k == 0:
            return dz, sub
        near_end = dz + upper * (3 - 2 * dz)
        low = k - near_end * ((3 - k) // 2)
        return low + upper * (3 - 2 * low), sub

    def rel_slot(rel, core_rel):
        return toggled(dx, rel % 2) * 4 + toggled(dy, rel // 2) * 2 + flip(dc, core_rel)

    halves = (pl.ds(0, half_tok), pl.ds(half_tok, half_tok))

    def core_copy(i, rel):
        return remote(send_core.at[two(i), rel], got_core.at[two(i), rel], core_send.at[two(i), rel], core_recv.at[two(i), rel], partner)

    def x_copy(i, rel):
        where = (3 - rel) // 2
        return remote(acc.at[two(i), rel, halves[0]], got_x.at[three(i), where], x_send.at[three(i), where], x_recv.at[three(i), where], across_x)

    def y_copy(i, rel):
        where = 3 - rel
        return remote(acc.at[two(i), rel, halves[1]], got_y.at[three(i), where], y_send.at[three(i), where], y_recv.at[three(i), where], across_y)

    def last_copy(i, which):
        rel, target = ((2, across_y), (1, across_x))[which]
        return remote(acc.at[two(i), rel, halves[which]], got_last.at[three(i), which], last_send.at[three(i), which], last_recv.at[three(i), which], target)

    def wait_down(i):
        p, sub = block_of(i)
        if not (isinstance(i, int) and i < n_sub):
            @pl.when(at_end)
            def _():
                wait_in(down_all.at[p, sub], z_recv.at[p, n_exp + 1 + sub])

    def y_block(i, low=0, high=n_exp):
        p, sub = block_of(i)
        wait_down(i)

        def y_body(e, carry):
            y_tall = jnp.dot(inner[e], down_all[p, sub, e], preferred_element_type=jnp.float32).astype(jnp.bfloat16)
            at = pl.ds(pl.multiple_of(e * pad_cap, pad_cap), pad_cap)
            for s in range(n_src):
                y_buf[s, at] = y_tall[s * pad_cap:(s + 1) * pad_cap]
            return carry

        lax.fori_loop(low, high, y_body, 0)

    def sum_block(i, with_y=False):
        p, sub = block_of(i)

        def partial(rel, core_rel):
            slot = rel_slot(rel, core_rel)
            if with_y:
                rows = pl.ds(pl.multiple_of(slot * pad_cap, pad_cap), pad_cap)
                for e in range(n_exp):
                    y_buf[slot, e * pad_cap:(e + 1) * pad_cap] = jnp.dot(inner[e, rows], down_all[p, sub, e], preferred_element_type=jnp.float32).astype(jnp.bfloat16)
            return jnp.dot(comb[slot], y_buf[slot], preferred_element_type=jnp.float32)

        def core_body(k, carry):
            rel = 3 - k
            send_core[two(i), rel] = partial(rel, 1)
            core_copy(i, rel).start()
            return carry

        def own_body(k, carry):
            rel = 3 - k
            own = partial(rel, 0)
            wait_in(got_core.at[two(i), rel], core_recv.at[two(i), rel])
            acc[two(i), rel] = own + got_core[two(i), rel]

            run_if(rel % 2 == 1, lambda: x_copy(i, rel).start())
            run_if(rel // 2 == 1, lambda: y_copy(i, rel).start())

            return carry

        if with_y:
            lax.fori_loop(0, 3, core_body, 0)
            own_body(0, 0)
            core_body(3, 0)
            lax.fori_loop(1, 4, own_body, 0)
        else:
            lax.fori_loop(0, 4, core_body, 0)
            lax.fori_loop(0, 4, own_body, 0)

    def turn_block(i):
        wait_in(got_x.at[three(i), 0], x_recv.at[three(i), 0])
        acc[two(i), 2, halves[0]] += got_x[three(i), 0]
        last_copy(i, 0).start()
        wait_in(got_y.at[three(i), 0], y_recv.at[three(i), 0])
        acc[two(i), 1, halves[1]] += got_y[three(i), 0]
        last_copy(i, 1).start()

    def end_block(i):
        p, sub = block_of(i)
        cols = pl.ds(pl.multiple_of((p * n_sub + sub) * block_cols, block_cols), block_cols)
        for half, got, got_sems in ((0, got_x, x_recv), (1, got_y, y_recv)):
            wait_in(got.at[three(i), 1], got_sems.at[three(i), 1])
            wait_in(got_last.at[three(i), half], last_recv.at[three(i), half])
            total = acc[two(i), 0, halves[half]] + got[three(i), 1] + got_last[three(i), half]
            out_ref[halves[half], cols] = (hidden[halves[half], cols].astype(jnp.float32) + total).astype(jnp.bfloat16)
        for rel in range(4):
            core_copy(i, rel).wait_send()
        for rel in (3, 1):
            x_copy(i, rel).wait_send()
        for rel in (3, 2):
            y_copy(i, rel).wait_send()
        for which in BOTH:
            last_copy(i, which).wait_send()

    wait_in(gate_up.at[0], load_sems[3])
    wait_in(down_all.at[0], load_sems[4])
    for e in range(last_exp):
        expert_inner(e)
    y_block(0, 0, last_exp)
    need(last_exp)
    tile_loop(last_gate)
    need(n_exp)
    tile_loop(last_up)

    blocks = 4 * n_sub
    y_block(0, last_exp, n_exp)
    sum_block(0)
    forward(near, down_js)
    y_block(1)
    turn_block(0)
    sum_block(1)
    end_block(0)
    y_block(2)
    turn_block(1)
    sum_block(2)
    forward(far, down_js)
    end_block(1)

    def block_body(i, carry):
        y_block(i + 1)
        turn_block(i)
        sum_block(i + 1)
        end_block(i)
        return carry

    lax.fori_loop(2, blocks - 3, block_body, 0)

    turn_block(blocks - 3)
    y_block(blocks - 2)
    sum_block(blocks - 2)
    end_block(blocks - 3)
    turn_block(blocks - 2)
    wait_down(blocks - 1)
    sum_block(blocks - 1, with_y=True)
    end_block(blocks - 2)
    turn_block(blocks - 1)
    end_block(blocks - 1)

    for kind, size in ((0, gate_up.at[0]), (1, down_all.at[0])):
        @pl.when(dz > 0)
        def _():
            wait_in(size, z_own.at[0, kind])

        @pl.when(dz < 3)
        def _():
            wait_in(size, z_own.at[1, kind])

        @pl.when(inside)
        def _():
            for which in range(3):
                wait_in(size, z_pass.at[which, kind])


def whole_layer(head_dim, pad_cap, x, idx_t, slot_t, gate_t, attn_gain, moe_gain, qkv, proj, gate_w, up_w, down_w, experts):
    tokens, d_model = x.shape
    n_exp = gate_w.shape[0] // 2
    part_depth, ffn = gate_w.shape[1:]
    parts, n_src, block_cols = 4, 8, LANES
    n_sub = down_w.shape[2] // block_cols
    chunks = n_exp + 1 + n_sub
    n_rows = n_src * pad_cap
    half = tokens // 2
    rope = np.stack(rope_tables(tokens, head_dim))
    dma = pltpu.SemaphoreType.DMA
    bf16, f32 = jnp.bfloat16, jnp.float32
    hbm = pl.BlockSpec(memory_space=pl.ANY)
    return pl.pallas_call(
        functools.partial(layer_kernel, head_dim, pad_cap),
        out_shape=(pltpu.VMEM(x.shape, bf16), jax.ShapeDtypeStruct((n_src, tokens + experts, d_model), bf16)),
        in_specs=[hbm] * 12,
        out_specs=(pl.BlockSpec(memory_space=pltpu.VMEM), hbm),
        scratch_shapes=[
            *(pltpu.VMEM(small.shape, small.dtype) for small in (idx_t, slot_t, gate_t, attn_gain, moe_gain)),
            pltpu.VMEM((tokens, d_model), bf16),
            pltpu.VMEM(rope.shape, f32),
            pltpu.VMEM((n_rows, ffn), f32),
            pltpu.VMEM((n_exp, n_rows, d_model), bf16),
            pltpu.VMEM((parts, n_exp, 2, part_depth, ffn), bf16),
            pltpu.VMEM((parts, n_sub, n_exp, ffn, block_cols), bf16),
            pltpu.VMEM((4, tokens + experts, d_model), bf16),
            pltpu.VMEM((tokens + experts, d_model), bf16),
            pltpu.VMEM((tokens, d_model), bf16),
            pltpu.VMEM((n_exp, n_rows, ffn), bf16),
            pltpu.VMEM((n_src, tokens, n_exp * pad_cap), bf16),
            pltpu.VMEM((n_src, n_exp * pad_cap, block_cols), bf16),
            *[pltpu.VMEM((2, 4, tokens, block_cols), f32)] * 3,
            *[pltpu.VMEM((3, 2, half, block_cols), f32)] * 3,
            dma((3,)), dma((3, 3, 2)), dma((3,)), dma((3, 2)), dma,
            dma((2, 2)), dma((3, 2)), dma((parts, chunks)), dma((2, 4)), dma((2, 4)), *[dma((3, 2))] * 3,
        ],
        compiler_params=pltpu.CompilerParams(collective_id=1, has_side_effects=True, vmem_limit_bytes=60 * 1024 * 1024),
        cost_estimate=pl.CostEstimate(flops=40_000_000_000, bytes_accessed=30_000_000, transcendentals=0),
        name='whole_layer',
    )(idx_t, slot_t, gate_t, attn_gain, moe_gain, x, rope, qkv, proj, gate_w, up_w, down_w)[0]


def solution(mesh):
    tok_spec = P(('data', 'fsdp', 'ep'), None, None)
    ep_count = mesh.shape['ep']

    def local_step(x_blk, idx_blk, slot_blk, gate_blk, attn_gain, qkv_shard, out_shard, moe_gain, gate_shard, up_shard, down_shard):
        batch_rows, seq_len, d_model = x_blk.shape
        tokens = batch_rows * seq_len
        top_k = idx_blk.shape[-1]
        head_dim = qkv_shard.shape[3]
        experts = gate_shard.shape[0] * ep_count
        capacity = capacity_of(tokens, top_k, experts)
        pad_cap = 16 * ((capacity + 15) // 16)
        by_choice = [blk.reshape(tokens, top_k).T for blk in (idx_blk, slot_blk, gate_blk)]
        qkv = qkv_shard.transpose(1, 2, 3, 0).reshape(3, d_model, -1)
        proj = out_shard.reshape(-1, d_model)
        result = whole_layer(head_dim, pad_cap, x_blk.reshape(tokens, d_model), *by_choice, attn_gain, moe_gain, qkv, proj, gate_shard, up_shard, down_shard, experts)
        return result.reshape(batch_rows, seq_len, d_model)

    return jax.shard_map(local_step, mesh=mesh, in_specs=(tok_spec, tok_spec, tok_spec, tok_spec, P(None), P('fsdp', None, None, None), P('fsdp', None, None), P(None), P('ep', 'fsdp', None), P('ep', 'fsdp', None), P('ep', None, 'fsdp')), out_specs=tok_spec, check_vma=False)
```

```python
import functools

import jax
import jax.numpy as jnp
import numpy as np
from jax import lax
from jax.experimental import pallas as pl
from jax.experimental.pallas import tpu as pltpu
from jax.sharding import PartitionSpec as P

NORM_EPS = 1e-6
ROPE_BASE = 10000.0
MESH_ID = pl.DeviceIdType.MESH
LANES = 128
BOTH = (0, 1)
LANES_BOTH = (((1,), (1,)), ((), ()))


def capacity_of(tok_count, top_k, experts):
    return 8 * ((5 * tok_count * top_k) // (32 * experts) + 1)


def rope_tables(seq_len, head_dim):
    half = head_dim // 2
    lane = np.arange(LANES)
    inv_freq = ROPE_BASE ** (-(lane % half) / half)
    angles = np.arange(seq_len)[:, None] * inv_freq[None, :]
    sign = np.where(lane % head_dim < half, -1.0, 1.0)
    return np.cos(angles).astype(np.float32), (np.sin(angles) * sign).astype(np.float32)


def two(i):
    return i % 2


def three(i):
    return i % 3


def layer_place():
    dx, dz, ep = lax.axis_index('data'), lax.axis_index('fsdp'), lax.axis_index('ep')
    return dx, dz, ep // 2, ep % 2


def flip(pos, bit):
    return (1 - pos) if bit else pos


def toggled(pos, bit):
    return pos + bit - 2 * pos * bit


def related(place, chip_rel, core_rel):
    dx, dz, dy, dc = place
    return flip(dx, chip_rel & 1), dz, flip(dy, chip_rel & 2), flip(dc, core_rel)


def slot_of(place):
    dx, _, dy, dc = place
    return dx * 4 + dy * 2 + dc


def dev_id(place):
    dx, dz, dy, dc = place
    return (dx, dz, dy * 2 + dc)


def remote(src, dst, send_sem, recv_sem, where):
    return pltpu.make_async_remote_copy(src_ref=src, dst_ref=dst, send_sem=send_sem, recv_sem=recv_sem, device_id=dev_id(where), device_id_type=MESH_ID)


def run_if(cond, body):
    if not isinstance(cond, bool):
        pl.when(cond)(body)
    elif cond:
        body()


def wait_in(ref, sem):
    pltpu.make_async_copy(ref, ref, sem).wait()


def spread_in_layer(place, own_refs, part_refs, send_sem, direct_sems, partner_sem, half_size, partner_size):
    across_x, across_y, partner = related(place, 1, 0), related(place, 2, 0), related(place, 0, 1)

    def pass_on(chip_rel, half, target, sem, first=False):
        owner = slot_of(related(place, chip_rel, 0))
        dsts = part_refs(owner, half)
        for src, dst in zip(own_refs(half) if first else dsts, dsts):
            remote(src, dst, send_sem, sem, target).start()

    def direct(rel_there, half):
        return direct_sems.at[rel_there - 1, half]

    for half in BOTH:
        pass_on(0, half, across_x, direct(1, half), True)
        pass_on(0, 1 - half, across_y, direct(2, 1 - half), True)
    for half in BOTH:
        pass_on(0, half, partner, partner_sem, True)
    yield

    def arrived(chip_rel, half):
        wait_in(half_size, direct(chip_rel, half))

    arrived(1, 0)
    pass_on(1, 0, across_y, direct(3, 0))
    pass_on(1, 0, partner, partner_sem)
    arrived(2, 1)
    pass_on(2, 1, across_x, direct(3, 1))
    pass_on(2, 1, partner, partner_sem)
    yield
    arrived(1, 1)
    pass_on(1, 1, partner, partner_sem)
    arrived(2, 0)
    pass_on(2, 0, partner, partner_sem)
    yield
    arrived(3, 0)
    pass_on(3, 0, partner, partner_sem)
    arrived(3, 1)
    pass_on(3, 1, partner, partner_sem)
    yield
    wait_in(partner_size, partner_sem)
    yield


def norm_rows(src, gain_ref, dst, rows):
    tile = 128
    gain = gain_ref[...].astype(jnp.float32).reshape(1, -1)

    def body(t, carry):
        at = pl.ds(pl.multiple_of(t * tile, tile), tile)
        wide = src[at].astype(jnp.float32)
        inv_rms = lax.rsqrt(jnp.mean(wide * wide, axis=-1, keepdims=True) + NORM_EPS)
        dst[at] = (wide * inv_rms * gain).astype(jnp.bfloat16)
        return carry

    lax.fori_loop(0, rows // tile, body, 0)


def attend(x_ref, normed, weights, rope, qkv, hidden, head_dim):
    tokens, d_model = x_ref.shape
    lane = lax.broadcasted_iota(jnp.int32, (tokens, LANES), 1)
    low_half = lane % head_dim < head_dim // 2
    first_head = lax.broadcasted_iota(jnp.int32, (tokens // 2, LANES), 1) < head_dim
    group = 2 * LANES
    q_tile = tokens // 2
    scale = head_dim ** -0.5

    def rotate(val):
        swapped = jnp.where(low_half, pltpu.roll(val, LANES - head_dim // 2, 1), pltpu.roll(val, head_dim // 2, 1))
        return (val * rope[0] + swapped * rope[1]).astype(jnp.bfloat16)

    def project(b, cols):
        return lax.dot_general(normed[:tokens], weights[b, cols, :], LANES_BOTH, preferred_element_type=jnp.float32)

    def group_body(g, carry):
        cols = pl.ds(pl.multiple_of(g * group, group), group)
        query, keys = project(0, cols), project(1, cols)
        values = project(2, cols).astype(jnp.bfloat16)
        for pair in BOTH:
            at = slice(pair * LANES, (pair + 1) * LANES)
            qkv[0, :tokens, at] = rotate(query[:, at])
            qkv[1, :tokens, at] = rotate(keys[:, at])
            qkv[2, :tokens, at] = values[:, at]
        for pair in BOTH:
            at = slice(pair * LANES, (pair + 1) * LANES)
            for tile in BOTH:
                n_keys = (tile + 1) * q_tile
                q_pair = qkv[0, tile * q_tile:(tile + 1) * q_tile, at]
                k_pair, v_pair = qkv[1, :n_keys, at], qkv[2, :n_keys, at]
                row_id = lax.broadcasted_iota(jnp.int32, (q_tile, n_keys), 0) + tile * q_tile
                causal = row_id >= lax.broadcasted_iota(jnp.int32, (q_tile, n_keys), 1)
                outs = []
                for head in BOTH:
                    q_head = jnp.where(first_head if head == 0 else ~first_head, q_pair, jnp.zeros((), jnp.bfloat16))
                    scores = lax.dot_general(q_head, k_pair, LANES_BOTH, preferred_element_type=jnp.float32)
                    scores = jnp.where(causal, scores * scale, -1e30)
                    top = jnp.max(scores, axis=-1, keepdims=True)
                    weight = jnp.exp(scores - top)
                    probs = (weight * (1.0 / jnp.sum(weight, axis=-1, keepdims=True))).astype(jnp.bfloat16)
                    outs.append(jnp.dot(probs, v_pair, preferred_element_type=jnp.float32))
                out_cols = pl.ds(pl.multiple_of(g * group + pair * LANES, LANES), LANES)
                qkv[3, tile * q_tile:(tile + 1) * q_tile, out_cols] = jnp.where(first_head, outs[0], outs[1]).astype(jnp.bfloat16)
        return carry

    lax.fori_loop(0, d_model // group, group_body, 0)

    def out_body(g, carry):
        cols = pl.ds(pl.multiple_of(g * group, group), group)
        attn_out = jnp.dot(qkv[3, :tokens], weights[3, :d_model, cols], preferred_element_type=jnp.float32)
        hidden[:, cols] = (x_ref[:, cols].astype(jnp.float32) + attn_out).astype(jnp.bfloat16)
        return carry

    lax.fori_loop(0, d_model // group, out_body, 0)


def layer_kernel(head_dim, pad_cap,
                 idx_hbm, slot_hbm, gate_idx_hbm, attn_gain_hbm, moe_gain_hbm, x_hbm, rope_hbm, qkv_hbm, proj_hbm, gate_hbm, up_hbm, down_hbm,
                 out_ref, tok_hbm,
                 idx_ref, slot_ref, gate_ref, attn_gain_ref, moe_gain_ref, x_ref, rope, gate_act, big, gate_up, down_all, work, own_tok, hidden, inner, comb, y_buf, send_core, acc, got_core, got_x, got_y, got_last,
                 attn_z_recv, attn_direct, attn_partner, tok_direct, tok_partner,
                 z_own, z_pass, z_recv, core_send, core_recv, x_send, y_send, last_send):
    place = layer_place()
    dx, dz, dy, dc = place
    tokens, d_model = x_ref.shape
    x_recv, y_recv, last_recv = [attn_direct.at[n] for n in range(3)]
    load_sems = [x_send.at[n // 2, n % 2] for n in range(5)]
    small_sems = [core_send.at[n // 4, n % 4] for n in range(5)]
    attn_send, attn_z_send = [[last_send.at[n, m] for n in range(3)] for m in BOTH]
    tok_send, tok_sem, tok_load = y_send.at[0, 0], y_send.at[0, 1], y_send.at[1]
    experts = own_tok.shape[0] - tokens
    n_exp, n_rows, ffn = inner.shape
    n_src = comb.shape[0]
    block_cols = acc.shape[-1]
    half_tok = tokens // 2
    n_sub = down_all.shape[1]
    chunks = n_exp + 2 + n_sub
    across_x, across_y, partner = related(place, 1, 0), related(place, 2, 0), related(place, 0, 1)
    upper = dz // 2
    inside = (dz == 1) | (dz == 2)
    at_end = (dz == 0) | (dz == 3)
    first_exp = dx * n_exp
    mine = slot_of(place)

    def at_z(z):
        return (dx, z, dy, dc)

    x_copy_in = pltpu.make_async_copy(x_hbm, x_ref, load_sems[0])
    rope_copy_in = pltpu.make_async_copy(rope_hbm, rope, load_sems[1])
    small_copies = [pltpu.make_async_copy(src, dst, small_sems[n]) for n, (src, dst) in enumerate(((idx_hbm, idx_ref), (slot_hbm, slot_ref), (gate_idx_hbm, gate_ref), (attn_gain_hbm, attn_gain_ref), (moe_gain_hbm, moe_gain_ref)))]
    for copy in [x_copy_in, rope_copy_in] + small_copies:
        copy.start()
    barrier = pltpu.get_barrier_semaphore()
    for target in [at_z((dz + step) % 4) for step in (1, 2, 3)] + [across_x, across_y, partner]:
        pl.semaphore_signal(barrier, inc=1, device_id=dev_id(target), device_id_type=MESH_ID)
    pl.semaphore_wait(barrier, 6)

    shard_rows = proj_hbm.shape[0]
    row_piece, col_piece = shard_rows // 8, d_model // 8

    def qkv_rows(start, rows, col_z=None):
        at = pl.ds(pl.multiple_of(start, rows), rows)
        if col_z is None:
            return qkv_hbm.at[:, at]
        return big.at[pl.ds(0, 3), at, pl.ds(pl.multiple_of(col_z * shard_rows, shard_rows), shard_rows)]

    def proj_rows(start, rows):
        return big.at[3, pl.ds(pl.multiple_of(start, rows), rows)]

    def size_of(halves):
        return big.at[0, pl.ds(0, halves * row_piece * 2)]

    z_steps = (1, 3, 2)
    for index, step in enumerate(z_steps):
        proj_src = proj_hbm.at[pl.ds(pl.multiple_of(mine * row_piece, row_piece), row_piece)]
        for src, dst in ((qkv_rows(mine * col_piece, col_piece), qkv_rows(mine * col_piece, col_piece, dz)), (proj_src, proj_rows(dz * shard_rows + mine * row_piece, row_piece))):
            remote(src, dst, attn_z_send[index], attn_z_recv.at[index], at_z((dz + step) % 4)).start()

    last_exp, last_sub = n_exp - 1, n_sub - 1

    def down_part(j):
        sub = j - n_exp - 1
        if sub < last_sub:
            return sub, 0, n_exp
        return (last_sub, 0, last_exp) if sub == last_sub else (last_sub, last_exp, 1)

    def chunk_refs(p, j):
        if j < last_exp:
            return [gate_up.at[p, j, m] for m in BOTH]
        if j <= n_exp:
            return [gate_up.at[p, last_exp, j - last_exp]]
        sub, low, count = down_part(j)
        return [down_all.at[p, sub, pl.ds(low, count)]]

    def chunk_srcs(j):
        if j < last_exp:
            return [gate_hbm.at[first_exp + j], up_hbm.at[first_exp + j]]
        if j <= n_exp:
            return [(gate_hbm, up_hbm)[j - last_exp].at[first_exp + last_exp]]
        sub, low, count = down_part(j)
        return [down_hbm.at[pl.ds(first_exp + low, count), :, pl.ds(sub * block_cols, block_cols)]]

    def kind_of(j):
        return 0 if j <= n_exp else 1

    def own_copies(side, j):
        target = at_z(dz - 1 if side == 0 else dz + 1)
        return [remote(src, dst, z_own.at[side, kind_of(j)], z_recv.at[dz, j], target) for src, dst in zip(chunk_srcs(j), chunk_refs(dz, j))]

    def whole_chunk(p, j):
        return gate_up.at[p, j] if j < last_exp else chunk_refs(p, j)[0]

    def pass_copy(which, p, j, z):
        return remote(whole_chunk(p, j), whole_chunk(p, j), z_pass.at[which, kind_of(j)], z_recv.at[p, j], at_z(z))

    def wait_chunk(p, j):
        wait_in(whole_chunk(p, j), z_recv.at[p, j])

    end_z, mid_z, far_z = 3 * (dz - 1), 3 - dz, 3 * (2 - dz)
    passes = ((end_z, mid_z), (mid_z, end_z), (far_z, end_z))

    def send_own(j):
        @pl.when(dz > 0)
        def _():
            for copy in own_copies(0, j):
                copy.start()

        @pl.when(dz < 3)
        def _():
            for copy in own_copies(1, j):
                copy.start()

    def forward(kinds, js):
        @pl.when(inside)
        def _():
            for j in js:
                for which in kinds:
                    p, z = passes[which]
                    wait_chunk(p, j)
                    pass_copy(which, p, j, z).start()

    near, far, expert_js, down_js = BOTH, (2,), range(n_exp + 1), range(n_exp + 1, chunks)

    def need(j):
        @pl.when(at_end)
        def _():
            for k in range(3):
                wait_chunk(k + 1 - upper, j)

    for j in expert_js:
        send_own(j)
    own_loads = [
        (qkv_hbm, big.at[pl.ds(0, 3), pl.ds(0, d_model), pl.ds(pl.multiple_of(dz * shard_rows, shard_rows), shard_rows)], 2),
        (proj_hbm, proj_rows(dz * shard_rows, shard_rows), 2),
    ]
    for j in range(chunks):
        own_loads += [(src, dst, 3 + kind_of(j)) for src, dst in zip(chunk_srcs(j), chunk_refs(dz, j))]
    for src, dst, sem in own_loads:
        pltpu.make_async_copy(src, dst, load_sems[sem]).start()

    for copy in [x_copy_in] + small_copies:
        copy.wait()
    norm_rows(x_ref, attn_gain_ref, own_tok, tokens)

    expert_ids = lax.broadcasted_iota(jnp.int32, (experts, tokens), 0)
    slot_tab = jnp.zeros((experts, tokens), jnp.float32)
    gate_tab = jnp.zeros((experts, tokens), jnp.float32)
    for k in range(idx_ref.shape[0]):
        hit = expert_ids == idx_ref[k:k + 1, :]
        slot_tab = slot_tab + jnp.where(hit, slot_ref[k:k + 1, :].astype(jnp.float32) + 1.0, 0.0)
        gate_tab = gate_tab + jnp.where(hit, gate_ref[k:k + 1, :].astype(jnp.float32), 0.0)
    own_tok[tokens:, :tokens] = (slot_tab - 1.0).astype(jnp.bfloat16)
    own_tok[tokens:, tokens:] = gate_tab.astype(jnp.bfloat16)

    streams = []
    for index, step in enumerate(z_steps):
        source_z = (dz + 4 - step) % 4

        def part_refs(slot, half, source_z=source_z):
            cols, rows = col_piece // 2, row_piece // 2
            return [qkv_rows(slot * col_piece + half * cols, cols, source_z), proj_rows(source_z * shard_rows + slot * row_piece + half * rows, rows)]

        streams.append(spread_in_layer(place, functools.partial(part_refs, mine), part_refs, attn_send[index], attn_direct.at[index], attn_partner.at[index], size_of(1), size_of(8)))
    for index, stream in enumerate(streams):
        wait_in(size_of(2), attn_z_recv.at[index])
        next(stream)
    for _ in range(4):
        for stream in streams:
            next(stream)
    wait_in(size_of(16), load_sems[2])
    rope_copy_in.wait()

    attend(x_ref, own_tok, big, rope, work, hidden, head_dim)
    norm_rows(hidden, moe_gain_ref, own_tok, tokens)
    for index in range(3):
        wait_in(size_of(14), attn_send[index])
        wait_in(size_of(2), attn_z_send[index])

    half_rows = own_tok.shape[0] // 2

    def tok_part(slot, half):
        return [tok_hbm.at[slot, pl.ds(half * half_rows, half_rows)]]

    def tok_half(half):
        return [own_tok.at[pl.ds(half * half_rows, half_rows)]]

    stream = spread_in_layer(place, tok_half, tok_part, tok_send, tok_direct, tok_partner, tok_part(0, 0)[0], tok_hbm.at[pl.ds(0, 4)])
    next(stream)
    tok_copy = pltpu.make_async_copy(own_tok, tok_hbm.at[mine], tok_sem)
    tok_copy.start()
    forward(near, expert_js)
    for _ in range(4):
        next(stream)
    tok_copy.wait()
    wait_in(tok_hbm.at[pl.ds(0, 7)], tok_send)
    forward(far, expert_js)
    for j in down_js:
        send_own(j)

    def tok_in(s):
        return pltpu.make_async_copy(tok_hbm.at[s], work.at[s % 2], tok_load.at[s % 2])

    my_first = (lax.axis_index('ep') * 2 + dx) * n_exp
    pick_row = (lax.broadcasted_iota(jnp.int32, (8, experts), 1) == my_first + lax.broadcasted_iota(jnp.int32, (8, experts), 0)).astype(jnp.bfloat16)
    pick_col = (lax.broadcasted_iota(jnp.int32, (experts, LANES), 0) == my_first + lax.broadcasted_iota(jnp.int32, (experts, LANES), 1)).astype(jnp.bfloat16)
    tok_in(0).start()

    def dispatch_body(s, carry):
        @pl.when(s + 1 < n_src)
        def _():
            tok_in(s + 1).start()

        tok_in(s).wait()
        u = work[s % 2, :tokens]
        tables = work[s % 2, tokens:]
        slot_row = jnp.dot(pick_row, tables, preferred_element_type=jnp.float32)
        col_tab = lax.dot_general(tables, pick_col, (((0,), (0,)), ((), ())), preferred_element_type=jnp.float32)
        slot_ids = lax.broadcasted_iota(jnp.int32, (pad_cap, tokens), 0).astype(jnp.float32)
        rows = pl.ds(pl.multiple_of(s * pad_cap, pad_cap), pad_cap)
        for e in range(n_exp):
            one_hot = jnp.where(slot_ids == slot_row[e:e + 1, :tokens], 1.0, 0.0).astype(jnp.bfloat16)
            big[e, rows] = jnp.dot(one_hot, u, preferred_element_type=jnp.float32).astype(jnp.bfloat16)
        buf_ids = lax.broadcasted_iota(jnp.int32, (tokens, n_exp * pad_cap), 1).astype(jnp.float32)
        gates = jnp.zeros((tokens, n_exp * pad_cap), jnp.float32)
        for e in range(n_exp):
            slot_e = col_tab[:tokens, e:e + 1]
            dest_e = jnp.where(slot_e >= 0.0, slot_e + float(e * pad_cap), -1.0)
            gates = jnp.where(buf_ids == dest_e, col_tab[tokens:, e:e + 1], gates)
        comb[s] = gates.astype(jnp.bfloat16)
        return carry

    lax.fori_loop(0, n_src, dispatch_body, 0)

    row_tile = n_rows // 4

    def tile_loop(body):
        def tile_body(t, carry):
            body(pl.ds(pl.multiple_of(t * row_tile, row_tile), row_tile))
            return carry

        lax.fori_loop(0, 4, tile_body, 0)

    def product(e, m, at):
        return jnp.dot(big[e, at], gate_up[:, e, m].reshape(d_model, ffn), preferred_element_type=jnp.float32)

    def expert_inner(e):
        def body(at):
            gate = product(e, 0, at)
            inner[e, at] = (gate * jax.nn.sigmoid(gate) * product(e, 1, at)).astype(jnp.bfloat16)

        need(e)
        tile_loop(body)

    def last_gate(at):
        gate = product(last_exp, 0, at)
        gate_act[at] = gate * jax.nn.sigmoid(gate)

    def last_up(at):
        inner[last_exp, at] = (gate_act[at] * product(last_exp, 1, at)).astype(jnp.bfloat16)

    def block_of(i):
        k, sub = i // n_sub, i % n_sub
        if isinstance(i, int) and k == 0:
            return dz, sub
        near_end = dz + upper * (3 - 2 * dz)
        low = k - near_end * ((3 - k) // 2)
        return low + upper * (3 - 2 * low), sub

    def rel_slot(rel, core_rel):
        return toggled(dx, rel % 2) * 4 + toggled(dy, rel // 2) * 2 + flip(dc, core_rel)

    halves = (pl.ds(0, half_tok), pl.ds(half_tok, half_tok))

    def core_copy(i, rel):
        return remote(send_core.at[two(i), rel], got_core.at[two(i), rel], core_send.at[two(i), rel], core_recv.at[two(i), rel], partner)

    def x_copy(i, rel):
        where = (3 - rel) // 2
        return remote(acc.at[two(i), rel, halves[0]], got_x.at[three(i), where], x_send.at[three(i), where], x_recv.at[three(i), where], across_x)

    def y_copy(i, rel):
        where = 3 - rel
        return remote(acc.at[two(i), rel, halves[1]], got_y.at[three(i), where], y_send.at[three(i), where], y_recv.at[three(i), where], across_y)

    def last_copy(i, which):
        rel, target = ((2, across_y), (1, across_x))[which]
        return remote(acc.at[two(i), rel, halves[which]], got_last.at[three(i), which], last_send.at[three(i), which], last_recv.at[three(i), which], target)

    def wait_down(i, last_parts=BOTH):
        p, sub = block_of(i)

        def wait_parts():
            for part in last_parts:
                wait_chunk(p, n_exp + 1 + last_sub + part)

        if not (isinstance(i, int) and i < n_sub):
            @pl.when(at_end)
            def _():
                run_if(sub < last_sub, lambda: wait_in(down_all.at[p, sub], z_recv.at[p, n_exp + 1 + sub]))
                run_if(sub == last_sub, wait_parts)

    def y_block(i, low=0, high=n_exp, last_parts=BOTH):
        p, sub = block_of(i)
        wait_down(i, last_parts)

        def y_body(e, carry):
            y_tall = jnp.dot(inner[e], down_all[p, sub, e], preferred_element_type=jnp.float32).astype(jnp.bfloat16)
            at = pl.ds(pl.multiple_of(e * pad_cap, pad_cap), pad_cap)
            for s in range(n_src):
                y_buf[s, at] = y_tall[s * pad_cap:(s + 1) * pad_cap]
            return carry

        lax.fori_loop(low, high, y_body, 0)

    def sum_block(i, with_y=False):
        p, sub = block_of(i)

        def partial(rel, core_rel):
            slot = rel_slot(rel, core_rel)
            if with_y:
                rows = pl.ds(pl.multiple_of(slot * pad_cap, pad_cap), pad_cap)
                for e in (last_exp,):
                    y_buf[slot, e * pad_cap:(e + 1) * pad_cap] = jnp.dot(inner[e, rows], down_all[p, sub, e], preferred_element_type=jnp.float32).astype(jnp.bfloat16)
            return jnp.dot(comb[slot], y_buf[slot], preferred_element_type=jnp.float32)

        def core_body(k, carry):
            rel = 3 - k
            send_core[two(i), rel] = partial(rel, 1)
            core_copy(i, rel).start()
            return carry

        def own_body(k, carry):
            rel = 3 - k
            own = partial(rel, 0)
            wait_in(got_core.at[two(i), rel], core_recv.at[two(i), rel])
            acc[two(i), rel] = own + got_core[two(i), rel]

            run_if(rel % 2 == 1, lambda: x_copy(i, rel).start())
            run_if(rel // 2 == 1, lambda: y_copy(i, rel).start())

            return carry

        if with_y:
            lax.fori_loop(0, 3, core_body, 0)
            own_body(0, 0)
            core_body(3, 0)
            lax.fori_loop(1, 4, own_body, 0)
        else:
            lax.fori_loop(0, 4, core_body, 0)
            lax.fori_loop(0, 4, own_body, 0)

    def turn_block(i):
        wait_in(got_x.at[three(i), 0], x_recv.at[three(i), 0])
        acc[two(i), 2, halves[0]] += got_x[three(i), 0]
        last_copy(i, 0).start()
        wait_in(got_y.at[three(i), 0], y_recv.at[three(i), 0])
        acc[two(i), 1, halves[1]] += got_y[three(i), 0]
        last_copy(i, 1).start()

    def end_block(i):
        p, sub = block_of(i)
        cols = pl.ds(pl.multiple_of((p * n_sub + sub) * block_cols, block_cols), block_cols)
        for half, got, got_sems in ((0, got_x, x_recv), (1, got_y, y_recv)):
            wait_in(got.at[three(i), 1], got_sems.at[three(i), 1])
            wait_in(got_last.at[three(i), half], last_recv.at[three(i), half])
            total = acc[two(i), 0, halves[half]] + got[three(i), 1] + got_last[three(i), half]
            out_ref[halves[half], cols] = (hidden[halves[half], cols].astype(jnp.float32) + total).astype(jnp.bfloat16)
        for rel in range(4):
            core_copy(i, rel).wait_send()
        for rel in (3, 1):
            x_copy(i, rel).wait_send()
        for rel in (3, 2):
            y_copy(i, rel).wait_send()
        for which in BOTH:
            last_copy(i, which).wait_send()

    wait_in(gate_up.at[0], load_sems[3])
    wait_in(down_all.at[0], load_sems[4])
    for e in range(last_exp):
        expert_inner(e)
    y_block(0, 0, last_exp)
    need(last_exp)
    tile_loop(last_gate)
    need(n_exp)
    tile_loop(last_up)

    blocks = 4 * n_sub
    y_block(0, last_exp, n_exp)
    sum_block(0)
    forward(near, down_js)
    y_block(1)
    turn_block(0)
    sum_block(1)
    end_block(0)
    y_block(2)
    turn_block(1)
    sum_block(2)
    forward(far, down_js)
    end_block(1)

    def block_body(i, carry):
        y_block(i + 1)
        turn_block(i)
        sum_block(i + 1)
        end_block(i)
        return carry

    lax.fori_loop(2, blocks - 3, block_body, 0)

    turn_block(blocks - 3)
    y_block(blocks - 2)
    sum_block(blocks - 2)
    end_block(blocks - 3)
    y_block(blocks - 1, 0, last_exp, (0,))
    turn_block(blocks - 2)
    wait_down(blocks - 1, (1,))
    sum_block(blocks - 1, with_y=True)
    end_block(blocks - 2)
    turn_block(blocks - 1)
    end_block(blocks - 1)

    for kind, size in ((0, gate_up.at[0]), (1, down_all.at[0])):
        @pl.when(dz > 0)
        def _():
            wait_in(size, z_own.at[0, kind])

        @pl.when(dz < 3)
        def _():
            wait_in(size, z_own.at[1, kind])

        @pl.when(inside)
        def _():
            for which in range(3):
                wait_in(size, z_pass.at[which, kind])


def whole_layer(head_dim, pad_cap, x, idx_t, slot_t, gate_t, attn_gain, moe_gain, qkv, proj, gate_w, up_w, down_w, experts):
    tokens, d_model = x.shape
    n_exp = gate_w.shape[0] // 2
    part_depth, ffn = gate_w.shape[1:]
    parts, n_src, block_cols = 4, 8, LANES
    n_sub = down_w.shape[2] // block_cols
    chunks = n_exp + 2 + n_sub
    n_rows = n_src * pad_cap
    half = tokens // 2
    rope = np.stack(rope_tables(tokens, head_dim))
    dma = pltpu.SemaphoreType.DMA
    bf16, f32 = jnp.bfloat16, jnp.float32
    hbm = pl.BlockSpec(memory_space=pl.ANY)
    return pl.pallas_call(
        functools.partial(layer_kernel, head_dim, pad_cap),
        out_shape=(pltpu.VMEM(x.shape, bf16), jax.ShapeDtypeStruct((n_src, tokens + experts, d_model), bf16)),
        in_specs=[hbm] * 12,
        out_specs=(pl.BlockSpec(memory_space=pltpu.VMEM), hbm),
        scratch_shapes=[
            *(pltpu.VMEM(small.shape, small.dtype) for small in (idx_t, slot_t, gate_t, attn_gain, moe_gain)),
            pltpu.VMEM((tokens, d_model), bf16),
            pltpu.VMEM(rope.shape, f32),
            pltpu.VMEM((n_rows, ffn), f32),
            pltpu.VMEM((n_exp, n_rows, d_model), bf16),
            pltpu.VMEM((parts, n_exp, 2, part_depth, ffn), bf16),
            pltpu.VMEM((parts, n_sub, n_exp, ffn, block_cols), bf16),
            pltpu.VMEM((4, tokens + experts, d_model), bf16),
            pltpu.VMEM((tokens + experts, d_model), bf16),
            pltpu.VMEM((tokens, d_model), bf16),
            pltpu.VMEM((n_exp, n_rows, ffn), bf16),
            pltpu.VMEM((n_src, tokens, n_exp * pad_cap), bf16),
            pltpu.VMEM((n_src, n_exp * pad_cap, block_cols), bf16),
            *[pltpu.VMEM((2, 4, tokens, block_cols), f32)] * 3,
            *[pltpu.VMEM((3, 2, half, block_cols), f32)] * 3,
            dma((3,)), dma((3, 3, 2)), dma((3,)), dma((3, 2)), dma,
            dma((2, 2)), dma((3, 2)), dma((parts, chunks)), dma((2, 4)), dma((2, 4)), *[dma((3, 2))] * 3,
        ],
        compiler_params=pltpu.CompilerParams(collective_id=1, has_side_effects=True, vmem_limit_bytes=60 * 1024 * 1024),
        cost_estimate=pl.CostEstimate(flops=40_000_000_000, bytes_accessed=30_000_000, transcendentals=0),
        name='whole_layer',
    )(idx_t, slot_t, gate_t, attn_gain, moe_gain, x, rope, qkv, proj, gate_w, up_w, down_w)[0]


def solution(mesh):
    tok_spec = P(('data', 'fsdp', 'ep'), None, None)
    ep_count = mesh.shape['ep']

    def local_step(x_blk, idx_blk, slot_blk, gate_blk, attn_gain, qkv_shard, out_shard, moe_gain, gate_shard, up_shard, down_shard):
        batch_rows, seq_len, d_model = x_blk.shape
        tokens = batch_rows * seq_len
        top_k = idx_blk.shape[-1]
        head_dim = qkv_shard.shape[3]
        experts = gate_shard.shape[0] * ep_count
        capacity = capacity_of(tokens, top_k, experts)
        pad_cap = 16 * ((capacity + 15) // 16)
        by_choice = [blk.reshape(tokens, top_k).T for blk in (idx_blk, slot_blk, gate_blk)]
        qkv = qkv_shard.transpose(1, 2, 3, 0).reshape(3, d_model, -1)
        proj = out_shard.reshape(-1, d_model)
        result = whole_layer(head_dim, pad_cap, x_blk.reshape(tokens, d_model), *by_choice, attn_gain, moe_gain, qkv, proj, gate_shard, up_shard, down_shard, experts)
        return result.reshape(batch_rows, seq_len, d_model)

    return jax.shard_map(local_step, mesh=mesh, in_specs=(tok_spec, tok_spec, tok_spec, tok_spec, P(None), P('fsdp', None, None, None), P('fsdp', None, None), P(None), P('ep', 'fsdp', None), P('ep', 'fsdp', None), P('ep', None, 'fsdp')), out_specs=tok_spec, check_vma=False)
```
